128 devices in a mesh: dp: 32 (over y, x, core), head: 4 (over z).
Axes of the slice: x: 4, y: 4, z: 4, core: 2. Of those that a mesh axis runs over, the one named last changes fastest.
Arguments:
- tokens: bfloat16 [8192, 2048], P('dp', 'head'), may hold values from -6 to 6
- mixer_gain: float32 [2048], replicated, may hold values from 0.1 to 1.9
- query_weight: bfloat16 [2048, 1024], P(None, 'head'), may hold values from -0.125 to 0.125
- key_weight: bfloat16 [3, 2048, 1024], P(None, None, 'head'), may hold values from -0.125 to 0.125
- value_weight: bfloat16 [3, 2048, 1024], P(None, None, 'head'), may hold values from -0.125 to 0.125
- beta_weight: bfloat16 [2048, 24], P(None, 'head'), may hold values from -0.125 to 0.125
- head_gain: float32 [128], replicated, may hold values from 0.1 to 1.9
- output_weight: bfloat16 [1024, 2048], P('head'), may hold values from -0.1875 to 0.1875
- expert_gain: float32 [2048], replicated, may hold values from 0.1 to 1.9
- router_weight: float32 [2048, 64], replicated, may hold values from -0.125 to 0.125
- expert_ids: int32 [8192, 2], P(('dp', 'head')), may hold values from 0 to 63, all different within a row; in each aligned block of 64 rows (0 to 63, 64 to 127, ...) at most 4 rows name the same one
- gate_weight: bfloat16 [64, 2048, 1408], P('dp'), may hold values from -0.125 to 0.125
- up_weight: bfloat16 [64, 2048, 1408], P('dp'), may hold values from -0.125 to 0.125
- down_weight: bfloat16 [64, 1408, 2048], P('dp'), may hold values from -0.15625 to 0.15625
Outputs:
- layer_out: bfloat16 [8192, 2048], P(('dp', 'head'))
The draws below stay inside these ranges and needn't reach their ends.
Inputs may be any that keep to these rules, and one draw needn't show every extreme that they name: `expert_ids`: taking the tokens in aligned blocks of 64 (the rows of one device), no expert is named by more than 4 rows of a block, a bound that some block reaches; a token's two experts differ.
All inputs are finite; a program needn't handle non-finite values.
Results may differ from the reference program's by a relative error of at most 0.012.
Values may be sent and summed in bfloat16 or wider, within the bound.
No kernel may reach another device: no remote copies, remote signals or barrier semaphores. Data moves between devices by JAX's collectives and lax.ppermute only.
A program may use at most 128 MiB of HBM per device.

```python
import math
import jax
import jax.numpy as jnp
import numpy as np
from jax import lax

D = 2048
HEADS = 8
DK = 128
NH = 3
FFE = 1408
TOK_DEV = 256
TOKENS = 8192
ROWS = 64
EXPERTS = 64
CAP = 4
N_DP = 32
N_HEAD = 4


def level_of(own_key, shape, shards, smallest, high):
    loudness, own = 1.0, jax.random.fold_in(own_key, 6)
    for dim, parts in shards:
        heights = jnp.exp(jax.random.uniform(jax.random.fold_in(own, dim), (parts,), jnp.float32, smallest / len(shards), high / len(shards)))
        loudness = loudness * jnp.repeat(heights, shape[dim] // parts).reshape([-1 if axis == dim else 1 for axis in range(len(shape))])
    return loudness


def deal_out(rng, own, number, rows, number_of, top, reach, skew):
    ranking = jax.random.permutation(rng, number_of)
    packed, common = load_shares(number_of, rows * top, reach, skew, True), load_shares(number_of, rows * top, reach, skew, False)
    places = jnp.arange(number_of)

    def named(tallies, rotation):
        used = int((tallies > 0).sum())
        fixed = max(1, used // 4)
        moved = fixed + (places - fixed + rotation * (used - fixed)) % max(1, number_of - fixed)
        return jnp.zeros((number_of,), jnp.int32).at[ranking[jnp.where(places < fixed, places, moved)]].set(jnp.asarray(tallies, jnp.int32))

    tallies = jnp.where(number % 4 == 0, named(packed, number // 4), named(common, number - number // 4 - 1))
    mixed = jax.random.permutation(jax.random.fold_in(own, 3), number_of)
    giver, sink = mixed[0:number_of // 2 * 2:2], mixed[1:number_of // 2 * 2:2]
    slack = jnp.minimum(tallies[giver] - 1, reach - tallies[sink]) // 2
    slack = jnp.where((giver == ranking[0]) | (sink == ranking[0]) | (tallies[sink] == 0), 0, jnp.maximum(slack, 0))
    moved = jax.random.randint(jax.random.fold_in(own, 4), (number_of // 2,), 0, 1 << 20) % (slack + 1)
    tallies = tallies.at[giver].add(-moved).at[sink].add(moved)
    labels = jnp.searchsorted(jnp.cumsum(tallies), jnp.arange(rows * top), side="right").astype(jnp.int32)
    listing = labels.reshape(top, rows).T
    listing = listing[jax.random.permutation(jax.random.fold_in(own, 1), rows)]
    rotation = jax.random.randint(jax.random.fold_in(own, 2), (rows, 1), 0, top)
    return jnp.take_along_axis(listing, (jnp.arange(top)[None, :] + rotation) % top, axis=1)


def load_shares(number_of, total, limit, lean, full):
    loads = [(1 << 20) // math.isqrt(standing ** lean) + 1 for standing in range(1, number_of + 1)]
    largest = limit if full else min(limit, max(-(-total // number_of), total * loads[0] // sum(loads)))
    least = 1 if total - largest >= number_of - 1 else 0
    holding, spare = [largest] + [least] * (number_of - 1), total - largest - least * (number_of - 1)
    while spare > 0:
        movable = [i for i in range(1, number_of) if holding[i] < largest] or [i for i in range(1, number_of) if holding[i] < limit]
        mass, remaining = sum([loads[i] for i in movable]), spare
        for i in movable:
            more = min(limit - holding[i], max(1, remaining * loads[i] // mass), spare)
            holding[i] = holding[i] + more
            spare = spare - more
    return np.array(holding)


def noise(key, shape, width, most, cuts=(), held_as=jnp.bfloat16):
    loudness = level_of(key, shape, cuts, -0.22, 0.18) if cuts else 1.0
    entries = jax.random.normal(key, shape, jnp.float32) * width * loudness
    return jnp.minimum(jnp.maximum(entries, -most), most).astype(held_as)


def setup_inputs(seed: int = 0) -> dict:
    streams_of = jax.random.split(jax.random.key(seed), 15)
    tokens = noise(streams_of[0], (TOKENS, D), 1.0, 6.0, ((0, 32), (1, 4)))
    mixer_gain = jnp.clip(1.0 + 0.18 * jax.random.normal(streams_of[1], (D,), jnp.float32), 0.1, 1.9)
    query_weight = noise(streams_of[2], (D, HEADS * DK), D ** -0.5, 0.125, ((1, 4),))
    key_weight = noise(streams_of[3], (NH, D, HEADS * DK), D ** -0.5, 0.125, ((2, 4),))
    value_weight = noise(streams_of[4], (NH, D, HEADS * DK), D ** -0.5, 0.125, ((2, 4),))
    beta_weight = noise(streams_of[5], (D, HEADS * NH), D ** -0.5, 0.125, ((1, 4),))
    head_gain = jnp.clip(1.0 + 0.18 * jax.random.normal(streams_of[6], (DK,), jnp.float32), 0.1, 1.9)
    output_weight = noise(streams_of[7], (HEADS * DK, D), (HEADS * DK) ** -0.5, 0.1875, ((0, 4),))
    expert_gain = jnp.clip(1.0 + 0.18 * jax.random.normal(streams_of[8], (D,), jnp.float32), 0.1, 1.9)
    router_weight = noise(streams_of[9], (D, EXPERTS), D ** -0.5, 0.125, (), jnp.float32)
    expert_ids_keys = jax.random.split(jax.random.fold_in(streams_of[10], 1), TOKENS // ROWS)
    expert_ids_turns = jax.random.permutation(jax.random.fold_in(streams_of[10], 3), TOKENS // ROWS)
    expert_ids = jax.vmap(lambda own, number: deal_out(jax.random.fold_in(streams_of[10], 2), own, number, ROWS, EXPERTS, 2, CAP, 2))(expert_ids_keys, expert_ids_turns).reshape((TOKENS, 2))
    gate_weight = noise(streams_of[11], (EXPERTS, D, FFE), D ** -0.5, 0.125, ((0, 32),))
    up_weight = noise(streams_of[12], (EXPERTS, D, FFE), D ** -0.5, 0.125, ((0, 32),))
    down_weight = noise(streams_of[13], (EXPERTS, FFE, D), FFE ** -0.5, 0.15625, ((0, 32),))
    return dict(tokens=tokens, mixer_gain=mixer_gain, query_weight=query_weight, key_weight=key_weight, value_weight=value_weight, beta_weight=beta_weight, head_gain=head_gain, output_weight=output_weight, expert_gain=expert_gain, router_weight=router_weight, expert_ids=expert_ids, gate_weight=gate_weight, up_weight=up_weight, down_weight=down_weight)


EPSILON = 1e-06
TOP_PRECISION = lax.Precision.HIGHEST

def root_norm(values, gain):
    return values * lax.rsqrt(lax.optimization_barrier(jnp.mean(values * values, -1, keepdims=True)) + EPSILON) * gain

def unit_vector(values):
    return values * lax.rsqrt(lax.optimization_barrier(jnp.sum(values * values, -1, keepdims=True)) + EPSILON)

def reference(tokens, mixer_gain, query_weight, key_weight, value_weight, beta_weight, head_gain, output_weight, expert_gain, router_weight, expert_ids, gate_weight, up_weight, down_weight):
    widened = tokens.astype(jnp.float32)
    normed = root_norm(widened, mixer_gain).astype(jnp.bfloat16)
    query = unit_vector(jnp.dot(normed, query_weight, preferred_element_type=jnp.float32).reshape(TOKENS, HEADS, DK)) * DK ** (-0.5)
    key_rows = unit_vector(jnp.stack([jnp.dot(normed, key_weight[member], preferred_element_type=jnp.float32) for member in range(NH)], 1).reshape(TOKENS, NH, HEADS, DK))
    value_rows = jnp.stack([jnp.dot(normed, value_weight[member], preferred_element_type=jnp.float32) for member in range(NH)], 1).reshape(TOKENS, NH, HEADS, DK)
    beta_rows = 2.0 * jax.nn.sigmoid(jnp.dot(normed, beta_weight, preferred_element_type=jnp.float32))
    beta_rows = jnp.transpose(beta_rows.reshape(TOKENS, HEADS, NH), (0, 2, 1))
    sequences = (jnp.transpose(query.reshape(N_DP, TOK_DEV, HEADS, DK), (1, 0, 2, 3)), jnp.transpose(key_rows.reshape(N_DP, TOK_DEV, NH, HEADS, DK), (1, 2, 0, 3, 4)), jnp.transpose(value_rows.reshape(N_DP, TOK_DEV, NH, HEADS, DK), (1, 2, 0, 3, 4)), jnp.transpose(beta_rows.reshape(N_DP, TOK_DEV, NH, HEADS), (1, 2, 0, 3)))

    def advance(memory_state, inputs):
        query_now, keys_now, values_now, betas_now = inputs
        for member in range(NH):
            predicted = jnp.einsum('bhkv,bhk->bhv', memory_state, keys_now[member], precision=TOP_PRECISION)
            update = betas_now[member][..., None] * (values_now[member] - predicted)
            memory_state = memory_state + keys_now[member][..., :, None] * update[..., None, :]
        return (memory_state, jnp.einsum('bhkv,bhk->bhv', memory_state, query_now, precision=TOP_PRECISION))
    start_memory = jnp.zeros((N_DP, HEADS, DK, DK), jnp.float32)
    mixed_heads = lax.scan(advance, start_memory, sequences)[1]
    mixed_heads = jnp.transpose(mixed_heads, (1, 0, 2, 3)).reshape(TOKENS, HEADS, DK)
    head_out = root_norm(mixed_heads, head_gain).astype(jnp.bfloat16).reshape(TOKENS, HEADS * DK)
    residual = widened + jnp.dot(head_out, output_weight, preferred_element_type=jnp.float32)
    routed = root_norm(residual, expert_gain)
    logits = jnp.dot(routed, router_weight, precision=TOP_PRECISION)
    choose = expert_ids[:, :, None] == jnp.arange(EXPERTS, dtype=jnp.int32)[None, None, :]
    chosen = lax.optimization_barrier(jnp.sum(jnp.where(choose, logits[:, None, :], 0.0), -1))
    leading = jax.nn.sigmoid(chosen[:, 0] - chosen[:, 1])
    pair_weight = jnp.stack([leading, 1.0 - leading], 1)
    block_count = N_DP * N_HEAD
    flat_ids = expert_ids.reshape(block_count, 2 * ROWS).astype(jnp.int32)
    one_hot = (flat_ids[:, :, None] == jnp.arange(EXPERTS, dtype=jnp.int32)[None, None, :]).astype(jnp.int32)
    position = lax.optimization_barrier(jnp.sum((jnp.cumsum(one_hot, 1) - one_hot) * one_hot, 2)).astype(jnp.int32)
    source = jnp.arange(block_count, dtype=jnp.int32)[:, None]
    target = (flat_ids * (block_count * CAP) + source * CAP + position).reshape(-1).astype(jnp.int32)
    expert_rows = routed.astype(jnp.bfloat16)
    buffer_rows = jnp.zeros((EXPERTS * block_count * CAP, D), jnp.bfloat16).at[target].set(jnp.repeat(expert_rows, 2, 0))
    buffer_rows = buffer_rows.reshape(EXPERTS, block_count * CAP, D)

    def one_expert(pieces):
        arrived, gate_part, up_part, down_part = pieces
        gate_rows = jnp.dot(arrived, gate_part, preferred_element_type=jnp.float32)
        lifted = jnp.dot(arrived, up_part, preferred_element_type=jnp.float32)
        hidden = (jax.nn.silu(gate_rows) * lifted).astype(jnp.bfloat16)
        return jnp.dot(hidden, down_part, preferred_element_type=jnp.float32).astype(jnp.bfloat16)
    produced = lax.map(one_expert, (buffer_rows, gate_weight, up_weight, down_weight))
    picked = produced.reshape(EXPERTS * block_count * CAP, D)[target].reshape(TOKENS, 2, D)
    blended = lax.optimization_barrier(jnp.sum(pair_weight[:, :, None] * picked.astype(jnp.float32), 1))
    return (residual + blended).astype(jnp.bfloat16)
```

```python
import jax
import jax.numpy as jnp
from jax import lax
from jax.experimental import pallas as pl
from jax.experimental.pallas import tpu as pltpu
from jax.sharding import PartitionSpec as P

DK = 128
NH = 3
CH = 32
SUB = CH * NH
BASE = 4
EPSILON = 1e-06
F32 = jnp.float32
BF16 = jnp.bfloat16
MIB = 1 << 20


def dot(a, b, dims=((1,), (0,))):
    return lax.dot_general(a, b, (dims, ((), ())), preferred_element_type=F32)


def split(a):
    high = a.astype(BF16)
    return high, (a - high.astype(F32)).astype(BF16)


def dot3(a, b, dims=((1,), (0,))):
    return dot(a[0], b[0], dims) + (dot(a[0], b[1], dims) + dot(a[1], b[0], dims))


def iota(shape, dim):
    return lax.broadcasted_iota(jnp.int32, shape, dim)


def rows_at(block, size):
    return pl.ds(pl.multiple_of(block * size, size), size)


def mixer_kernel(heads, place_ref, x0, x1, x2, x3, gain_ref, wq_ref, wk_ref, wv_ref, wb_ref, head_gain_ref,
                 wo_ref, o0, o1, o2, o3, normed, keys, beta_keys, rhs, queries, reduced, state_map, added, out_add, mixed):
    me = place_ref[0]
    xs = (x0, x1, x2, x3)
    count = len(xs)
    length, part = x0.shape
    sources = [lax.rem(me - k + count, count) for k in range(count)]
    total = 0.0
    for x in xs:
        wide = x[...].astype(F32)
        total = total + jnp.sum(wide * wide, -1, keepdims=True)
    scale = lax.rsqrt(total / (count * part) + EPSILON)
    for k in range(count):
        gain = gain_ref[pl.ds(sources[k], 1), :]
        normed[k] = (xs[k][...].astype(F32) * scale * gain).astype(BF16)

    def project(weight):
        return sum(dot(normed[k], weight(rows_at(sources[k], part))) for k in range(count))

    beta = sum(
        dot(normed[k], wb_ref[:, rows_at(sources[k], part)], ((1,), (1,))) for k in range(count)
    )
    beta = 2.0 / (1.0 + jnp.exp(-beta))
    blocks = length // CH
    query = project(lambda r: wq_ref[r, :])
    for h in range(heads):
        q = query[:, h * DK:(h + 1) * DK]
        q = q * lax.rsqrt(jnp.sum(q * q, -1, keepdims=True) + EPSILON) * DK ** (-0.5)
        queries[h] = q.reshape(blocks, CH, DK)
    for m in range(NH):
        key = project(lambda r: wk_ref[m, r, :])
        value = project(lambda r: wv_ref[m, r, :])
        for h in range(heads):
            b = beta[:, h * NH + m:h * NH + m + 1]
            k = key[:, h * DK:(h + 1) * DK]
            k = k * lax.rsqrt(jnp.sum(k * k, -1, keepdims=True) + EPSILON)
            keys[h, :, m * CH:(m + 1) * CH, :] = k.reshape(blocks, CH, DK)
            rhs[h, :, m * CH:(m + 1) * CH, :DK] = (k * b).astype(BF16).reshape(blocks, CH, DK)
            rhs[h, :, m * CH:(m + 1) * CH, DK:] = (value[:, h * DK:(h + 1) * DK] * b).astype(BF16).reshape(blocks, CH, DK)
            beta_keys[h, :, m * CH:(m + 1) * CH, :] = jnp.broadcast_to(b, (length, DK)).reshape(blocks, CH, DK)

    row, col = iota((SUB, SUB), 0), iota((SUB, SUB), 1)
    row_t, col_t = row % CH, col % CH
    causal = (col_t < row_t) | ((col_t == row_t) & (col < row))
    same = [row_t // s == col_t // s for s in (BASE, BASE * 2, BASE * 4, BASE * 8)]
    eye = (row == col).astype(F32)
    seen = iota((CH, SUB), 1) % CH <= iota((CH, SUB), 0)

    unroll = UNROLL
    for start in range(0, blocks, unroll):
        at = [(h, c) for c in range(start, start + unroll) for h in range(heads)]
        ks = [split(keys[i]) for i in at]
        lower = [
            jnp.where(causal, dot3(k, k, ((1,), (1,))) * beta_keys[i][:, :SUB], 0.0) for i, k in zip(at, ks)
        ]
        power = [jnp.where(same[0], -l, 0.0) for l in lower]
        inverse = [eye + p for p in power]
        span = 2
        while span < BASE * NH:
            power = [p.astype(BF16) for p in power]
            power = [dot(p, p) for p in power]
            inverse = [t + dot(t.astype(BF16), p.astype(BF16)) for t, p in zip(inverse, power)]
            span *= 2
        for small, large in zip(same[:-1], same[1:]):
            low = [t.astype(BF16) for t in inverse]
            step = [dot(jnp.where(large & ~small, l, 0.0).astype(BF16), t) for l, t in zip(lower, low)]
            inverse = [t - dot(b, s.astype(BF16)) for t, b, s in zip(inverse, low, step)]
        high = [split(t) for t in inverse]
        error = [eye - t - dot3(split(l), s) for t, l, s in zip(inverse, lower, high)]
        inverse = [t + dot(s[0], e.astype(BF16)) for t, s, e in zip(inverse, high, error)]
        solved = [dot(t.astype(BF16), rhs[i]).astype(BF16) for i, t in zip(at, inverse)]
        change = [dot(k[0], s, ((0,), (0,))) for k, s in zip(ks, solved)]
        qs = [queries[i] for i in at]
        attend = [jnp.where(seen, dot(q.astype(BF16), k[0], ((1,), (1,))), 0.0).astype(BF16) for q, k in zip(qs, ks)]
        effect = [dot(a, s) for a, s in zip(attend, solved)]
        for i, g, q, e in zip(at, change, qs, effect):
            state_map[i + (slice(0, CH),)] = (q - e[:, :DK]).astype(BF16)
            state_map[i + (slice(CH, CH + DK),)] = g[:, :DK].astype(BF16)
            added[i] = g[:, DK:]
            out_add[i] = e[:, DK:]

    states = [jnp.zeros((DK, DK), F32) for _ in range(heads)]
    for c in range(blocks):
        for h in range(heads):
            moved = dot(state_map[h, c], states[h].astype(BF16))
            out = moved[:CH] + out_add[h, c]
            states[h] = states[h] - moved[CH:] + added[h, c]
            out = out * lax.rsqrt(jnp.mean(out * out, -1, keepdims=True) + EPSILON) * head_gain_ref[...]
            mixed[c * CH:(c + 1) * CH, h * DK:(h + 1) * DK] = out.astype(BF16)
    own = length // count
    turned = jnp.concatenate([mixed[rows_at(lax.rem(me + k, count), own), :] for k in range(count)], 0)
    result = dot(turned, wo_ref[...]).astype(BF16)
    for k, o in enumerate((o0, o1, o2, o3)):
        o[...] = result[k * own:(k + 1) * own]


UNROLL = 8


def mixer(me, xs, gain, wq, wk, wv, wb, head_gain, wo):
    length, part = xs[0].shape
    heads = wq.shape[1] // DK
    blocks = length // CH
    own = length // len(xs)
    vmem = pl.BlockSpec(memory_space=pltpu.VMEM)
    return pl.pallas_call(
        lambda *refs: mixer_kernel(heads, *refs),
        out_shape=[jax.ShapeDtypeStruct((own, wo.shape[1]), BF16)] * len(xs),
        in_specs=[pl.BlockSpec(memory_space=pltpu.SMEM)] + [vmem] * 11,
        out_specs=[vmem] * len(xs),
        scratch_shapes=[
            pltpu.VMEM((len(xs), length, part), BF16),
            pltpu.VMEM((heads, blocks, SUB, DK), F32),
            pltpu.VMEM((heads, blocks, SUB, DK), F32),
            pltpu.VMEM((heads, blocks, SUB, 2 * DK), BF16),
            pltpu.VMEM((heads, blocks, CH, DK), F32),
            pltpu.VMEM((8, DK), F32),
            pltpu.VMEM((heads, blocks, CH + DK, DK), BF16),
            pltpu.VMEM((heads, blocks, DK, DK), F32),
            pltpu.VMEM((heads, blocks, CH, DK), F32),
            pltpu.VMEM((length, heads * DK), BF16),
        ],
        compiler_params=pltpu.CompilerParams(vmem_limit_bytes=32 * MIB),
        cost_estimate=pl.CostEstimate(flops=2 * 10 ** 10, bytes_accessed=10 ** 7, transcendentals=0),
        name="mixer",
    )(me, *xs, gain, wq, wk, wv, wb, head_gain, wo)


def slots(ids_ref, experts, capacity):
    tokens = ids_ref.shape[1]
    label = iota((experts, tokens), 0)
    chosen = [(label == ids_ref[k:k + 1, :]).astype(F32) for k in range(2)]
    count = chosen[0] + chosen[1]
    before = (iota((tokens, tokens), 0) < iota((tokens, tokens), 1)).astype(BF16)
    earlier = dot(count.astype(BF16), before)
    total = experts * capacity
    spread = (iota((total, experts), 0) // capacity == iota((total, experts), 1)).astype(BF16)
    place = dot(spread, earlier.astype(BF16))
    fits = place == (iota((total, tokens), 0) % capacity).astype(F32)
    return chosen, [jnp.where(fits, dot(spread, c.astype(BF16)), 0.0) for c in chosen]


def route_kernel(place_ref, p0, p1, p2, p3, x0, x1, x2, x3, gain_ref, ids_ref, residual_ref, routed_ref, send_ref):
    me = place_ref[0]
    xs = (x0, x1, x2, x3)
    count = len(xs)
    own, part = p0.shape[0], x0.shape[1]
    for k in range(count):
        columns = rows_at(lax.rem(me - k + count, count), part)
        residual_ref[:, columns] = xs[k][rows_at(me, own), :].astype(F32)
    arrived = [p[...].astype(F32) for p in (p0, p1, p2, p3)]
    residual = residual_ref[...] + ((arrived[0] + arrived[1]) + (arrived[2] + arrived[3]))
    residual_ref[...] = residual
    mean = jnp.mean(residual * residual, -1, keepdims=True)
    routed = residual * lax.rsqrt(mean + EPSILON) * gain_ref[...]
    routed_ref[...] = routed
    _, parts = slots(ids_ref, 64, send_ref.shape[0] // 64)
    chosen = (parts[0] + parts[1]).astype(BF16)
    send_ref[...] = dot(chosen, routed.astype(BF16)).astype(BF16)


def route(me, ps, xs, gain, ids, experts, capacity):
    own, width = ps[0].shape
    vmem = pl.BlockSpec(memory_space=pltpu.VMEM)
    return pl.pallas_call(
        route_kernel,
        out_shape=[
            jax.ShapeDtypeStruct((own, width), F32),
            jax.ShapeDtypeStruct((own, width), F32),
            jax.ShapeDtypeStruct((experts * capacity, width), BF16),
        ],
        in_specs=[pl.BlockSpec(memory_space=pltpu.SMEM)] + [vmem] * 10,
        out_specs=[vmem] * 3,
        compiler_params=pltpu.CompilerParams(vmem_limit_bytes=16 * MIB),
        cost_estimate=pl.CostEstimate(flops=10 ** 9, bytes_accessed=10 ** 7, transcendentals=0),
        name="route",
    )(me, *ps, *xs, gain, ids)


def weigh_kernel(routed_ref, router_ref, ids_ref, pick_ref, leading_ref):
    experts = router_ref.shape[0]
    chosen, parts = slots(ids_ref, experts, pick_ref.shape[1] // experts)
    tokens = routed_ref.shape[0]
    for k in range(2):
        pick_ref[k * tokens:(k + 1) * tokens, :] = jnp.transpose(parts[k]).astype(BF16)
    logits = lax.dot_general(
        router_ref[...], routed_ref[...], (((1,), (1,)), ((), ())),
        precision=lax.Precision.HIGHEST, preferred_element_type=F32,
    )
    gap = jnp.sum((chosen[0] - chosen[1]) * logits, 0, keepdims=True)
    leading = 1.0 / (1.0 + jnp.exp(-gap))
    leading_ref[...] = jnp.transpose(jnp.broadcast_to(leading, (128, tokens)))


def weigh(routed, router, ids, capacity):
    tokens = routed.shape[0]
    experts = router.shape[0]
    vmem = pl.BlockSpec(memory_space=pltpu.VMEM)
    return pl.pallas_call(
        weigh_kernel,
        out_shape=[
            jax.ShapeDtypeStruct((2 * tokens, experts * capacity), BF16),
            jax.ShapeDtypeStruct((tokens, 128), F32),
        ],
        in_specs=[vmem] * 3,
        out_specs=[vmem] * 2,
        compiler_params=pltpu.CompilerParams(vmem_limit_bytes=8 * MIB),
        cost_estimate=pl.CostEstimate(flops=10 ** 9, bytes_accessed=10 ** 6, transcendentals=0),
        name="weigh",
    )(routed, router, ids)


PIECES = 4


def load_kernel(*refs):
    half = (len(refs) - 1) // 2
    sems = refs[-1]
    copies = []
    for i in range(half):
        copies.append(pltpu.make_async_copy(refs[i], refs[half + i], sems.at[i]))
        copies[-1].start()
    for copy in copies:
        copy.wait()


def load(*weights):
    return pl.pallas_call(
        load_kernel,
        out_shape=[pltpu.VMEM(w.shape, w.dtype) for w in weights],
        in_specs=[pl.BlockSpec(memory_space=pltpu.HBM)] * len(weights),
        out_specs=[pl.BlockSpec(memory_space=pltpu.VMEM)] * len(weights),
        scratch_shapes=[pltpu.SemaphoreType.DMA((len(weights),))],
        compiler_params=pltpu.CompilerParams(vmem_limit_bytes=1 * MIB),
        cost_estimate=pl.CostEstimate(flops=2 * 10 ** 9, bytes_accessed=10 ** 6, transcendentals=0),
        name="load",
    )(*[pltpu.with_memory_space_constraint(w, pltpu.HBM) for w in weights])


def expert_kernel(rows_ref, gate_hbm, up_hbm, down_hbm, out_ref, gate_ref, up_ref, down_ref, sems):
    total = rows_ref.shape[0]
    here, width, middle = gate_hbm.shape
    per = total // here
    cap = 4
    deep, tall = width // PIECES, middle // PIECES
    copies = {}
    for e in range(here):
        for part, (source, target) in enumerate(((gate_hbm, gate_ref), (up_hbm, up_ref), (down_hbm, down_ref))):
            size = tall if part == 2 else deep
            for p in range(PIECES):
                at = (e, pl.ds(p * size, size))
                copies[e, part, p] = pltpu.make_async_copy(source.at[at], target.at[at], sems.at[e, part, p])
    for e in range(here):
        for p in range(PIECES):
            copies[e, 0, p].start()
            copies[e, 1, p].start()
        for p in range(PIECES):
            copies[e, 2, p].start()
    r, c = iota((total, total), 0), iota((total, total), 1)

    def source(i):
        return (i % per) // cap * (here * cap) + i // per * cap + i % cap

    by_expert = (source(r) == c).astype(BF16)
    by_source = (source(c) == r).astype(BF16)
    rows = dot(by_expert, rows_ref[...]).astype(BF16)
    results = []
    for e in range(here):
        mine = rows[e * per:(e + 1) * per]
        gate = up = 0.0
        for p in range(PIECES):
            at = slice(p * deep, (p + 1) * deep)
            copies[e, 0, p].wait()
            gate = gate + dot(mine[:, at], gate_ref[e, at])
            copies[e, 1, p].wait()
            up = up + dot(mine[:, at], up_ref[e, at])
        hidden = (gate / (1.0 + jnp.exp(-gate)) * up).astype(BF16)
        for p in range(PIECES):
            copies[e, 2, p].wait()
        results.append(dot(hidden, down_ref[e]).astype(BF16))
    out_ref[...] = dot(by_source, jnp.concatenate(results, 0)).astype(BF16)


def experts_here(rows, gate, up, down):
    vmem = pl.BlockSpec(memory_space=pltpu.VMEM)
    hbm = pl.BlockSpec(memory_space=pltpu.HBM)
    return pl.pallas_call(
        expert_kernel,
        out_shape=jax.ShapeDtypeStruct(rows.shape, BF16),
        in_specs=[vmem] + [hbm] * 3,
        out_specs=vmem,
        scratch_shapes=[
            pltpu.VMEM(gate.shape, BF16),
            pltpu.VMEM(up.shape, BF16),
            pltpu.VMEM(down.shape, BF16),
            pltpu.SemaphoreType.DMA((gate.shape[0], 3, PIECES)),
        ],
        compiler_params=pltpu.CompilerParams(vmem_limit_bytes=56 * MIB),
        cost_estimate=pl.CostEstimate(flops=5 * 10 ** 9, bytes_accessed=10 ** 7, transcendentals=0),
        name="experts",
    )(rows, *[pltpu.with_memory_space_constraint(w, pltpu.HBM) for w in (gate, up, down)])


def combine_kernel(residual_ref, leading_ref, pick_ref, back_ref, out_ref):
    tokens = residual_ref.shape[0]
    picked = dot(pick_ref[...], back_ref[...])
    leading = leading_ref[:, 0:1]
    blended = leading * picked[:tokens] + (1.0 - leading) * picked[tokens:]
    out_ref[...] = (residual_ref[...] + blended).astype(BF16)


def combine(residual, leading, pick, back):
    vmem = pl.BlockSpec(memory_space=pltpu.VMEM)
    return pl.pallas_call(
        combine_kernel,
        out_shape=jax.ShapeDtypeStruct(residual.shape, BF16),
        in_specs=[vmem] * 4,
        out_specs=vmem,
        compiler_params=pltpu.CompilerParams(vmem_limit_bytes=16 * MIB),
        cost_estimate=pl.CostEstimate(flops=10 ** 9, bytes_accessed=10 ** 6, transcendentals=0),
        name="combine",
    )(residual, leading, pick, back)


def turned(x, k, axis):
    size = lax.axis_size(axis)
    return lax.ppermute(x, axis, [(i, (i + k) % size) for i in range(size)])


def shards(tokens, mixer_gain, query_weight, key_weight, value_weight, beta_weight, head_gain, output_weight,
           expert_gain, router_weight, expert_ids, gate_weight, up_weight, down_weight):
    peers = lax.axis_size("head")
    owners = lax.axis_size("dp")
    me = lax.axis_index("head").reshape(1).astype(jnp.int32)
    xs = [tokens] + [turned(tokens, k, "head") for k in range(1, peers)]
    here = load(tokens, query_weight, key_weight, value_weight, beta_weight.T, head_gain.reshape(1, -1), output_weight)
    xs[0] = here[0]
    parts = mixer(me, xs, mixer_gain.reshape(peers, -1), *here[1:])
    parts = [parts[0]] + [turned(parts[k], k, "head") for k in range(1, peers)]
    experts = router_weight.shape[1]
    own = parts[0].shape[0]
    capacity = 4 * own // experts
    ids = expert_ids.T
    residual, routed, outgoing = route(me, parts, xs, expert_gain.reshape(1, -1), ids, experts, capacity)
    width = outgoing.shape[1]
    outgoing = outgoing.reshape(owners, -1, width)
    arrived = lax.all_to_all(outgoing, "dp", split_axis=0, concat_axis=0, tiled=True)
    pick, leading = weigh(routed, router_weight.T, ids, capacity)
    result = experts_here(arrived.reshape(-1, width), gate_weight, up_weight, down_weight)
    back = lax.all_to_all(result.reshape(owners, -1, width), "dp", split_axis=0, concat_axis=0, tiled=True)
    return combine(residual, leading, pick, back.reshape(-1, width))


def solution(mesh):
    return jax.shard_map(
        shards,
        mesh=mesh,
        in_specs=(
            P("dp", "head"),
            P(),
            P(None, "head"),
            P(None, None, "head"),
            P(None, None, "head"),
            P(None, "head"),
            P(),
            P("head", None),
            P(),
            P(),
            P(("dp", "head"), None),
            P("dp", None, None),
            P("dp", None, None),
            P("dp", None, None),
        ),
        out_specs=P(("dp", "head"), None),
        check_vma=False,
    )
```

```python
import jax
import jax.numpy as jnp
from jax import lax
from jax.experimental import pallas as pl
from jax.experimental.pallas import tpu as pltpu
from jax.sharding import PartitionSpec as P

DK = 128
NH = 3
CH = 32
SUB = CH * NH
BASE = 4
EPSILON = 1e-06
F32 = jnp.float32
BF16 = jnp.bfloat16
MIB = 1 << 20


def dot(a, b, dims=((1,), (0,))):
    return lax.dot_general(a, b, (dims, ((), ())), preferred_element_type=F32)


def split(a):
    high = a.astype(BF16)
    return high, (a - high.astype(F32)).astype(BF16)


def dot3(a, b, dims=((1,), (0,))):
    return dot(a[0], b[0], dims) + (dot(a[0], b[1], dims) + dot(a[1], b[0], dims))


def iota(shape, dim):
    return lax.broadcasted_iota(jnp.int32, shape, dim)


def rows_at(block, size):
    return pl.ds(pl.multiple_of(block * size, size), size)


def mixer_kernel(heads, place_ref, x0, x1, x2, x3, gain_ref, wq_ref, wk_ref, wv_ref, wb_ref, head_gain_ref,
                 wo_ref, out_ref, normed, keys, beta_keys, rhs, queries, reduced, state_map, added, out_add, mixed):
    me = place_ref[0]
    xs = (x0, x1, x2, x3)
    count = len(xs)
    length, part = x0.shape
    sources = [lax.rem(me - k + count, count) for k in range(count)]
    total = 0.0
    for x in xs:
        wide = x[...].astype(F32)
        total = total + jnp.sum(wide * wide, -1, keepdims=True)
    scale = lax.rsqrt(total / (count * part) + EPSILON)
    for k in range(count):
        gain = gain_ref[pl.ds(sources[k], 1), :]
        normed[k] = (xs[k][...].astype(F32) * scale * gain).astype(BF16)

    def project(weight):
        return sum(dot(normed[k], weight(rows_at(sources[k], part))) for k in range(count))

    beta = sum(
        dot(normed[k], wb_ref[:, rows_at(sources[k], part)], ((1,), (1,))) for k in range(count)
    )
    beta = 2.0 / (1.0 + jnp.exp(-beta))
    blocks = length // CH
    query = project(lambda r: wq_ref[r, :])
    for h in range(heads):
        q = query[:, h * DK:(h + 1) * DK]
        q = q * lax.rsqrt(jnp.sum(q * q, -1, keepdims=True) + EPSILON) * DK ** (-0.5)
        queries[h] = q.reshape(blocks, CH, DK)
    for m in range(NH):
        key = project(lambda r: wk_ref[m, r, :])
        value = project(lambda r: wv_ref[m, r, :])
        for h in range(heads):
            b = beta[:, h * NH + m:h * NH + m + 1]
            k = key[:, h * DK:(h + 1) * DK]
            k = k * lax.rsqrt(jnp.sum(k * k, -1, keepdims=True) + EPSILON)
            keys[h, :, m * CH:(m + 1) * CH, :] = k.reshape(blocks, CH, DK)
            rhs[h, :, m * CH:(m + 1) * CH, :DK] = (k * b).astype(BF16).reshape(blocks, CH, DK)
            rhs[h, :, m * CH:(m + 1) * CH, DK:] = (value[:, h * DK:(h + 1) * DK] * b).astype(BF16).reshape(blocks, CH, DK)
            beta_keys[h, :, m * CH:(m + 1) * CH, :] = jnp.broadcast_to(b, (length, DK)).reshape(blocks, CH, DK)

    row, col = iota((SUB, SUB), 0), iota((SUB, SUB), 1)
    row_t, col_t = row % CH, col % CH
    causal = (col_t < row_t) | ((col_t == row_t) & (col < row))
    same = [row_t // s == col_t // s for s in (BASE, BASE * 2, BASE * 4, BASE * 8)]
    eye = (row == col).astype(F32)
    seen = iota((CH, SUB), 1) % CH <= iota((CH, SUB), 0)

    unroll = UNROLL
    for start in range(0, blocks, unroll):
        at = [(h, c) for c in range(start, start + unroll) for h in range(heads)]
        ks = [split(keys[i]) for i in at]
        lower = [
            jnp.where(causal, dot3(k, k, ((1,), (1,))) * beta_keys[i][:, :SUB], 0.0) for i, k in zip(at, ks)
        ]
        power = [jnp.where(same[0], -l, 0.0) for l in lower]
        inverse = [eye + p for p in power]
        span = 2
        while span < BASE * NH:
            power = [p.astype(BF16) for p in power]
            power = [dot(p, p) for p in power]
            inverse = [t + dot(t.astype(BF16), p.astype(BF16)) for t, p in zip(inverse, power)]
            span *= 2
        for small, large in zip(same[:-1], same[1:]):
            low = [t.astype(BF16) for t in inverse]
            step = [dot(jnp.where(large & ~small, l, 0.0).astype(BF16), t) for l, t in zip(lower, low)]
            inverse = [t - dot(b, s.astype(BF16)) for t, b, s in zip(inverse, low, step)]
        high = [split(t) for t in inverse]
        error = [eye - t - dot3(split(l), s) for t, l, s in zip(inverse, lower, high)]
        inverse = [t + dot(s[0], e.astype(BF16)) for t, s, e in zip(inverse, high, error)]
        solved = [dot(t.astype(BF16), rhs[i]).astype(BF16) for i, t in zip(at, inverse)]
        change = [dot(k[0], s, ((0,), (0,))) for k, s in zip(ks, solved)]
        qs = [queries[i] for i in at]
        attend = [jnp.where(seen, dot(q.astype(BF16), k[0], ((1,), (1,))), 0.0).astype(BF16) for q, k in zip(qs, ks)]
        effect = [dot(a, s) for a, s in zip(attend, solved)]
        for i, g, q, e in zip(at, change, qs, effect):
            state_map[i + (slice(0, CH),)] = (q - e[:, :DK]).astype(BF16)
            state_map[i + (slice(CH, CH + DK),)] = g[:, :DK].astype(BF16)
            added[i] = g[:, DK:]
            out_add[i] = e[:, DK:]

    states = [jnp.zeros((DK, DK), F32) for _ in range(heads)]
    for c in range(blocks):
        for h in range(heads):
            moved = dot(state_map[h, c], states[h].astype(BF16))
            out = moved[:CH] + out_add[h, c]
            states[h] = states[h] - moved[CH:] + added[h, c]
            out = out * lax.rsqrt(jnp.mean(out * out, -1, keepdims=True) + EPSILON) * head_gain_ref[...]
            mixed[c * CH:(c + 1) * CH, h * DK:(h + 1) * DK] = out.astype(BF16)
    out_ref[...] = dot(mixed[...], wo_ref[...]).astype(BF16)


UNROLL = 8


def mixer(me, xs, gain, wq, wk, wv, wb, head_gain, wo):
    length, part = xs[0].shape
    heads = wq.shape[1] // DK
    blocks = length // CH
    vmem = pl.BlockSpec(memory_space=pltpu.VMEM)
    return pl.pallas_call(
        lambda *refs: mixer_kernel(heads, *refs),
        out_shape=jax.ShapeDtypeStruct((length, wo.shape[1]), BF16),
        in_specs=[pl.BlockSpec(memory_space=pltpu.SMEM)] + [vmem] * 11,
        out_specs=vmem,
        scratch_shapes=[
            pltpu.VMEM((len(xs), length, part), BF16),
            pltpu.VMEM((heads, blocks, SUB, DK), F32),
            pltpu.VMEM((heads, blocks, SUB, DK), F32),
            pltpu.VMEM((heads, blocks, SUB, 2 * DK), BF16),
            pltpu.VMEM((heads, blocks, CH, DK), F32),
            pltpu.VMEM((8, DK), F32),
            pltpu.VMEM((heads, blocks, CH + DK, DK), BF16),
            pltpu.VMEM((heads, blocks, DK, DK), F32),
            pltpu.VMEM((heads, blocks, CH, DK), F32),
            pltpu.VMEM((length, heads * DK), BF16),
        ],
        compiler_params=pltpu.CompilerParams(vmem_limit_bytes=32 * MIB),
        cost_estimate=pl.CostEstimate(flops=2 * 10 ** 10, bytes_accessed=10 ** 7, transcendentals=0),
        name="mixer",
    )(me, *xs, gain, wq, wk, wv, wb, head_gain, wo)


def slots(ids_ref, experts, capacity):
    tokens = ids_ref.shape[1]
    label = iota((experts, tokens), 0)
    chosen = [(label == ids_ref[k:k + 1, :]).astype(F32) for k in range(2)]
    count = chosen[0] + chosen[1]
    before = (iota((tokens, tokens), 0) < iota((tokens, tokens), 1)).astype(BF16)
    earlier = dot(count.astype(BF16), before)
    total = experts * capacity
    spread = (iota((total, experts), 0) // capacity == iota((total, experts), 1)).astype(BF16)
    place = dot(spread, earlier.astype(BF16))
    fits = place == (iota((total, tokens), 0) % capacity).astype(F32)
    return chosen, [jnp.where(fits, dot(spread, c.astype(BF16)), 0.0) for c in chosen]


def route_kernel(place_ref, parts_ref, x0, x1, x2, x3, gain_ref, ids_ref, residual_ref, routed_ref, send_ref):
    me = place_ref[0]
    xs = (x0, x1, x2, x3)
    count = len(xs)
    own, part = parts_ref.shape[1], x0.shape[1]
    for k in range(count):
        columns = rows_at(lax.rem(me - k + count, count), part)
        residual_ref[:, columns] = xs[k][rows_at(me, own), :].astype(F32)
    arrived = [parts_ref[k].astype(F32) for k in range(count)]
    residual = residual_ref[...] + ((arrived[0] + arrived[1]) + (arrived[2] + arrived[3]))
    residual_ref[...] = residual
    mean = jnp.mean(residual * residual, -1, keepdims=True)
    routed = residual * lax.rsqrt(mean + EPSILON) * gain_ref[...]
    routed_ref[...] = routed
    _, chosen = slots(ids_ref, 64, send_ref.shape[0] // 64)
    chosen = (chosen[0] + chosen[1]).astype(BF16)
    send_ref[...] = dot(chosen, routed.astype(BF16)).astype(BF16)


def route(me, parts, xs, gain, ids, experts, capacity):
    _, own, width = parts.shape
    vmem = pl.BlockSpec(memory_space=pltpu.VMEM)
    return pl.pallas_call(
        route_kernel,
        out_shape=[
            jax.ShapeDtypeStruct((own, width), F32),
            jax.ShapeDtypeStruct((own, width), F32),
            jax.ShapeDtypeStruct((experts * capacity, width), BF16),
        ],
        in_specs=[pl.BlockSpec(memory_space=pltpu.SMEM)] + [vmem] * 7,
        out_specs=[vmem] * 3,
        compiler_params=pltpu.CompilerParams(vmem_limit_bytes=16 * MIB),
        cost_estimate=pl.CostEstimate(flops=10 ** 9, bytes_accessed=10 ** 7, transcendentals=0),
        name="route",
    )(me, parts, *xs, gain, ids)


def weigh(routed_ref, router_ref, ids_ref, pick_ref, leading_ref):
    experts = router_ref.shape[0]
    chosen, parts = slots(ids_ref, experts, pick_ref.shape[1] // experts)
    tokens = routed_ref.shape[0]
    for k in range(2):
        pick_ref[k * tokens:(k + 1) * tokens, :] = jnp.transpose(parts[k]).astype(BF16)
    logits = lax.dot_general(
        router_ref[...], routed_ref[...], (((1,), (1,)), ((), ())),
        precision=lax.Precision.HIGHEST, preferred_element_type=F32,
    )
    gap = jnp.sum((chosen[0] - chosen[1]) * logits, 0, keepdims=True)
    leading = 1.0 / (1.0 + jnp.exp(-gap))
    leading_ref[...] = jnp.transpose(jnp.broadcast_to(leading, (128, tokens)))


def load_kernel(*refs):
    half = (len(refs) - 1) // 2
    sems = refs[-1]
    copies = []
    for i in range(half):
        copies.append(pltpu.make_async_copy(refs[i], refs[half + i], sems.at[i]))
        copies[-1].start()
    for copy in copies:
        copy.wait()


def load(*weights):
    return pl.pallas_call(
        load_kernel,
        out_shape=[pltpu.VMEM(w.shape, w.dtype) for w in weights],
        in_specs=[pl.BlockSpec(memory_space=pltpu.HBM)] * len(weights),
        out_specs=[pl.BlockSpec(memory_space=pltpu.VMEM)] * len(weights),
        scratch_shapes=[pltpu.SemaphoreType.DMA((len(weights),))],
        compiler_params=pltpu.CompilerParams(vmem_limit_bytes=1 * MIB),
        cost_estimate=pl.CostEstimate(flops=2 * 10 ** 9, bytes_accessed=10 ** 6, transcendentals=0),
        name="load",
    )(*[pltpu.with_memory_space_constraint(w, pltpu.HBM) for w in weights])


def expert_kernel(rows_ref, gate_hbm, up_hbm, down_hbm, routed_ref, router_ref, ids_ref, out_ref, pick_ref, leading_ref,
                  gate_ref, up_ref, down_ref, hidden_ref, finished_ref, sems):
    total = rows_ref.shape[0]
    here, width, middle = gate_hbm.shape
    per = total // here
    experts = router_ref.shape[0]
    cap = pick_ref.shape[1] // experts
    deep, tall = width // PIECES, middle // PIECES
    copies, order = {}, []
    for e in range(here):
        for part, (source, target) in enumerate(((gate_hbm, gate_ref), (up_hbm, up_ref), (down_hbm, down_ref))):
            size = tall if part == 2 else deep
            for p in range(PIECES):
                at = (e, pl.ds(p * size, size))
                copies[e, part, p] = pltpu.make_async_copy(source.at[at], target.at[at], sems.at[e, part, p])
        for p in range(PIECES):
            order += [(e, 0, p), (e, 1, p)]
        order += [(e, 2, p) for p in range(PIECES)]
    for key in order[:FLIGHT]:
        copies[key].start()

    def take(*key):
        copies[key].wait()
        following = order.index(key) + FLIGHT
        if following < len(order):
            copies[order[following]].start()

    weigh(routed_ref, router_ref, ids_ref, pick_ref, leading_ref)
    r, c = iota((total, total), 0), iota((total, total), 1)

    def source(i):
        return (i % per) // cap * (here * cap) + i // per * cap + i % cap

    by_expert = (source(r) == c).astype(BF16)
    by_source = (source(c) == r).astype(BF16)
    rows = dot(by_expert, rows_ref[...]).astype(BF16)
    for e in range(here):
        mine = rows[e * per:(e + 1) * per]
        gate = up = 0.0
        for p in range(PIECES):
            at = slice(p * deep, (p + 1) * deep)
            take(e, 0, p)
            gate = gate + dot(mine[:, at], gate_ref[e, at])
            take(e, 1, p)
            up = up + dot(mine[:, at], up_ref[e, at])
        hidden_ref[...] = (gate / (1.0 + jnp.exp(-gate)) * up).astype(BF16)
        result = 0.0
        for p in range(PIECES):
            take(e, 2, p)
            at = slice(p * tall, (p + 1) * tall)
            result = result + dot(hidden_ref[:, at], down_ref[e, at])
        finished_ref[e * per:(e + 1) * per, :] = result.astype(BF16)
    for start in range(0, width, 512):
        at = slice(start, start + 512)
        out_ref[:, at] = dot(by_source, finished_ref[:, at]).astype(BF16)


PIECES = 4
FLIGHT = 10


def experts_here(rows, gate, up, down, routed, router, ids):
    here, width, middle = gate.shape
    per = rows.shape[0] // here
    tokens, experts = routed.shape[0], router.shape[0]
    capacity = 4 * tokens // experts
    vmem = pl.BlockSpec(memory_space=pltpu.VMEM)
    hbm = pl.BlockSpec(memory_space=pltpu.HBM)
    return pl.pallas_call(
        expert_kernel,
        out_shape=[
            jax.ShapeDtypeStruct(rows.shape, BF16),
            jax.ShapeDtypeStruct((2 * tokens, experts * capacity), BF16),
            jax.ShapeDtypeStruct((tokens, 128), F32),
        ],
        in_specs=[vmem] + [hbm] * 3 + [vmem] * 3,
        out_specs=[vmem] * 3,
        scratch_shapes=[
            pltpu.VMEM(gate.shape, BF16),
            pltpu.VMEM(up.shape, BF16),
            pltpu.VMEM(down.shape, BF16),
            pltpu.VMEM((per, middle), BF16),
            pltpu.VMEM(rows.shape, BF16),
            pltpu.SemaphoreType.DMA((here, 3, PIECES)),
        ],
        compiler_params=pltpu.CompilerParams(vmem_limit_bytes=46 * MIB),
        cost_estimate=pl.CostEstimate(flops=5 * 10 ** 9, bytes_accessed=10 ** 7, transcendentals=0),
        name="experts",
    )(rows, *[pltpu.with_memory_space_constraint(w, pltpu.HBM) for w in (gate, up, down)], routed, router, ids)


def combine_kernel(residual_ref, leading_ref, pick_ref, back_ref, out_ref):
    tokens = residual_ref.shape[0]
    picked = dot(pick_ref[...], back_ref[...])
    leading = leading_ref[:, 0:1]
    blended = leading * picked[:tokens] + (1.0 - leading) * picked[tokens:]
    out_ref[...] = (residual_ref[...] + blended).astype(BF16)


def combine(residual, leading, pick, back):
    vmem = pl.BlockSpec(memory_space=pltpu.VMEM)
    return pl.pallas_call(
        combine_kernel,
        out_shape=jax.ShapeDtypeStruct(residual.shape, BF16),
        in_specs=[vmem] * 4,
        out_specs=vmem,
        compiler_params=pltpu.CompilerParams(vmem_limit_bytes=16 * MIB),
        cost_estimate=pl.CostEstimate(flops=10 ** 9, bytes_accessed=10 ** 6, transcendentals=0),
        name="combine",
    )(residual, leading, pick, back)


def turned(x, k, axis):
    size = lax.axis_size(axis)
    return lax.ppermute(x, axis, [(i, (i + k) % size) for i in range(size)])


def shards(tokens, mixer_gain, query_weight, key_weight, value_weight, beta_weight, head_gain, output_weight,
           expert_gain, router_weight, expert_ids, gate_weight, up_weight, down_weight):
    peers = lax.axis_size("head")
    owners = lax.axis_size("dp")
    me = lax.axis_index("head").reshape(1).astype(jnp.int32)
    xs = [tokens] + [turned(tokens, k, "head") for k in range(1, peers)]
    here = load(tokens, query_weight, key_weight, value_weight, beta_weight.T, head_gain.reshape(1, -1), output_weight)
    xs[0] = here[0]
    parts = mixer(me, xs, mixer_gain.reshape(peers, -1), *here[1:])
    parts = parts.reshape(peers, -1, parts.shape[1])
    parts = lax.all_to_all(parts, "head", split_axis=0, concat_axis=0, tiled=True)
    experts = router_weight.shape[1]
    own = parts.shape[1]
    capacity = 4 * own // experts
    ids = expert_ids.T
    residual, routed, outgoing = route(me, parts, xs, expert_gain.reshape(1, -1), ids, experts, capacity)
    width = outgoing.shape[1]
    outgoing = outgoing.reshape(owners, -1, width)
    arrived = lax.all_to_all(outgoing, "dp", split_axis=0, concat_axis=0, tiled=True)
    result, pick, leading = experts_here(
        arrived.reshape(-1, width), gate_weight, up_weight, down_weight, routed, router_weight.T, ids
    )
    back = lax.all_to_all(result.reshape(owners, -1, width), "dp", split_axis=0, concat_axis=0, tiled=True)
    return combine(residual, leading, pick, back.reshape(-1, width))


def solution(mesh):
    return jax.shard_map(
        shards,
        mesh=mesh,
        in_specs=(
            P("dp", "head"),
            P(),
            P(None, "head"),
            P(None, None, "head"),
            P(None, None, "head"),
            P(None, "head"),
            P(),
            P("head", None),
            P(),
            P(),
            P(("dp", "head"), None),
            P("dp", None, None),
            P("dp", None, None),
            P("dp", None, None),
        ),
        out_specs=P(("dp", "head"), None),
        check_vma=False,
    )
```

```python
import jax
import jax.numpy as jnp
from jax import lax
from jax.experimental import pallas as pl
from jax.experimental.pallas import tpu as pltpu
from jax.sharding import PartitionSpec as P

DK = 128
NH = 3
CH = 32
SUB = CH * NH
BASE = 4
EPSILON = 1e-06
F32 = jnp.float32
BF16 = jnp.bfloat16
MIB = 1 << 20


def dot(a, b, dims=((1,), (0,))):
    return lax.dot_general(a, b, (dims, ((), ())), preferred_element_type=F32)


def split(a):
    high = a.astype(BF16)
    return high, (a - high.astype(F32)).astype(BF16)


def dot3(a, b, dims=((1,), (0,))):
    return dot(a[0], b[0], dims) + (dot(a[0], b[1], dims) + dot(a[1], b[0], dims))


def iota(shape, dim):
    return lax.broadcasted_iota(jnp.int32, shape, dim)


def rows_at(block, size):
    return pl.ds(pl.multiple_of(block * size, size), size)


def gained(x_ref, gain_ref, source):
    wide = x_ref[...].astype(F32)
    return (wide * gain_ref[pl.ds(source, 1), :]).astype(BF16), jnp.sum(wide * wide, -1, keepdims=True)


def products(x, source, wq_ref, wk_ref, wv_ref, wb_ref):
    rows = rows_at(source, x.shape[1])
    yield dot(x, wq_ref[rows, :])
    for ref in (wk_ref, wv_ref):
        for m in range(NH):
            yield dot(x, ref[m, rows, :])
    yield dot(x, wb_ref[:, rows], ((1,), (1,)))


def first_kernel(place_ref, gain_ref, *refs):
    count = (len(refs) - 4) // 2
    here, there = refs[:count], refs[count:2 * count]
    sums_ref, beta_ref, square_ref, sems = refs[2 * count:]
    copies = [pltpu.make_async_copy(h, t, sems.at[i]) for i, (h, t) in enumerate(zip(here, there))]
    for copy in copies:
        copy.start()
    for copy in copies:
        copy.wait()
    x, square_ref[...] = gained(there[0], gain_ref, place_ref[0])
    for i, product in enumerate(products(x, place_ref[0], *there[1:5])):
        if i < 1 + 2 * NH:
            sums_ref[i] = product
        else:
            beta_ref[...] = product


def first(me, gain, tokens, wq, wk, wv, wb, *others):
    moved = (tokens, wq, wk, wv, wb, *others)
    length = tokens.shape[0]
    vmem = pl.BlockSpec(memory_space=pltpu.VMEM)
    made = [
        pltpu.VMEM((1 + 2 * NH, length, wq.shape[1]), F32),
        pltpu.VMEM((length, wb.shape[0]), F32),
        pltpu.VMEM((length, 1), F32),
    ]
    return pl.pallas_call(
        first_kernel,
        out_shape=[pltpu.VMEM(w.shape, w.dtype) for w in moved] + made,
        in_specs=[pl.BlockSpec(memory_space=pltpu.SMEM), vmem] + [pl.BlockSpec(memory_space=pltpu.HBM)] * len(moved),
        out_specs=[vmem] * (len(moved) + 3),
        scratch_shapes=[pltpu.SemaphoreType.DMA((len(moved),))],
        compiler_params=pltpu.CompilerParams(vmem_limit_bytes=4 * MIB),
        cost_estimate=pl.CostEstimate(flops=2 * 10 ** 9, bytes_accessed=10 ** 6, transcendentals=0),
        name="first",
    )(me, gain, *[pltpu.with_memory_space_constraint(w, pltpu.HBM) for w in moved])


def more_kernel(shift, place_ref, gain_ref, x_ref, wq_ref, wk_ref, wv_ref, wb_ref, sums_ref, beta_ref, square_ref,
                new_sums_ref, new_beta_ref, new_square_ref):
    source = (place_ref[0] + (gain_ref.shape[0] - shift)) % gain_ref.shape[0]
    x, square = gained(x_ref, gain_ref, source)
    new_square_ref[...] = square_ref[...] + square
    for i, product in enumerate(products(x, source, wq_ref, wk_ref, wv_ref, wb_ref)):
        if i < 1 + 2 * NH:
            new_sums_ref[i] = sums_ref[i] + product
        else:
            new_beta_ref[...] = beta_ref[...] + product


def more(shift, me, gain, x, weights, sums):
    vmem = pl.BlockSpec(memory_space=pltpu.VMEM)
    return pl.pallas_call(
        lambda *refs: more_kernel(shift, *refs),
        out_shape=[pltpu.VMEM(a.shape, a.dtype) for a in sums],
        in_specs=[pl.BlockSpec(memory_space=pltpu.SMEM)] + [vmem] * 9,
        out_specs=[vmem] * 3,
        input_output_aliases={7: 0, 8: 1, 9: 2},
        compiler_params=pltpu.CompilerParams(vmem_limit_bytes=4 * MIB),
        cost_estimate=pl.CostEstimate(flops=10 ** 9, bytes_accessed=10 ** 6, transcendentals=0),
        name="more",
    )(me, gain, x, *weights, *sums)


def mixer_kernel(heads, shift, place_ref, gain_ref, x_ref, wq_ref, wk_ref, wv_ref, wb_ref, sums_ref, beta_ref, square_ref,
                 head_gain_ref, wo_ref, o0, o1, o2, o3, keys, beta_keys, rhs, queries, state_map, added, out_add, mixed):
    me = place_ref[0]
    count, part = gain_ref.shape
    length = x_ref.shape[0]
    source = lax.rem(me + (count - shift), count)
    x, square = gained(x_ref, gain_ref, source)
    scale = lax.rsqrt((square_ref[...] + square) / (count * part) + EPSILON)
    last = products(x, source, wq_ref, wk_ref, wv_ref, wb_ref)
    whole = [(sums_ref[i] + next(last)) * scale for i in range(1 + 2 * NH)]
    beta = (beta_ref[...] + next(last)) * scale
    beta = 2.0 / (1.0 + jnp.exp(-beta))
    blocks = length // CH
    query = whole[0]
    for h in range(heads):
        q = query[:, h * DK:(h + 1) * DK]
        q = q * lax.rsqrt(jnp.sum(q * q, -1, keepdims=True) + EPSILON) * DK ** (-0.5)
        queries[h] = q.reshape(blocks, CH, DK)
    for m in range(NH):
        key = whole[1 + m]
        value = whole[1 + NH + m]
        for h in range(heads):
            b = beta[:, h * NH + m:h * NH + m + 1]
            k = key[:, h * DK:(h + 1) * DK]
            k = k * lax.rsqrt(jnp.sum(k * k, -1, keepdims=True) + EPSILON)
            keys[h, :, m * CH:(m + 1) * CH, :] = k.reshape(blocks, CH, DK)
            rhs[h, :, m * CH:(m + 1) * CH, :DK] = (k * b).astype(BF16).reshape(blocks, CH, DK)
            rhs[h, :, m * CH:(m + 1) * CH, DK:] = (value[:, h * DK:(h + 1) * DK] * b).astype(BF16).reshape(blocks, CH, DK)
            beta_keys[h, :, m * CH:(m + 1) * CH, :] = jnp.broadcast_to(b, (length, DK)).reshape(blocks, CH, DK)

    row, col = iota((SUB, SUB), 0), iota((SUB, SUB), 1)
    row_t, col_t = row % CH, col % CH
    causal = (col_t < row_t) | ((col_t == row_t) & (col < row))
    same = [row_t // s == col_t // s for s in (BASE, BASE * 2, BASE * 4, BASE * 8)]
    eye = (row == col).astype(F32)
    seen = iota((CH, SUB), 1) % CH <= iota((CH, SUB), 0)

    unroll = UNROLL
    for start in range(0, blocks, unroll):
        at = [(h, c) for c in range(start, start + unroll) for h in range(heads)]
        ks = [split(keys[i]) for i in at]
        lower = [
            jnp.where(causal, dot3(k, k, ((1,), (1,))) * beta_keys[i][:, :SUB], 0.0) for i, k in zip(at, ks)
        ]
        power = [jnp.where(same[0], -l, 0.0) for l in lower]
        inverse = [eye + p for p in power]
        span = 2
        while span < BASE * NH:
            power = [p.astype(BF16) for p in power]
            power = [dot(p, p) for p in power]
            inverse = [t + dot(t.astype(BF16), p.astype(BF16)) for t, p in zip(inverse, power)]
            span *= 2
        for small, large in zip(same[:-1], same[1:]):
            low = [t.astype(BF16) for t in inverse]
            step = [dot(jnp.where(large & ~small, l, 0.0).astype(BF16), t) for l, t in zip(lower, low)]
            inverse = [t - dot(b, s.astype(BF16)) for t, b, s in zip(inverse, low, step)]
        high = [split(t) for t in inverse]
        error = [eye - t - dot3(split(l), s) for t, l, s in zip(inverse, lower, high)]
        inverse = [t + dot(s[0], e.astype(BF16)) for t, s, e in zip(inverse, high, error)]
        solved = [dot(t.astype(BF16), rhs[i]).astype(BF16) for i, t in zip(at, inverse)]
        change = [dot(k[0], s, ((0,), (0,))) for k, s in zip(ks, solved)]
        qs = [queries[i] for i in at]
        attend = [jnp.where(seen, dot(q.astype(BF16), k[0], ((1,), (1,))), 0.0).astype(BF16) for q, k in zip(qs, ks)]
        effect = [dot(a, s) for a, s in zip(attend, solved)]
        for i, g, q, e in zip(at, change, qs, effect):
            state_map[i + (slice(0, CH),)] = (q - e[:, :DK]).astype(BF16)
            state_map[i + (slice(CH, CH + DK),)] = g[:, :DK].astype(BF16)
            added[i] = g[:, DK:]
            out_add[i] = e[:, DK:]

    states = [jnp.zeros((DK, DK), F32) for _ in range(heads)]
    for c in range(blocks):
        for h in range(heads):
            moved = dot(state_map[h, c], states[h].astype(BF16))
            out = moved[:CH] + out_add[h, c]
            states[h] = states[h] - moved[CH:] + added[h, c]
            out = out * lax.rsqrt(jnp.mean(out * out, -1, keepdims=True) + EPSILON) * head_gain_ref[...]
            mixed[c * CH:(c + 1) * CH, h * DK:(h + 1) * DK] = out.astype(BF16)
    own = length // count
    rolled = jnp.concatenate([mixed[rows_at(lax.rem(me + k, count), own), :] for k in range(count)], 0)
    result = dot(rolled, wo_ref[...]).astype(BF16)
    for k, o in enumerate((o0, o1, o2, o3)):
        o[...] = result[k * own:(k + 1) * own]


UNROLL = 8


def mixer(me, gain, x, shift, weights, sums, head_gain, wo):
    count = gain.shape[0]
    length = x.shape[0]
    heads = weights[0].shape[1] // DK
    blocks = length // CH
    own = length // count
    vmem = pl.BlockSpec(memory_space=pltpu.VMEM)
    return pl.pallas_call(
        lambda *refs: mixer_kernel(heads, shift, *refs),
        out_shape=[jax.ShapeDtypeStruct((own, wo.shape[1]), BF16)] * count,
        in_specs=[pl.BlockSpec(memory_space=pltpu.SMEM)] + [vmem] * 11,
        out_specs=[vmem] * count,
        scratch_shapes=[
            pltpu.VMEM((heads, blocks, SUB, DK), F32),
            pltpu.VMEM((heads, blocks, SUB, DK), F32),
            pltpu.VMEM((heads, blocks, SUB, 2 * DK), BF16),
            pltpu.VMEM((heads, blocks, CH, DK), F32),
            pltpu.VMEM((heads, blocks, CH + DK, DK), BF16),
            pltpu.VMEM((heads, blocks, DK, DK), F32),
            pltpu.VMEM((heads, blocks, CH, DK), F32),
            pltpu.VMEM((length, heads * DK), BF16),
        ],
        compiler_params=pltpu.CompilerParams(vmem_limit_bytes=32 * MIB),
        cost_estimate=pl.CostEstimate(flops=2 * 10 ** 10, bytes_accessed=10 ** 7, transcendentals=0),
        name="mixer",
    )(me, gain, x, *weights, *sums, head_gain, wo)


def slots(ids_ref, experts, capacity):
    tokens = ids_ref.shape[1]
    label = iota((experts, tokens), 0)
    chosen = [(label == ids_ref[k:k + 1, :]).astype(F32) for k in range(2)]
    count = chosen[0] + chosen[1]
    before = (iota((tokens, tokens), 0) < iota((tokens, tokens), 1)).astype(BF16)
    earlier = dot(count.astype(BF16), before)
    total = experts * capacity
    spread = (iota((total, experts), 0) // capacity == iota((total, experts), 1)).astype(BF16)
    place = dot(spread, earlier.astype(BF16))
    fits = place == (iota((total, tokens), 0) % capacity).astype(F32)
    return chosen, [jnp.where(fits, dot(spread, c.astype(BF16)), 0.0) for c in chosen]


def route_kernel(place_ref, p0, p1, p2, p3, x0, x1, x2, x3, gain_ref, ids_ref, residual_ref, routed_ref, send_ref):
    me = place_ref[0]
    xs = (x0, x1, x2, x3)
    count = len(xs)
    own, part = p0.shape[0], x0.shape[1]
    for k in range(count):
        columns = rows_at(lax.rem(me - k + count, count), part)
        residual_ref[:, columns] = xs[k][rows_at(me, own), :].astype(F32)
    arrived = [p[...].astype(F32) for p in (p0, p1, p2, p3)]
    residual = residual_ref[...] + ((arrived[0] + arrived[1]) + (arrived[2] + arrived[3]))
    residual_ref[...] = residual
    mean = jnp.mean(residual * residual, -1, keepdims=True)
    routed = residual * lax.rsqrt(mean + EPSILON) * gain_ref[...]
    routed_ref[...] = routed
    _, chosen = slots(ids_ref, 64, send_ref.shape[0] // 64)
    chosen = (chosen[0] + chosen[1]).astype(BF16)
    send_ref[...] = dot(chosen, routed.astype(BF16)).astype(BF16)


def route(me, parts, xs, gain, ids, experts, capacity):
    own, width = parts[0].shape
    vmem = pl.BlockSpec(memory_space=pltpu.VMEM)
    return pl.pallas_call(
        route_kernel,
        out_shape=[
            jax.ShapeDtypeStruct((own, width), F32),
            jax.ShapeDtypeStruct((own, width), F32),
            jax.ShapeDtypeStruct((experts * capacity, width), BF16),
        ],
        in_specs=[pl.BlockSpec(memory_space=pltpu.SMEM)] + [vmem] * 10,
        out_specs=[vmem] * 3,
        compiler_params=pltpu.CompilerParams(vmem_limit_bytes=16 * MIB),
        cost_estimate=pl.CostEstimate(flops=10 ** 9, bytes_accessed=10 ** 7, transcendentals=0),
        name="route",
    )(me, *parts, *xs, gain, ids)


def weigh(routed_ref, router_ref, ids_ref, pick_ref, leading_ref):
    experts = router_ref.shape[0]
    chosen, parts = slots(ids_ref, experts, pick_ref.shape[1] // experts)
    tokens = routed_ref.shape[0]
    for k in range(2):
        pick_ref[k * tokens:(k + 1) * tokens, :] = jnp.transpose(parts[k]).astype(BF16)
    logits = lax.dot_general(
        router_ref[...], routed_ref[...], (((1,), (1,)), ((), ())),
        precision=lax.Precision.HIGHEST, preferred_element_type=F32,
    )
    gap = jnp.sum((chosen[0] - chosen[1]) * logits, 0, keepdims=True)
    leading = 1.0 / (1.0 + jnp.exp(-gap))
    leading_ref[...] = jnp.transpose(jnp.broadcast_to(leading, (128, tokens)))


def expert_kernel(rows_ref, gate_hbm, up_hbm, down_hbm, routed_ref, router_ref, ids_ref, out_ref, pick_ref, leading_ref,
                  gate_ref, up_ref, down_ref, hidden_ref, finished_ref, sems):
    total = rows_ref.shape[0]
    here, width, middle = gate_hbm.shape
    per = total // here
    experts = router_ref.shape[0]
    cap = pick_ref.shape[1] // experts
    deep, tall = width // PIECES, middle // PIECES
    copies, order = {}, []
    for e in range(here):
        for part, (source, target) in enumerate(((gate_hbm, gate_ref), (up_hbm, up_ref), (down_hbm, down_ref))):
            size = tall if part == 2 else deep
            for p in range(PIECES):
                at = (e, pl.ds(p * size, size))
                copies[e, part, p] = pltpu.make_async_copy(source.at[at], target.at[at], sems.at[e, part, p])
        for p in range(PIECES):
            order += [(e, 0, p), (e, 1, p)]
        order += [(e, 2, p) for p in range(PIECES)]
    for key in order[:FLIGHT]:
        copies[key].start()

    def take(*key):
        copies[key].wait()
        following = order.index(key) + FLIGHT
        if following < len(order):
            copies[order[following]].start()

    weigh(routed_ref, router_ref, ids_ref, pick_ref, leading_ref)
    r, c = iota((total, total), 0), iota((total, total), 1)

    def source(i):
        return (i % per) // cap * (here * cap) + i // per * cap + i % cap

    by_expert = (source(r) == c).astype(BF16)
    by_source = (source(c) == r).astype(BF16)
    rows = dot(by_expert, rows_ref[...]).astype(BF16)
    for e in range(here):
        mine = rows[e * per:(e + 1) * per]
        gate = up = 0.0
        for p in range(PIECES):
            at = slice(p * deep, (p + 1) * deep)
            take(e, 0, p)
            gate = gate + dot(mine[:, at], gate_ref[e, at])
            take(e, 1, p)
            up = up + dot(mine[:, at], up_ref[e, at])
        hidden_ref[...] = (gate / (1.0 + jnp.exp(-gate)) * up).astype(BF16)
        result = 0.0
        for p in range(PIECES):
            take(e, 2, p)
            at = slice(p * tall, (p + 1) * tall)
            result = result + dot(hidden_ref[:, at], down_ref[e, at])
        finished_ref[e * per:(e + 1) * per, :] = result.astype(BF16)
    for start in range(0, width, 512):
        at = slice(start, start + 512)
        out_ref[:, at] = dot(by_source, finished_ref[:, at]).astype(BF16)


PIECES = 4
FLIGHT = 10


def experts_here(rows, gate, up, down, routed, router, ids):
    here, width, middle = gate.shape
    per = rows.shape[0] // here
    tokens, experts = routed.shape[0], router.shape[0]
    capacity = 4 * tokens // experts
    vmem = pl.BlockSpec(memory_space=pltpu.VMEM)
    hbm = pl.BlockSpec(memory_space=pltpu.HBM)
    return pl.pallas_call(
        expert_kernel,
        out_shape=[
            jax.ShapeDtypeStruct(rows.shape, BF16),
            jax.ShapeDtypeStruct((2 * tokens, experts * capacity), BF16),
            jax.ShapeDtypeStruct((tokens, 128), F32),
        ],
        in_specs=[vmem] + [hbm] * 3 + [vmem] * 3,
        out_specs=[vmem] * 3,
        scratch_shapes=[
            pltpu.VMEM(gate.shape, BF16),
            pltpu.VMEM(up.shape, BF16),
            pltpu.VMEM(down.shape, BF16),
            pltpu.VMEM((per, middle), BF16),
            pltpu.VMEM(rows.shape, BF16),
            pltpu.SemaphoreType.DMA((here, 3, PIECES)),
        ],
        compiler_params=pltpu.CompilerParams(vmem_limit_bytes=46 * MIB),
        cost_estimate=pl.CostEstimate(flops=5 * 10 ** 9, bytes_accessed=10 ** 7, transcendentals=0),
        name="experts",
    )(rows, *[pltpu.with_memory_space_constraint(w, pltpu.HBM) for w in (gate, up, down)], routed, router, ids)


def combine_kernel(residual_ref, leading_ref, pick_ref, back_ref, out_ref):
    tokens = residual_ref.shape[0]
    picked = dot(pick_ref[...], back_ref[...])
    leading = leading_ref[:, 0:1]
    blended = leading * picked[:tokens] + (1.0 - leading) * picked[tokens:]
    out_ref[...] = (residual_ref[...] + blended).astype(BF16)


def combine(residual, leading, pick, back):
    vmem = pl.BlockSpec(memory_space=pltpu.VMEM)
    return pl.pallas_call(
        combine_kernel,
        out_shape=jax.ShapeDtypeStruct(residual.shape, BF16),
        in_specs=[vmem] * 4,
        out_specs=vmem,
        compiler_params=pltpu.CompilerParams(vmem_limit_bytes=16 * MIB),
        cost_estimate=pl.CostEstimate(flops=10 ** 9, bytes_accessed=10 ** 6, transcendentals=0),
        name="combine",
    )(residual, leading, pick, back)


def turned(x, k, axis):
    size = lax.axis_size(axis)
    return lax.ppermute(x, axis, [(i, (i + k) % size) for i in range(size)])


def shards(tokens, mixer_gain, query_weight, key_weight, value_weight, beta_weight, head_gain, output_weight,
           expert_gain, router_weight, expert_ids, gate_weight, up_weight, down_weight):
    peers = lax.axis_size("head")
    owners = lax.axis_size("dp")
    me = lax.axis_index("head").reshape(1).astype(jnp.int32)
    xs = [tokens] + [turned(tokens, k, "head") for k in range(1, peers)]
    gain = mixer_gain.reshape(peers, -1)
    here = first(me, gain, tokens, query_weight, key_weight, value_weight, beta_weight.T, head_gain.reshape(1, -1),
                 output_weight)
    xs[0], weights, sums = here[0], here[1:5], here[7:]
    for shift in (1, 3):
        sums = more(shift, me, gain, xs[shift], weights, sums)
    parts = mixer(me, gain, xs[2], 2, weights, sums, here[5], here[6])
    parts = [parts[0]] + [turned(parts[k], k, "head") for k in range(1, peers)]
    experts = router_weight.shape[1]
    own = parts[0].shape[0]
    capacity = 4 * own // experts
    ids = expert_ids.T
    residual, routed, outgoing = route(me, parts, xs, expert_gain.reshape(1, -1), ids, experts, capacity)
    width = outgoing.shape[1]
    outgoing = outgoing.reshape(owners, -1, width)
    arrived = lax.all_to_all(outgoing, "dp", split_axis=0, concat_axis=0, tiled=True)
    result, pick, leading = experts_here(
        arrived.reshape(-1, width), gate_weight, up_weight, down_weight, routed, router_weight.T, ids
    )
    back = lax.all_to_all(result.reshape(owners, -1, width), "dp", split_axis=0, concat_axis=0, tiled=True)
    return combine(residual, leading, pick, back.reshape(-1, width))


def solution(mesh):
    return jax.shard_map(
        shards,
        mesh=mesh,
        in_specs=(
            P("dp", "head"),
            P(),
            P(None, "head"),
            P(None, None, "head"),
            P(None, None, "head"),
            P(None, "head"),
            P(),
            P("head", None),
            P(),
            P(),
            P(("dp", "head"), None),
            P("dp", None, None),
            P("dp", None, None),
            P("dp", None, None),
        ),
        out_specs=P(("dp", "head"), None),
        check_vma=False,
    )
```

```python
import jax
import jax.numpy as jnp
from jax import lax
from jax.experimental import pallas as pl
from jax.experimental.pallas import tpu as pltpu
from jax.sharding import PartitionSpec as P

DK = 128
NH = 3
CH = 32
SUB = CH * NH
WIDE = 128
BASE = 4
EPSILON = 1e-06
F32 = jnp.float32
BF16 = jnp.bfloat16
MIB = 1 << 20


def dot(a, b, dims=((1,), (0,))):
    return lax.dot_general(a, b, (dims, ((), ())), preferred_element_type=F32)


def split(a):
    high = a.astype(BF16)
    return high, (a - high.astype(F32)).astype(BF16)


def dot3(a, b, dims=((1,), (0,))):
    return dot(a[0], b[0], dims) + (dot(a[0], b[1], dims) + dot(a[1], b[0], dims))


def iota(shape, dim):
    return lax.broadcasted_iota(jnp.int32, shape, dim)


def rows_at(block, size):
    return pl.ds(pl.multiple_of(block * size, size), size)


def gained(x_ref, gain_ref, source):
    wide = x_ref[...].astype(F32)
    return (wide * gain_ref[pl.ds(source, 1), :]).astype(BF16), jnp.sum(wide * wide, -1, keepdims=True)


def products(x, source, wq_ref, wk_ref, wv_ref, wb_ref):
    rows = rows_at(source, x.shape[1])
    yield dot(x, wq_ref[rows, :])
    for ref in (wk_ref, wv_ref):
        for m in range(NH):
            yield dot(x, ref[m, rows, :])
    yield dot(x, wb_ref[:, rows], ((1,), (1,)))


def first_kernel(place_ref, gain_ref, *refs):
    count = (len(refs) - 4) // 2
    here, there = refs[:count], refs[count:2 * count]
    sums_ref, beta_ref, square_ref, sems = refs[2 * count:]
    copies = [pltpu.make_async_copy(h, t, sems.at[i]) for i, (h, t) in enumerate(zip(here, there))]
    for copy in copies:
        copy.start()
    for copy in copies:
        copy.wait()
    x, square_ref[...] = gained(there[0], gain_ref, place_ref[0])
    for i, product in enumerate(products(x, place_ref[0], *there[1:5])):
        if i < 1 + 2 * NH:
            sums_ref[i] = product
        else:
            beta_ref[...] = product


def first(me, gain, tokens, wq, wk, wv, wb, *others):
    moved = (tokens, wq, wk, wv, wb, *others)
    length = tokens.shape[0]
    vmem = pl.BlockSpec(memory_space=pltpu.VMEM)
    made = [
        pltpu.VMEM((1 + 2 * NH, length, wq.shape[1]), F32),
        pltpu.VMEM((length, wb.shape[0]), F32),
        pltpu.VMEM((length, 1), F32),
    ]
    return pl.pallas_call(
        first_kernel,
        out_shape=[pltpu.VMEM(w.shape, w.dtype) for w in moved] + made,
        in_specs=[pl.BlockSpec(memory_space=pltpu.SMEM), vmem] + [pl.BlockSpec(memory_space=pltpu.HBM)] * len(moved),
        out_specs=[vmem] * (len(moved) + 3),
        scratch_shapes=[pltpu.SemaphoreType.DMA((len(moved),))],
        compiler_params=pltpu.CompilerParams(vmem_limit_bytes=4 * MIB),
        cost_estimate=pl.CostEstimate(flops=2 * 10 ** 9, bytes_accessed=10 ** 6, transcendentals=0),
        name="first",
    )(me, gain, *[pltpu.with_memory_space_constraint(w, pltpu.HBM) for w in moved])


def more_kernel(shift, place_ref, gain_ref, x_ref, wq_ref, wk_ref, wv_ref, wb_ref, sums_ref, beta_ref, square_ref,
                new_sums_ref, new_beta_ref, new_square_ref):
    source = (place_ref[0] + (gain_ref.shape[0] - shift)) % gain_ref.shape[0]
    x, square = gained(x_ref, gain_ref, source)
    new_square_ref[...] = square_ref[...] + square
    for i, product in enumerate(products(x, source, wq_ref, wk_ref, wv_ref, wb_ref)):
        if i < 1 + 2 * NH:
            new_sums_ref[i] = sums_ref[i] + product
        else:
            new_beta_ref[...] = beta_ref[...] + product


def more(shift, me, gain, x, weights, sums):
    vmem = pl.BlockSpec(memory_space=pltpu.VMEM)
    return pl.pallas_call(
        lambda *refs: more_kernel(shift, *refs),
        out_shape=[pltpu.VMEM(a.shape, a.dtype) for a in sums],
        in_specs=[pl.BlockSpec(memory_space=pltpu.SMEM)] + [vmem] * 9,
        out_specs=[vmem] * 3,
        input_output_aliases={7: 0, 8: 1, 9: 2},
        compiler_params=pltpu.CompilerParams(vmem_limit_bytes=4 * MIB),
        cost_estimate=pl.CostEstimate(flops=10 ** 9, bytes_accessed=10 ** 6, transcendentals=0),
        name="more",
    )(me, gain, x, *weights, *sums)


def mixer_kernel(heads, shift, place_ref, gain_ref, x_ref, wq_ref, wk_ref, wv_ref, wb_ref, sums_ref, beta_ref, square_ref,
                 head_gain_ref, wo_ref, o0, o1, o2, o3, keys, beta_keys, rhs, queries, state_map, added, out_add, mixed):
    me = place_ref[0]
    count, part = gain_ref.shape
    length = x_ref.shape[0]
    source = lax.rem(me + (count - shift), count)
    x, square = gained(x_ref, gain_ref, source)
    scale = lax.rsqrt((square_ref[...] + square) / (count * part) + EPSILON)
    last = products(x, source, wq_ref, wk_ref, wv_ref, wb_ref)
    whole = [(sums_ref[i] + next(last)) * scale for i in range(1 + 2 * NH)]
    beta = (beta_ref[...] + next(last)) * scale
    beta = 2.0 / (1.0 + jnp.exp(-beta))
    blocks = length // CH
    query = whole[0]
    for h in range(heads):
        q = query[:, h * DK:(h + 1) * DK]
        q = q * lax.rsqrt(jnp.sum(q * q, -1, keepdims=True) + EPSILON) * DK ** (-0.5)
        queries[h] = q.reshape(blocks, CH, DK)
    for edge in (SUB, WIDE + SUB):
        keys[:, :, edge:edge + WIDE - SUB, :] = jnp.zeros((heads, blocks, WIDE - SUB, DK), BF16)
    for m in range(NH):
        key = whole[1 + m]
        value = whole[1 + NH + m]
        for h in range(heads):
            b = beta[:, h * NH + m:h * NH + m + 1]
            k = key[:, h * DK:(h + 1) * DK]
            k = k * lax.rsqrt(jnp.sum(k * k, -1, keepdims=True) + EPSILON)
            high, low = split(k)
            keys[h, :, m * CH:(m + 1) * CH, :] = high.reshape(blocks, CH, DK)
            keys[h, :, WIDE + m * CH:WIDE + (m + 1) * CH, :] = low.reshape(blocks, CH, DK)
            rhs[h, :, m * CH:(m + 1) * CH, :DK] = (k * b).astype(BF16).reshape(blocks, CH, DK)
            rhs[h, :, m * CH:(m + 1) * CH, DK:] = (value[:, h * DK:(h + 1) * DK] * b).astype(BF16).reshape(blocks, CH, DK)
            beta_keys[h, :, m * CH:(m + 1) * CH, :] = jnp.broadcast_to(b, (length, DK)).reshape(blocks, CH, DK)

    row, col = iota((SUB, WIDE), 0), iota((SUB, WIDE), 1)
    inside = col < SUB
    row_t, col_t = row % CH, col % CH
    causal = inside & ((col_t < row_t) | ((col_t == row_t) & (col < row)))
    near = row_t // BASE == col_t // BASE
    eye = (row == col).astype(F32)
    seen = iota((CH, SUB), 1) % CH <= iota((CH, SUB), 0)
    blank = jnp.zeros((WIDE - SUB, WIDE), F32)

    def square(p):
        return dot(p[:, :SUB], p)

    def both(p, t):
        made = dot(p[:, :SUB], jnp.concatenate([p, t.astype(BF16)], 1))
        return made[:, :WIDE].astype(BF16), t + made[:, WIDE:]

    def doubled(powers, sums, terms):
        span = 2
        while 2 * span < terms:
            stepped = [both(p, t) for p, t in zip(powers, sums)]
            powers, sums = [p for p, _ in stepped], [t for _, t in stepped]
            span *= 2
        return [t + dot(p[:, :SUB], t.astype(BF16)) for p, t in zip(powers, sums)]

    unroll = UNROLL
    for start in range(0, blocks, unroll):
        at = [(h, c) for c in range(start, start + unroll) for h in range(heads)]
        pairs = [keys[i] for i in at]
        alike = [dot(k[:SUB], k, ((1,), (1,))) for k in pairs]
        alike = [
            a[:, :WIDE] + a[:, WIDE:] + jnp.transpose(jnp.concatenate([a[:, WIDE:], blank], 0))[:SUB] for a in alike
        ]
        lower = [jnp.where(causal, a * beta_keys[i], 0.0) for i, a in zip(at, alike)]
        power = [jnp.where(near, -l, 0.0) for l in lower]
        inverse = [eye + p for p in power]
        power = [square(p.astype(BF16)).astype(BF16) for p in power]
        inverse = doubled(power, inverse, BASE * NH)
        low = [t.astype(BF16) for t in inverse]
        power = [
            -dot(t[:, :SUB], jnp.where(near, 0.0, l).astype(BF16)) for t, l in zip(low, lower)
        ]
        power = [p.astype(BF16) for p in power]
        stepped = [both(p, t) for p, t in zip(power, inverse)]
        inverse = doubled([p for p, _ in stepped], [t for _, t in stepped], CH // BASE)
        high = [split(t) for t in inverse]
        parts = [split(l) for l in lower]
        made = [dot(l[0][:, :SUB], jnp.concatenate([s[0], s[1]], 1)) for l, s in zip(parts, high)]
        rest = [dot(l[1][:, :SUB], s[0]) for l, s in zip(parts, high)]
        error = [eye - t - (m[:, :WIDE] + (m[:, WIDE:] + r)) for t, m, r in zip(inverse, made, rest)]
        inverse = [t + dot(s[0][:, :SUB], e.astype(BF16)) for t, s, e in zip(inverse, high, error)]
        solved = [dot(t[:, :SUB].astype(BF16), rhs[i]).astype(BF16) for i, t in zip(at, inverse)]
        change = [dot(k[:SUB], s, ((0,), (0,))) for k, s in zip(pairs, solved)]
        qs = [queries[i] for i in at]
        attend = [jnp.where(seen, dot(q.astype(BF16), k[:SUB], ((1,), (1,))), 0.0).astype(BF16) for q, k in zip(qs, pairs)]
        effect = [dot(a, s) for a, s in zip(attend, solved)]
        for i, g, q, e in zip(at, change, qs, effect):
            state_map[i + (slice(0, CH),)] = (q - e[:, :DK]).astype(BF16)
            state_map[i + (slice(CH, CH + DK),)] = g[:, :DK].astype(BF16)
            added[i] = g[:, DK:]
            out_add[i] = e[:, DK:]

    states = [jnp.zeros((DK, DK), F32) for _ in range(heads)]
    for c in range(blocks):
        for h in range(heads):
            moved = dot(state_map[h, c], states[h].astype(BF16))
            out = moved[:CH] + out_add[h, c]
            states[h] = states[h] - moved[CH:] + added[h, c]
            out = out * lax.rsqrt(jnp.mean(out * out, -1, keepdims=True) + EPSILON) * head_gain_ref[...]
            mixed[c * CH:(c + 1) * CH, h * DK:(h + 1) * DK] = out.astype(BF16)
    own = length // count
    rolled = jnp.concatenate([mixed[rows_at(lax.rem(me + k, count), own), :] for k in range(count)], 0)
    result = dot(rolled, wo_ref[...]).astype(BF16)
    for k, o in enumerate((o0, o1, o2, o3)):
        o[...] = result[k * own:(k + 1) * own]


UNROLL = 8


def mixer(me, gain, x, shift, weights, sums, head_gain, wo):
    count = gain.shape[0]
    length = x.shape[0]
    heads = weights[0].shape[1] // DK
    blocks = length // CH
    own = length // count
    vmem = pl.BlockSpec(memory_space=pltpu.VMEM)
    return pl.pallas_call(
        lambda *refs: mixer_kernel(heads, shift, *refs),
        out_shape=[jax.ShapeDtypeStruct((own, wo.shape[1]), BF16)] * count,
        in_specs=[pl.BlockSpec(memory_space=pltpu.SMEM)] + [vmem] * 11,
        out_specs=[vmem] * count,
        scratch_shapes=[
            pltpu.VMEM((heads, blocks, 2 * WIDE, DK), BF16),
            pltpu.VMEM((heads, blocks, SUB, DK), F32),
            pltpu.VMEM((heads, blocks, SUB, 2 * DK), BF16),
            pltpu.VMEM((heads, blocks, CH, DK), F32),
            pltpu.VMEM((heads, blocks, CH + DK, DK), BF16),
            pltpu.VMEM((heads, blocks, DK, DK), F32),
            pltpu.VMEM((heads, blocks, CH, DK), F32),
            pltpu.VMEM((length, heads * DK), BF16),
        ],
        compiler_params=pltpu.CompilerParams(vmem_limit_bytes=32 * MIB),
        cost_estimate=pl.CostEstimate(flops=2 * 10 ** 10, bytes_accessed=10 ** 7, transcendentals=0),
        name="mixer",
    )(me, gain, x, *weights, *sums, head_gain, wo)


def slots(ids_ref, experts, capacity):
    tokens = ids_ref.shape[1]
    label = iota((experts, tokens), 0)
    chosen = [(label == ids_ref[k:k + 1, :]).astype(F32) for k in range(2)]
    count = chosen[0] + chosen[1]
    before = (iota((tokens, tokens), 0) < iota((tokens, tokens), 1)).astype(BF16)
    earlier = dot(count.astype(BF16), before)
    total = experts * capacity
    spread = (iota((total, experts), 0) // capacity == iota((total, experts), 1)).astype(BF16)
    place = dot(spread, earlier.astype(BF16))
    fits = place == (iota((total, tokens), 0) % capacity).astype(F32)
    return chosen, [jnp.where(fits, dot(spread, c.astype(BF16)), 0.0) for c in chosen]


def route_kernel(place_ref, p0, p1, p2, p3, x0, x1, x2, x3, gain_ref, ids_ref, residual_ref, routed_ref, send_ref):
    me = place_ref[0]
    xs = (x0, x1, x2, x3)
    count = len(xs)
    own, part = p0.shape[0], x0.shape[1]
    for k in range(count):
        columns = rows_at(lax.rem(me - k + count, count), part)
        residual_ref[:, columns] = xs[k][rows_at(me, own), :].astype(F32)
    arrived = [p[...].astype(F32) for p in (p0, p1, p2, p3)]
    residual = residual_ref[...] + ((arrived[0] + arrived[1]) + (arrived[2] + arrived[3]))
    residual_ref[...] = residual
    mean = jnp.mean(residual * residual, -1, keepdims=True)
    routed = residual * lax.rsqrt(mean + EPSILON) * gain_ref[...]
    routed_ref[...] = routed
    _, chosen = slots(ids_ref, 64, send_ref.shape[0] // 64)
    chosen = (chosen[0] + chosen[1]).astype(BF16)
    send_ref[...] = dot(chosen, routed.astype(BF16)).astype(BF16)


def route(me, parts, xs, gain, ids, experts, capacity):
    own, width = parts[0].shape
    vmem = pl.BlockSpec(memory_space=pltpu.VMEM)
    return pl.pallas_call(
        route_kernel,
        out_shape=[
            jax.ShapeDtypeStruct((own, width), F32),
            jax.ShapeDtypeStruct((own, width), F32),
            jax.ShapeDtypeStruct((experts * capacity, width), BF16),
        ],
        in_specs=[pl.BlockSpec(memory_space=pltpu.SMEM)] + [vmem] * 10,
        out_specs=[vmem] * 3,
        compiler_params=pltpu.CompilerParams(vmem_limit_bytes=16 * MIB),
        cost_estimate=pl.CostEstimate(flops=10 ** 9, bytes_accessed=10 ** 7, transcendentals=0),
        name="route",
    )(me, *parts, *xs, gain, ids)


def weigh(routed_ref, router_ref, ids_ref, pick_ref, leading_ref):
    experts = router_ref.shape[0]
    chosen, parts = slots(ids_ref, experts, pick_ref.shape[1] // experts)
    tokens = routed_ref.shape[0]
    for k in range(2):
        pick_ref[k * tokens:(k + 1) * tokens, :] = jnp.transpose(parts[k]).astype(BF16)
    logits = lax.dot_general(
        router_ref[...], routed_ref[...], (((1,), (1,)), ((), ())),
        precision=lax.Precision.HIGHEST, preferred_element_type=F32,
    )
    gap = jnp.sum((chosen[0] - chosen[1]) * logits, 0, keepdims=True)
    leading = 1.0 / (1.0 + jnp.exp(-gap))
    leading_ref[...] = jnp.transpose(jnp.broadcast_to(leading, (128, tokens)))


def expert_kernel(rows_ref, gate_hbm, up_hbm, down_hbm, routed_ref, router_ref, ids_ref, out_ref, pick_ref, leading_ref,
                  gate_ref, up_ref, down_ref, hidden_ref, finished_ref, sems):
    total = rows_ref.shape[0]
    here, width, middle = gate_hbm.shape
    per = total // here
    experts = router_ref.shape[0]
    cap = pick_ref.shape[1] // experts
    deep, tall = width // PIECES, middle // PIECES
    copies, order = {}, []
    for e in range(here):
        for part, (source, target) in enumerate(((gate_hbm, gate_ref), (up_hbm, up_ref), (down_hbm, down_ref))):
            size = tall if part == 2 else deep
            for p in range(PIECES):
                at = (e, pl.ds(p * size, size))
                copies[e, part, p] = pltpu.make_async_copy(source.at[at], target.at[at], sems.at[e, part, p])
        for p in range(PIECES):
            order += [(e, 0, p), (e, 1, p)]
        order += [(e, 2, p) for p in range(PIECES)]
    for key in order[:FLIGHT]:
        copies[key].start()

    def take(*key):
        copies[key].wait()
        following = order.index(key) + FLIGHT
        if following < len(order):
            copies[order[following]].start()

    weigh(routed_ref, router_ref, ids_ref, pick_ref, leading_ref)
    r, c = iota((total, total), 0), iota((total, total), 1)

    def source(i):
        return (i % per) // cap * (here * cap) + i // per * cap + i % cap

    by_expert = (source(r) == c).astype(BF16)
    by_source = (source(c) == r).astype(BF16)
    rows = dot(by_expert, rows_ref[...]).astype(BF16)
    for e in range(here):
        mine = rows[e * per:(e + 1) * per]
        gate = up = 0.0
        for p in range(PIECES):
            at = slice(p * deep, (p + 1) * deep)
            take(e, 0, p)
            gate = gate + dot(mine[:, at], gate_ref[e, at])
            take(e, 1, p)
            up = up + dot(mine[:, at], up_ref[e, at])
        hidden_ref[...] = (gate / (1.0 + jnp.exp(-gate)) * up).astype(BF16)
        result = 0.0
        for p in range(PIECES):
            take(e, 2, p)
            at = slice(p * tall, (p + 1) * tall)
            result = result + dot(hidden_ref[:, at], down_ref[e, at])
        finished_ref[e * per:(e + 1) * per, :] = result.astype(BF16)
    for start in range(0, width, 512):
        at = slice(start, start + 512)
        out_ref[:, at] = dot(by_source, finished_ref[:, at]).astype(BF16)


PIECES = 4
FLIGHT = 10


def experts_here(rows, gate, up, down, routed, router, ids):
    here, width, middle = gate.shape
    per = rows.shape[0] // here
    tokens, experts = routed.shape[0], router.shape[0]
    capacity = 4 * tokens // experts
    vmem = pl.BlockSpec(memory_space=pltpu.VMEM)
    hbm = pl.BlockSpec(memory_space=pltpu.HBM)
    return pl.pallas_call(
        expert_kernel,
        out_shape=[
            jax.ShapeDtypeStruct(rows.shape, BF16),
            jax.ShapeDtypeStruct((2 * tokens, experts * capacity), BF16),
            jax.ShapeDtypeStruct((tokens, 128), F32),
        ],
        in_specs=[vmem] + [hbm] * 3 + [vmem] * 3,
        out_specs=[vmem] * 3,
        scratch_shapes=[
            pltpu.VMEM(gate.shape, BF16),
            pltpu.VMEM(up.shape, BF16),
            pltpu.VMEM(down.shape, BF16),
            pltpu.VMEM((per, middle), BF16),
            pltpu.VMEM(rows.shape, BF16),
            pltpu.SemaphoreType.DMA((here, 3, PIECES)),
        ],
        compiler_params=pltpu.CompilerParams(vmem_limit_bytes=46 * MIB),
        cost_estimate=pl.CostEstimate(flops=5 * 10 ** 9, bytes_accessed=10 ** 7, transcendentals=0),
        name="experts",
    )(rows, *[pltpu.with_memory_space_constraint(w, pltpu.HBM) for w in (gate, up, down)], routed, router, ids)


def combine_kernel(residual_ref, leading_ref, pick_ref, back_ref, out_ref):
    tokens = residual_ref.shape[0]
    picked = dot(pick_ref[...], back_ref[...])
    leading = leading_ref[:, 0:1]
    blended = leading * picked[:tokens] + (1.0 - leading) * picked[tokens:]
    out_ref[...] = (residual_ref[...] + blended).astype(BF16)


def combine(residual, leading, pick, back):
    vmem = pl.BlockSpec(memory_space=pltpu.VMEM)
    return pl.pallas_call(
        combine_kernel,
        out_shape=jax.ShapeDtypeStruct(residual.shape, BF16),
        in_specs=[vmem] * 4,
        out_specs=vmem,
        compiler_params=pltpu.CompilerParams(vmem_limit_bytes=16 * MIB),
        cost_estimate=pl.CostEstimate(flops=10 ** 9, bytes_accessed=10 ** 6, transcendentals=0),
        name="combine",
    )(residual, leading, pick, back)


def turned(x, k, axis):
    size = lax.axis_size(axis)
    return lax.ppermute(x, axis, [(i, (i + k) % size) for i in range(size)])


def shards(tokens, mixer_gain, query_weight, key_weight, value_weight, beta_weight, head_gain, output_weight,
           expert_gain, router_weight, expert_ids, gate_weight, up_weight, down_weight):
    peers = lax.axis_size("head")
    owners = lax.axis_size("dp")
    me = lax.axis_index("head").reshape(1).astype(jnp.int32)
    xs = [tokens] + [turned(tokens, k, "head") for k in range(1, peers)]
    gain = mixer_gain.reshape(peers, -1)
    here = first(me, gain, tokens, query_weight, key_weight, value_weight, beta_weight.T, head_gain.reshape(1, -1),
                 output_weight)
    xs[0], weights, sums = here[0], here[1:5], here[7:]
    for shift in (1, 3):
        sums = more(shift, me, gain, xs[shift], weights, sums)
    parts = mixer(me, gain, xs[2], 2, weights, sums, here[5], here[6])
    parts = [parts[0]] + [turned(parts[k], k, "head") for k in range(1, peers)]
    experts = router_weight.shape[1]
    own = parts[0].shape[0]
    capacity = 4 * own // experts
    ids = expert_ids.T
    residual, routed, outgoing = route(me, parts, xs, expert_gain.reshape(1, -1), ids, experts, capacity)
    width = outgoing.shape[1]
    outgoing = outgoing.reshape(owners, -1, width)
    arrived = lax.all_to_all(outgoing, "dp", split_axis=0, concat_axis=0, tiled=True)
    result, pick, leading = experts_here(
        arrived.reshape(-1, width), gate_weight, up_weight, down_weight, routed, router_weight.T, ids
    )
    back = lax.all_to_all(result.reshape(owners, -1, width), "dp", split_axis=0, concat_axis=0, tiled=True)
    return combine(residual, leading, pick, back.reshape(-1, width))


def solution(mesh):
    return jax.shard_map(
        shards,
        mesh=mesh,
        in_specs=(
            P("dp", "head"),
            P(),
            P(None, "head"),
            P(None, None, "head"),
            P(None, None, "head"),
            P(None, "head"),
            P(),
            P("head", None),
            P(),
            P(),
            P(("dp", "head"), None),
            P("dp", None, None),
            P("dp", None, None),
            P("dp", None, None),
        ),
        out_specs=P(("dp", "head"), None),
        check_vma=False,
    )
```

```python
import jax
import jax.numpy as jnp
from jax import lax
from jax.experimental import pallas as pl
from jax.experimental.pallas import tpu as pltpu
from jax.sharding import PartitionSpec as P

DK = 128
NH = 3
CH = 32
SUB = CH * NH
WIDE = 128
BASE = 4
EPSILON = 1e-06
F32 = jnp.float32
BF16 = jnp.bfloat16
MIB = 1 << 20


def dot(a, b, dims=((1,), (0,))):
    return lax.dot_general(a, b, (dims, ((), ())), preferred_element_type=F32)


def split(a):
    high = a.astype(BF16)
    return high, (a - high.astype(F32)).astype(BF16)


def dot3(a, b, dims=((1,), (0,))):
    return dot(a[0], b[0], dims) + (dot(a[0], b[1], dims) + dot(a[1], b[0], dims))


def iota(shape, dim):
    return lax.broadcasted_iota(jnp.int32, shape, dim)


def rows_at(block, size):
    return pl.ds(pl.multiple_of(block * size, size), size)


def gained(x_ref, gain_ref, source):
    wide = x_ref[...].astype(F32)
    return (wide * gain_ref[pl.ds(source, 1), :]).astype(BF16), jnp.sum(wide * wide, -1, keepdims=True)


def products(x, source, wq_ref, wk_ref, wv_ref, wb_ref):
    rows = rows_at(source, x.shape[1])
    yield dot(x, wq_ref[rows, :])
    for ref in (wk_ref, wv_ref):
        for m in range(NH):
            yield dot(x, ref[m, rows, :])
    yield dot(x, wb_ref[:, rows], ((1,), (1,)))


def first_kernel(place_ref, gain_ref, *refs):
    count = (len(refs) - 4) // 2
    here, there = refs[:count], refs[count:2 * count]
    sums_ref, beta_ref, square_ref, sems = refs[2 * count:]
    copies = [pltpu.make_async_copy(h, t, sems.at[i]) for i, (h, t) in enumerate(zip(here, there))]
    for copy in copies:
        copy.start()
    for copy in copies:
        copy.wait()
    x, square_ref[...] = gained(there[0], gain_ref, place_ref[0])
    for i, product in enumerate(products(x, place_ref[0], *there[1:5])):
        if i < 1 + 2 * NH:
            sums_ref[i] = product
        else:
            beta_ref[...] = product


def first(me, gain, tokens, wq, wk, wv, wb, *others):
    moved = (tokens, wq, wk, wv, wb, *others)
    length = tokens.shape[0]
    vmem = pl.BlockSpec(memory_space=pltpu.VMEM)
    made = [
        pltpu.VMEM((1 + 2 * NH, length, wq.shape[1]), F32),
        pltpu.VMEM((length, wb.shape[0]), F32),
        pltpu.VMEM((length, 1), F32),
    ]
    return pl.pallas_call(
        first_kernel,
        out_shape=[pltpu.VMEM(w.shape, w.dtype) for w in moved] + made,
        in_specs=[pl.BlockSpec(memory_space=pltpu.SMEM), vmem] + [pl.BlockSpec(memory_space=pltpu.HBM)] * len(moved),
        out_specs=[vmem] * (len(moved) + 3),
        scratch_shapes=[pltpu.SemaphoreType.DMA((len(moved),))],
        compiler_params=pltpu.CompilerParams(vmem_limit_bytes=4 * MIB),
        cost_estimate=pl.CostEstimate(flops=2 * 10 ** 9, bytes_accessed=10 ** 6, transcendentals=0),
        name="first",
    )(me, gain, *[pltpu.with_memory_space_constraint(w, pltpu.HBM) for w in moved])


def more_kernel(place_ref, gain_ref, x_ref, wq_ref, wk_ref, wv_ref, wb_ref, sums_ref, beta_ref, square_ref,
                new_sums_ref, new_beta_ref, new_square_ref):
    source = place_ref[1]
    x, square = gained(x_ref, gain_ref, source)
    new_square_ref[...] = square_ref[...] + square
    for i, product in enumerate(products(x, source, wq_ref, wk_ref, wv_ref, wb_ref)):
        if i < 1 + 2 * NH:
            new_sums_ref[i] = sums_ref[i] + product
        else:
            new_beta_ref[...] = beta_ref[...] + product


def more(me, gain, x, weights, sums):
    vmem = pl.BlockSpec(memory_space=pltpu.VMEM)
    return pl.pallas_call(
        more_kernel,
        out_shape=[pltpu.VMEM(a.shape, a.dtype) for a in sums],
        in_specs=[pl.BlockSpec(memory_space=pltpu.SMEM)] + [vmem] * 9,
        out_specs=[vmem] * 3,
        input_output_aliases={7: 0, 8: 1, 9: 2},
        compiler_params=pltpu.CompilerParams(vmem_limit_bytes=4 * MIB),
        cost_estimate=pl.CostEstimate(flops=10 ** 9, bytes_accessed=10 ** 6, transcendentals=0),
        name="more",
    )(me, gain, x, *weights, *sums)


def mixer_kernel(heads, place_ref, gain_ref, x2, x3, wq_ref, wk_ref, wv_ref, wb_ref, sums_ref, beta_ref, square_ref,
                 head_gain_ref, wo_ref, o0, o1, o2, o3, keys, beta_keys, rhs, queries, state_map, added, out_add, mixed):
    count, part = gain_ref.shape
    length = x2.shape[0]
    total, last = square_ref[...], []
    for x_ref, source in ((x2, place_ref[2]), (x3, place_ref[3])):
        x, square = gained(x_ref, gain_ref, source)
        total = total + square
        last.append(products(x, source, wq_ref, wk_ref, wv_ref, wb_ref))
    scale = lax.rsqrt(total / (count * part) + EPSILON)
    whole = [(sums_ref[i] + (next(last[0]) + next(last[1]))) * scale for i in range(1 + 2 * NH)]
    beta = (beta_ref[...] + (next(last[0]) + next(last[1]))) * scale
    beta = 2.0 / (1.0 + jnp.exp(-beta))
    blocks = length // CH
    query = whole[0]
    for h in range(heads):
        q = query[:, h * DK:(h + 1) * DK]
        q = q * lax.rsqrt(jnp.sum(q * q, -1, keepdims=True) + EPSILON) * DK ** (-0.5)
        queries[h] = q.reshape(blocks, CH, DK)
    for edge in (SUB, WIDE + SUB):
        keys[:, :, edge:edge + WIDE - SUB, :] = jnp.zeros((heads, blocks, WIDE - SUB, DK), BF16)
    for m in range(NH):
        key = whole[1 + m]
        value = whole[1 + NH + m]
        for h in range(heads):
            b = beta[:, h * NH + m:h * NH + m + 1]
            k = key[:, h * DK:(h + 1) * DK]
            k = k * lax.rsqrt(jnp.sum(k * k, -1, keepdims=True) + EPSILON)
            high, low = split(k)
            keys[h, :, m * CH:(m + 1) * CH, :] = high.reshape(blocks, CH, DK)
            keys[h, :, WIDE + m * CH:WIDE + (m + 1) * CH, :] = low.reshape(blocks, CH, DK)
            rhs[h, :, m * CH:(m + 1) * CH, :DK] = (k * b).astype(BF16).reshape(blocks, CH, DK)
            rhs[h, :, m * CH:(m + 1) * CH, DK:] = (value[:, h * DK:(h + 1) * DK] * b).astype(BF16).reshape(blocks, CH, DK)
            beta_keys[h, :, m * CH:(m + 1) * CH, :] = jnp.broadcast_to(b, (length, DK)).reshape(blocks, CH, DK)

    row, col = iota((SUB, WIDE), 0), iota((SUB, WIDE), 1)
    inside = col < SUB
    row_t, col_t = row % CH, col % CH
    causal = inside & ((col_t < row_t) | ((col_t == row_t) & (col < row)))
    near = row_t // BASE == col_t // BASE
    eye = (row == col).astype(F32)
    seen = iota((CH, SUB), 1) % CH <= iota((CH, SUB), 0)
    blank = jnp.zeros((WIDE - SUB, WIDE), F32)

    def square(p):
        return dot(p[:, :SUB], p)

    def both(p, t):
        made = dot(p[:, :SUB], jnp.concatenate([p, t.astype(BF16)], 1))
        return made[:, :WIDE].astype(BF16), t + made[:, WIDE:]

    def doubled(powers, sums, terms):
        span = 2
        while 2 * span < terms:
            stepped = [both(p, t) for p, t in zip(powers, sums)]
            powers, sums = [p for p, _ in stepped], [t for _, t in stepped]
            span *= 2
        return [t + dot(p[:, :SUB], t.astype(BF16)) for p, t in zip(powers, sums)]

    unroll = UNROLL
    for start in range(0, blocks, unroll):
        at = [(h, c) for c in range(start, start + unroll) for h in range(heads)]
        pairs = [keys[i] for i in at]
        alike = [dot(k[:SUB], k, ((1,), (1,))) for k in pairs]
        alike = [
            a[:, :WIDE] + a[:, WIDE:] + jnp.transpose(jnp.concatenate([a[:, WIDE:], blank], 0))[:SUB] for a in alike
        ]
        lower = [jnp.where(causal, a * beta_keys[i], 0.0) for i, a in zip(at, alike)]
        power = [jnp.where(near, -l, 0.0) for l in lower]
        inverse = [eye + p for p in power]
        power = [square(p.astype(BF16)).astype(BF16) for p in power]
        inverse = doubled(power, inverse, BASE * NH)
        low = [t.astype(BF16) for t in inverse]
        power = [
            -dot(t[:, :SUB], jnp.where(near, 0.0, l).astype(BF16)) for t, l in zip(low, lower)
        ]
        power = [p.astype(BF16) for p in power]
        stepped = [both(p, t) for p, t in zip(power, inverse)]
        inverse = doubled([p for p, _ in stepped], [t for _, t in stepped], CH // BASE)
        high = [split(t) for t in inverse]
        parts = [split(l) for l in lower]
        made = [dot(l[0][:, :SUB], jnp.concatenate([s[0], s[1]], 1)) for l, s in zip(parts, high)]
        rest = [dot(l[1][:, :SUB], s[0]) for l, s in zip(parts, high)]
        error = [eye - t - (m[:, :WIDE] + (m[:, WIDE:] + r)) for t, m, r in zip(inverse, made, rest)]
        inverse = [t + dot(s[0][:, :SUB], e.astype(BF16)) for t, s, e in zip(inverse, high, error)]
        solved = [dot(t[:, :SUB].astype(BF16), rhs[i]).astype(BF16) for i, t in zip(at, inverse)]
        change = [dot(k[:SUB], s, ((0,), (0,))) for k, s in zip(pairs, solved)]
        qs = [queries[i] for i in at]
        attend = [jnp.where(seen, dot(q.astype(BF16), k[:SUB], ((1,), (1,))), 0.0).astype(BF16) for q, k in zip(qs, pairs)]
        effect = [dot(a, s) for a, s in zip(attend, solved)]
        for i, g, q, e in zip(at, change, qs, effect):
            state_map[i + (slice(0, CH),)] = (q - e[:, :DK]).astype(BF16)
            state_map[i + (slice(CH, CH + DK),)] = g[:, :DK].astype(BF16)
            added[i] = g[:, DK:]
            out_add[i] = e[:, DK:]

    states = [jnp.zeros((DK, DK), F32) for _ in range(heads)]
    for c in range(blocks):
        for h in range(heads):
            moved = dot(state_map[h, c], states[h].astype(BF16))
            out = moved[:CH] + out_add[h, c]
            states[h] = states[h] - moved[CH:] + added[h, c]
            out = out * lax.rsqrt(jnp.mean(out * out, -1, keepdims=True) + EPSILON) * head_gain_ref[...]
            mixed[c * CH:(c + 1) * CH, h * DK:(h + 1) * DK] = out.astype(BF16)
    own = length // count
    rolled = jnp.concatenate([mixed[rows_at(place_ref[k], own), :] for k in range(count)], 0)
    result = dot(rolled, wo_ref[...]).astype(BF16)
    for k, o in enumerate((o0, o1, o2, o3)):
        o[...] = result[k * own:(k + 1) * own]


UNROLL = 8


def mixer(me, gain, x2, x3, weights, sums, head_gain, wo):
    count = gain.shape[0]
    length = x2.shape[0]
    heads = weights[0].shape[1] // DK
    blocks = length // CH
    own = length // count
    vmem = pl.BlockSpec(memory_space=pltpu.VMEM)
    return pl.pallas_call(
        lambda *refs: mixer_kernel(heads, *refs),
        out_shape=[jax.ShapeDtypeStruct((own, wo.shape[1]), BF16)] * count,
        in_specs=[pl.BlockSpec(memory_space=pltpu.SMEM)] + [vmem] * 12,
        out_specs=[vmem] * count,
        scratch_shapes=[
            pltpu.VMEM((heads, blocks, 2 * WIDE, DK), BF16),
            pltpu.VMEM((heads, blocks, SUB, DK), F32),
            pltpu.VMEM((heads, blocks, SUB, 2 * DK), BF16),
            pltpu.VMEM((heads, blocks, CH, DK), F32),
            pltpu.VMEM((heads, blocks, CH + DK, DK), BF16),
            pltpu.VMEM((heads, blocks, DK, DK), F32),
            pltpu.VMEM((heads, blocks, CH, DK), F32),
            pltpu.VMEM((length, heads * DK), BF16),
        ],
        compiler_params=pltpu.CompilerParams(vmem_limit_bytes=32 * MIB),
        cost_estimate=pl.CostEstimate(flops=2 * 10 ** 10, bytes_accessed=10 ** 7, transcendentals=0),
        name="mixer",
    )(me, gain, x2, x3, *weights, *sums, head_gain, wo)


def slots(ids_ref, experts, total):
    tokens = ids_ref.shape[1]
    capacity = total // experts
    label = iota((experts, tokens), 0)
    chosen = [(label == ids_ref[k:k + 1, :]).astype(F32) for k in range(2)]
    count = chosen[0] + chosen[1]
    before = (iota((tokens, tokens), 0) < iota((tokens, tokens), 1)).astype(BF16)
    earlier = dot(count.astype(BF16), before)
    spread = (iota((total, experts), 0) // capacity == iota((total, experts), 1)).astype(BF16)
    place = dot(spread, earlier.astype(BF16))
    fits = place == (iota((total, tokens), 0) % capacity).astype(F32)
    return chosen, [jnp.where(fits, dot(spread, c.astype(BF16)), 0.0) for c in chosen]


def ready_kernel(experts, place_ref, part_ref, x0, x1, x2, x3, ids_ref, base_ref, chosen_ref):
    own, part = part_ref.shape[0], x0.shape[1]
    for k, x in enumerate((x0, x1, x2, x3)):
        columns = rows_at(place_ref[k], part)
        base_ref[:, columns] = x[rows_at(place_ref[0], own), :].astype(F32)
    base_ref[...] = base_ref[...] + part_ref[...].astype(F32)
    _, chosen = slots(ids_ref, experts, chosen_ref.shape[0])
    chosen_ref[...] = (chosen[0] + chosen[1]).astype(BF16)


def ready(me, part, xs, ids, experts, capacity):
    own, width = part.shape
    vmem = pl.BlockSpec(memory_space=pltpu.VMEM)
    return pl.pallas_call(
        lambda *refs: ready_kernel(experts, *refs),
        out_shape=[
            jax.ShapeDtypeStruct((own, width), F32),
            jax.ShapeDtypeStruct((experts * capacity, own), BF16),
        ],
        in_specs=[pl.BlockSpec(memory_space=pltpu.SMEM)] + [vmem] * 6,
        out_specs=[vmem] * 2,
        compiler_params=pltpu.CompilerParams(vmem_limit_bytes=8 * MIB),
        cost_estimate=pl.CostEstimate(flops=2 * 10 ** 9, bytes_accessed=10 ** 6, transcendentals=0),
        name="ready",
    )(me, part, *xs, ids)


def route_kernel(base_ref, p1, p2, p3, gain_ref, chosen_ref, residual_ref, routed_ref, send_ref):
    arrived = [p[...].astype(F32) for p in (p1, p2, p3)]
    residual = (base_ref[...] + arrived[0]) + (arrived[1] + arrived[2])
    residual_ref[...] = residual
    mean = jnp.mean(residual * residual, -1, keepdims=True)
    routed = residual * lax.rsqrt(mean + EPSILON) * gain_ref[...]
    routed_ref[...] = routed
    send_ref[...] = dot(chosen_ref[...], routed.astype(BF16)).astype(BF16)


def route(base, parts, gain, chosen):
    own, width = base.shape
    vmem = pl.BlockSpec(memory_space=pltpu.VMEM)
    return pl.pallas_call(
        route_kernel,
        out_shape=[
            jax.ShapeDtypeStruct((own, width), F32),
            jax.ShapeDtypeStruct((own, width), F32),
            jax.ShapeDtypeStruct((chosen.shape[0], width), BF16),
        ],
        in_specs=[vmem] * 6,
        out_specs=[vmem] * 3,
        compiler_params=pltpu.CompilerParams(vmem_limit_bytes=8 * MIB),
        cost_estimate=pl.CostEstimate(flops=10 ** 9, bytes_accessed=10 ** 7, transcendentals=0),
        name="route",
    )(base, *parts, gain, chosen)


def weigh(routed_ref, router_ref, ids_ref, pick_ref, leading_ref):
    chosen, parts = slots(ids_ref, router_ref.shape[0], pick_ref.shape[1])
    tokens = routed_ref.shape[0]
    for k in range(2):
        pick_ref[k * tokens:(k + 1) * tokens, :] = jnp.transpose(parts[k]).astype(BF16)
    logits = lax.dot_general(
        router_ref[...], routed_ref[...], (((1,), (1,)), ((), ())),
        precision=lax.Precision.HIGHEST, preferred_element_type=F32,
    )
    gap = jnp.sum((chosen[0] - chosen[1]) * logits, 0, keepdims=True)
    leading = 1.0 / (1.0 + jnp.exp(-gap))
    leading_ref[...] = jnp.transpose(jnp.broadcast_to(leading, (128, tokens)))


def expert_kernel(rows_ref, gate_hbm, up_hbm, down_hbm, routed_ref, router_ref, ids_ref, out_ref, pick_ref,
                  leading_ref, gate_ref, up_ref, down_ref, hidden_ref, finished_ref, sems):
    total = rows_ref.shape[0]
    here, width, middle = gate_hbm.shape
    per = total // here
    experts = router_ref.shape[0]
    cap = pick_ref.shape[1] // experts
    deep, tall = width // PIECES, middle // PIECES
    copies, order = {}, []
    for e in range(here):
        for part, (source, target) in enumerate(((gate_hbm, gate_ref), (up_hbm, up_ref), (down_hbm, down_ref))):
            size = tall if part == 2 else deep
            for p in range(PIECES):
                at = (e, pl.ds(p * size, size))
                copies[e, part, p] = pltpu.make_async_copy(source.at[at], target.at[at], sems.at[e, part, p])
        for p in range(PIECES):
            order += [(e, 0, p), (e, 1, p)]
        order += [(e, 2, p) for p in range(PIECES)]
    for key in order[:FLIGHT]:
        copies[key].start()

    def take(*key):
        copies[key].wait()
        following = order.index(key) + FLIGHT
        if following < len(order):
            copies[order[following]].start()

    weigh(routed_ref, router_ref, ids_ref, pick_ref, leading_ref)
    r, c = iota((total, total), 0), iota((total, total), 1)

    def source(i):
        return (i % per) // cap * (here * cap) + i // per * cap + i % cap

    by_expert = (source(r) == c).astype(BF16)
    by_source = (source(c) == r).astype(BF16)
    rows = dot(by_expert, rows_ref[...]).astype(BF16)
    for e in range(here):
        mine = rows[e * per:(e + 1) * per]
        gate = up = 0.0
        for p in range(PIECES):
            at = slice(p * deep, (p + 1) * deep)
            take(e, 0, p)
            gate = gate + dot(mine[:, at], gate_ref[e, at])
            take(e, 1, p)
            up = up + dot(mine[:, at], up_ref[e, at])
        hidden_ref[...] = (gate / (1.0 + jnp.exp(-gate)) * up).astype(BF16)
        result = 0.0
        for p in range(PIECES):
            take(e, 2, p)
            at = slice(p * tall, (p + 1) * tall)
            result = result + dot(hidden_ref[:, at], down_ref[e, at])
        finished_ref[e * per:(e + 1) * per, :] = result.astype(BF16)
    for start in range(0, width, 512):
        at = slice(start, start + 512)
        out_ref[:, at] = dot(by_source, finished_ref[:, at]).astype(BF16)


PIECES = 4
FLIGHT = 10


def experts_here(rows, gate, up, down, routed, router, ids):
    here, width, middle = gate.shape
    per = rows.shape[0] // here
    tokens, experts = routed.shape[0], router.shape[0]
    capacity = 4 * tokens // experts
    vmem = pl.BlockSpec(memory_space=pltpu.VMEM)
    hbm = pl.BlockSpec(memory_space=pltpu.HBM)
    return pl.pallas_call(
        expert_kernel,
        out_shape=[
            jax.ShapeDtypeStruct(rows.shape, BF16),
            jax.ShapeDtypeStruct((2 * tokens, experts * capacity), BF16),
            jax.ShapeDtypeStruct((tokens, 128), F32),
        ],
        in_specs=[vmem] + [hbm] * 3 + [vmem] * 3,
        out_specs=[vmem] * 3,
        scratch_shapes=[
            pltpu.VMEM(gate.shape, BF16),
            pltpu.VMEM(up.shape, BF16),
            pltpu.VMEM(down.shape, BF16),
            pltpu.VMEM((per, middle), BF16),
            pltpu.VMEM(rows.shape, BF16),
            pltpu.SemaphoreType.DMA((here, 3, PIECES)),
        ],
        compiler_params=pltpu.CompilerParams(vmem_limit_bytes=46 * MIB),
        cost_estimate=pl.CostEstimate(flops=5 * 10 ** 9, bytes_accessed=10 ** 7, transcendentals=0),
        name="experts",
    )(rows, *[pltpu.with_memory_space_constraint(w, pltpu.HBM) for w in (gate, up, down)], routed, router, ids)


def combine_kernel(residual_ref, leading_ref, pick_ref, back_ref, out_ref):
    tokens = residual_ref.shape[0]
    picked = dot(pick_ref[...], back_ref[...])
    leading = leading_ref[:, 0:1]
    blended = leading * picked[:tokens] + (1.0 - leading) * picked[tokens:]
    out_ref[...] = (residual_ref[...] + blended).astype(BF16)


def combine(residual, leading, pick, back):
    vmem = pl.BlockSpec(memory_space=pltpu.VMEM)
    return pl.pallas_call(
        combine_kernel,
        out_shape=jax.ShapeDtypeStruct(residual.shape, BF16),
        in_specs=[vmem] * 4,
        out_specs=vmem,
        compiler_params=pltpu.CompilerParams(vmem_limit_bytes=16 * MIB),
        cost_estimate=pl.CostEstimate(flops=10 ** 9, bytes_accessed=10 ** 6, transcendentals=0),
        name="combine",
    )(residual, leading, pick, back)


def swapped(x, step, axes=("dp", "head")):
    owners, peers = (lax.axis_size(a) for a in axes)
    pairs = [(d * peers + z, d * peers + (z ^ step(d))) for d in range(owners) for z in range(peers)]
    return lax.ppermute(x, axes, pairs)


def near(owner):
    return 1 if owner >= EDGE else 3


def far(owner):
    return 3 if owner >= EDGE else 1


def across(owner):
    return 2


EDGE = 8
STEPS = (near, far, across)


def shards(tokens, mixer_gain, query_weight, key_weight, value_weight, beta_weight, head_gain, output_weight,
           expert_gain, router_weight, expert_ids, gate_weight, up_weight, down_weight):
    owners = lax.axis_size("dp")
    me = lax.axis_index("head").astype(jnp.int32)
    edge = lax.axis_index("dp") < EDGE
    one, three = jnp.where(edge, 3, 1), jnp.where(edge, 1, 3)
    me = jnp.stack([me, me ^ one, me ^ three, me ^ 2]).astype(jnp.int32)
    xs = [tokens] + [swapped(tokens, step) for step in STEPS]
    gain = mixer_gain.reshape(lax.axis_size("head"), -1)
    here = first(me, gain, tokens, query_weight, key_weight, value_weight, beta_weight.T, head_gain.reshape(1, -1),
                 output_weight)
    xs[0], weights, sums = here[0], here[1:5], here[7:]
    sums = more(me, gain, xs[1], weights, sums)
    parts = mixer(me, gain, xs[2], xs[3], weights, sums, here[5], here[6])
    arriving = [swapped(part, step) for part, step in zip(parts[1:], STEPS)]
    experts = router_weight.shape[1]
    capacity = 4 * parts[0].shape[0] // experts
    ids = expert_ids.T
    base, chosen = ready(me, parts[0], xs, ids, experts, capacity)
    residual, routed, outgoing = route(base, arriving, expert_gain.reshape(1, -1), chosen)
    width = outgoing.shape[1]

    def exchanged(rows):
        rows = rows.reshape(owners, -1, width)
        rows = lax.all_to_all(rows, "dp", split_axis=0, concat_axis=0, tiled=True)
        return rows.reshape(-1, width)

    result, pick, leading = experts_here(
        exchanged(outgoing), gate_weight, up_weight, down_weight, routed, router_weight.T, ids
    )
    return combine(residual, leading, pick, exchanged(result))


def solution(mesh):
    return jax.shard_map(
        shards,
        mesh=mesh,
        in_specs=(
            P("dp", "head"),
            P(),
            P(None, "head"),
            P(None, None, "head"),
            P(None, None, "head"),
            P(None, "head"),
            P(),
            P("head", None),
            P(),
            P(),
            P(("dp", "head"), None),
            P("dp", None, None),
            P("dp", None, None),
            P("dp", None, None),
        ),
        out_specs=P(("dp", "head"), None),
        check_vma=False,
    )
```

```python
import jax
import jax.numpy as jnp
from jax import lax
from jax.experimental import pallas as pl
from jax.experimental.pallas import tpu as pltpu
from jax.sharding import PartitionSpec as P

DK = 128
NH = 3
CH = 32
SUB = CH * NH
WIDE = 128
BASE = 4
EPSILON = 1e-06
F32 = jnp.float32
BF16 = jnp.bfloat16
MIB = 1 << 20


def dot(a, b, dims=((1,), (0,))):
    return lax.dot_general(a, b, (dims, ((), ())), preferred_element_type=F32)


def split(a):
    high = a.astype(BF16)
    return high, (a - high.astype(F32)).astype(BF16)


def dot3(a, b, dims=((1,), (0,))):
    return dot(a[0], b[0], dims) + (dot(a[0], b[1], dims) + dot(a[1], b[0], dims))


def iota(shape, dim):
    return lax.broadcasted_iota(jnp.int32, shape, dim)


def rows_at(block, size):
    return pl.ds(pl.multiple_of(block * size, size), size)


EDGE = 8
STEPS = ((3, 1, 2), (1, 3, 2))


def step(owner_ref, slot):
    return jnp.where(owner_ref[0] < EDGE, STEPS[1][slot], STEPS[0][slot])


def source_of(me_ref, owner_ref, slot, count):
    return lax.rem(me_ref[0] + (count - step(owner_ref, slot)), count)


def gained(x_ref, gain_ref, source):
    wide = x_ref[...].astype(F32)
    return (wide * gain_ref[pl.ds(source, 1), :]).astype(BF16), jnp.sum(wide * wide, -1, keepdims=True)


def products(x, source, wq_ref, wk_ref, wv_ref, wb_ref):
    rows = rows_at(source, x.shape[1])
    yield dot(x, wq_ref[rows, :])
    for ref in (wk_ref, wv_ref):
        for m in range(NH):
            yield dot(x, ref[m, rows, :])
    yield dot(x, wb_ref[:, rows], ((1,), (1,)))


def first_kernel(me_ref, owner_ref, gain_ref, *refs):
    count = (len(refs) - 4) // 2
    here, there = refs[:count], refs[count:2 * count]
    sums_ref, beta_ref, square_ref, sems = refs[2 * count:]
    copies = [pltpu.make_async_copy(h, t, sems.at[i]) for i, (h, t) in enumerate(zip(here, there))]
    for copy in copies:
        copy.start()
    for copy in copies:
        copy.wait()
    x, square_ref[...] = gained(there[0], gain_ref, me_ref[0])
    for i, product in enumerate(products(x, me_ref[0], *there[1:5])):
        if i < 1 + 2 * NH:
            sums_ref[i] = product
        else:
            beta_ref[...] = product


def first(me, owner, gain, tokens, wq, wk, wv, wb, *others):
    moved = (tokens, wq, wk, wv, wb, *others)
    length = tokens.shape[0]
    vmem = pl.BlockSpec(memory_space=pltpu.VMEM)
    made = [
        pltpu.VMEM((1 + 2 * NH, length, wq.shape[1]), F32),
        pltpu.VMEM((length, wb.shape[0]), F32),
        pltpu.VMEM((length, 1), F32),
    ]
    return pl.pallas_call(
        first_kernel,
        out_shape=[pltpu.VMEM(w.shape, w.dtype) for w in moved] + made,
        in_specs=[pl.BlockSpec(memory_space=pltpu.SMEM)] * 2 + [vmem] + [pl.BlockSpec(memory_space=pltpu.HBM)] * len(moved),
        out_specs=[vmem] * (len(moved) + 3),
        scratch_shapes=[pltpu.SemaphoreType.DMA((len(moved),))],
        compiler_params=pltpu.CompilerParams(vmem_limit_bytes=4 * MIB),
        cost_estimate=pl.CostEstimate(flops=2 * 10 ** 9, bytes_accessed=10 ** 6, transcendentals=0),
        name="first",
    )(me, owner, gain, *[pltpu.with_memory_space_constraint(w, pltpu.HBM) for w in moved])


def more_kernel(slot, me_ref, owner_ref, gain_ref, x_ref, wq_ref, wk_ref, wv_ref, wb_ref, sums_ref, beta_ref, square_ref,
                new_sums_ref, new_beta_ref, new_square_ref):
    source = source_of(me_ref, owner_ref, slot, gain_ref.shape[0])
    x, square = gained(x_ref, gain_ref, source)
    new_square_ref[...] = square_ref[...] + square
    for i, product in enumerate(products(x, source, wq_ref, wk_ref, wv_ref, wb_ref)):
        if i < 1 + 2 * NH:
            new_sums_ref[i] = sums_ref[i] + product
        else:
            new_beta_ref[...] = beta_ref[...] + product


def more(slot, me, owner, gain, x, weights, sums):
    vmem = pl.BlockSpec(memory_space=pltpu.VMEM)
    return pl.pallas_call(
        lambda *refs: more_kernel(slot, *refs),
        out_shape=[pltpu.VMEM(a.shape, a.dtype) for a in sums],
        in_specs=[pl.BlockSpec(memory_space=pltpu.SMEM)] * 2 + [vmem] * 9,
        out_specs=[vmem] * 3,
        input_output_aliases={8: 0, 9: 1, 10: 2},
        compiler_params=pltpu.CompilerParams(vmem_limit_bytes=4 * MIB),
        cost_estimate=pl.CostEstimate(flops=10 ** 9, bytes_accessed=10 ** 6, transcendentals=0),
        name="more",
    )(me, owner, gain, x, *weights, *sums)


def mixer_kernel(heads, me_ref, owner_ref, gain_ref, x_ref, wq_ref, wk_ref, wv_ref, wb_ref, sums_ref, beta_ref, square_ref,
                 head_gain_ref, wo_ref, o0, o1, o2, o3, keys, beta_keys, rhs, queries, state_map, added, out_add, mixed):
    count, part = gain_ref.shape
    length = x_ref.shape[0]
    source = source_of(me_ref, owner_ref, count - 2, count)
    x, square = gained(x_ref, gain_ref, source)
    scale = lax.rsqrt((square_ref[...] + square) / (count * part) + EPSILON)
    last = products(x, source, wq_ref, wk_ref, wv_ref, wb_ref)
    whole = [(sums_ref[i] + next(last)) * scale for i in range(1 + 2 * NH)]
    beta = (beta_ref[...] + next(last)) * scale
    beta = 2.0 / (1.0 + jnp.exp(-beta))
    blocks = length // CH
    query = whole[0]
    for h in range(heads):
        q = query[:, h * DK:(h + 1) * DK]
        q = q * lax.rsqrt(jnp.sum(q * q, -1, keepdims=True) + EPSILON) * DK ** (-0.5)
        queries[h] = q.reshape(blocks, CH, DK)
    for edge in (SUB, WIDE + SUB):
        keys[:, :, edge:edge + WIDE - SUB, :] = jnp.zeros((heads, blocks, WIDE - SUB, DK), BF16)
    for m in range(NH):
        key = whole[1 + m]
        value = whole[1 + NH + m]
        for h in range(heads):
            b = beta[:, h * NH + m:h * NH + m + 1]
            k = key[:, h * DK:(h + 1) * DK]
            k = k * lax.rsqrt(jnp.sum(k * k, -1, keepdims=True) + EPSILON)
            high, low = split(k)
            keys[h, :, m * CH:(m + 1) * CH, :] = high.reshape(blocks, CH, DK)
            keys[h, :, WIDE + m * CH:WIDE + (m + 1) * CH, :] = low.reshape(blocks, CH, DK)
            rhs[h, :, m * CH:(m + 1) * CH, :DK] = (k * b).astype(BF16).reshape(blocks, CH, DK)
            rhs[h, :, m * CH:(m + 1) * CH, DK:] = (value[:, h * DK:(h + 1) * DK] * b).astype(BF16).reshape(blocks, CH, DK)
            beta_keys[h, :, m * CH:(m + 1) * CH, :] = jnp.broadcast_to(b, (length, DK)).reshape(blocks, CH, DK)

    row, col = iota((SUB, WIDE), 0), iota((SUB, WIDE), 1)
    inside = col < SUB
    row_t, col_t = row % CH, col % CH
    causal = inside & ((col_t < row_t) | ((col_t == row_t) & (col < row)))
    near = row_t // BASE == col_t // BASE
    eye = (row == col).astype(F32)
    seen = iota((CH, SUB), 1) % CH <= iota((CH, SUB), 0)
    blank = jnp.zeros((WIDE - SUB, WIDE), F32)

    def square(p):
        return dot(p[:, :SUB], p)

    def both(p, t):
        made = dot(p[:, :SUB], jnp.concatenate([p, t.astype(BF16)], 1))
        return made[:, :WIDE].astype(BF16), t + made[:, WIDE:]

    def doubled(powers, sums, terms):
        span = 2
        while 2 * span < terms:
            stepped = [both(p, t) for p, t in zip(powers, sums)]
            powers, sums = [p for p, _ in stepped], [t for _, t in stepped]
            span *= 2
        return [t + dot(p[:, :SUB], t.astype(BF16)) for p, t in zip(powers, sums)]

    unroll = UNROLL
    for start in range(0, blocks, unroll):
        at = [(h, c) for c in range(start, start + unroll) for h in range(heads)]
        pairs = [keys[i] for i in at]
        alike = [dot(k[:SUB], k, ((1,), (1,))) for k in pairs]
        alike = [
            a[:, :WIDE] + a[:, WIDE:] + jnp.transpose(jnp.concatenate([a[:, WIDE:], blank], 0))[:SUB] for a in alike
        ]
        lower = [jnp.where(causal, a * beta_keys[i], 0.0) for i, a in zip(at, alike)]
        power = [jnp.where(near, -l, 0.0) for l in lower]
        inverse = [eye + p for p in power]
        power = [square(p.astype(BF16)).astype(BF16) for p in power]
        inverse = doubled(power, inverse, BASE * NH)
        low = [t.astype(BF16) for t in inverse]
        power = [
            -dot(t[:, :SUB], jnp.where(near, 0.0, l).astype(BF16)) for t, l in zip(low, lower)
        ]
        power = [p.astype(BF16) for p in power]
        stepped = [both(p, t) for p, t in zip(power, inverse)]
        inverse = doubled([p for p, _ in stepped], [t for _, t in stepped], CH // BASE)
        high = [split(t) for t in inverse]
        parts = [split(l) for l in lower]
        none, gap = jnp.zeros((SUB, WIDE), BF16), jnp.zeros((WIDE - SUB, 2 * WIDE), BF16)
        made = [
            dot(
                jnp.concatenate([l[0], l[1]], 1),
                jnp.concatenate([jnp.concatenate(s, 1), gap, jnp.concatenate([s[0], none], 1), gap], 0),
            )
            for l, s in zip(parts, high)
        ]
        error = [eye - t - (m[:, :WIDE] + m[:, WIDE:]) for t, m in zip(inverse, made)]
        inverse = [t + dot(s[0][:, :SUB], e.astype(BF16)) for t, s, e in zip(inverse, high, error)]
        solved = [dot(t[:, :SUB].astype(BF16), rhs[i]).astype(BF16) for i, t in zip(at, inverse)]
        change = [dot(k[:SUB], s, ((0,), (0,))) for k, s in zip(pairs, solved)]
        qs = [queries[i] for i in at]
        attend = [jnp.where(seen, dot(q.astype(BF16), k[:SUB], ((1,), (1,))), 0.0).astype(BF16) for q, k in zip(qs, pairs)]
        effect = [dot(a, s) for a, s in zip(attend, solved)]
        for i, g, q, e in zip(at, change, qs, effect):
            state_map[i + (slice(0, CH),)] = (q - e[:, :DK]).astype(BF16)
            state_map[i + (slice(CH, CH + DK),)] = g[:, :DK].astype(BF16)
            added[i] = g[:, DK:]
            out_add[i] = e[:, DK:]

    states = [jnp.zeros((DK, DK), F32) for _ in range(heads)]
    for c in range(blocks):
        for h in range(heads):
            moved = dot(state_map[h, c], states[h].astype(BF16))
            out = moved[:CH] + out_add[h, c]
            states[h] = states[h] - moved[CH:] + added[h, c]
            out = out * lax.rsqrt(jnp.mean(out * out, -1, keepdims=True) + EPSILON) * head_gain_ref[...]
            mixed[c * CH:(c + 1) * CH, h * DK:(h + 1) * DK] = out.astype(BF16)
    own = length // count
    targets = [me_ref[0]] + [lax.rem(me_ref[0] + step(owner_ref, k), count) for k in range(count - 1)]
    rolled = jnp.concatenate([mixed[rows_at(block, own), :] for block in targets], 0)
    result = dot(rolled, wo_ref[...]).astype(BF16)
    for k, o in enumerate((o0, o1, o2, o3)):
        o[...] = result[k * own:(k + 1) * own]


UNROLL = 8


def mixer(me, owner, gain, x, weights, sums, head_gain, wo):
    count = gain.shape[0]
    length = x.shape[0]
    heads = weights[0].shape[1] // DK
    blocks = length // CH
    own = length // count
    vmem = pl.BlockSpec(memory_space=pltpu.VMEM)
    return pl.pallas_call(
        lambda *refs: mixer_kernel(heads, *refs),
        out_shape=[jax.ShapeDtypeStruct((own, wo.shape[1]), BF16)] * count,
        in_specs=[pl.BlockSpec(memory_space=pltpu.SMEM)] * 2 + [vmem] * 11,
        out_specs=[vmem] * count,
        scratch_shapes=[
            pltpu.VMEM((heads, blocks, 2 * WIDE, DK), BF16),
            pltpu.VMEM((heads, blocks, SUB, DK), F32),
            pltpu.VMEM((heads, blocks, SUB, 2 * DK), BF16),
            pltpu.VMEM((heads, blocks, CH, DK), F32),
            pltpu.VMEM((heads, blocks, CH + DK, DK), BF16),
            pltpu.VMEM((heads, blocks, DK, DK), F32),
            pltpu.VMEM((heads, blocks, CH, DK), F32),
            pltpu.VMEM((length, heads * DK), BF16),
        ],
        compiler_params=pltpu.CompilerParams(vmem_limit_bytes=32 * MIB),
        cost_estimate=pl.CostEstimate(flops=2 * 10 ** 10, bytes_accessed=10 ** 7, transcendentals=0),
        name="mixer",
    )(me, owner, gain, x, *weights, *sums, head_gain, wo)


def slots(ids_ref, experts, total):
    tokens = ids_ref.shape[1]
    capacity = total // experts
    label = iota((experts, tokens), 0)
    chosen = [(label == ids_ref[k:k + 1, :]).astype(F32) for k in range(2)]
    count = chosen[0] + chosen[1]
    before = (iota((tokens, tokens), 0) < iota((tokens, tokens), 1)).astype(BF16)
    earlier = dot(count.astype(BF16), before)
    spread = (iota((total, experts), 0) // capacity == iota((total, experts), 1)).astype(BF16)
    place = dot(spread, earlier.astype(BF16))
    fits = place == (iota((total, tokens), 0) % capacity).astype(F32)
    return chosen, [jnp.where(fits, dot(spread, c.astype(BF16)), 0.0) for c in chosen]


def ready_kernel(experts, me_ref, owner_ref, part_ref, x0, x1, x2, x3, ids_ref, base_ref, chosen_ref):
    own, part = part_ref.shape[0], x0.shape[1]
    for k, x in enumerate((x0, x1, x2, x3)):
        block = me_ref[0] if k == 0 else source_of(me_ref, owner_ref, k - 1, 4)
        base_ref[:, rows_at(block, part)] = x[rows_at(me_ref[0], own), :].astype(F32)
    base_ref[...] = base_ref[...] + part_ref[...].astype(F32)
    _, chosen = slots(ids_ref, experts, chosen_ref.shape[0])
    chosen_ref[...] = (chosen[0] + chosen[1]).astype(BF16)


def ready(me, owner, part, xs, ids, experts, capacity):
    own, width = part.shape
    vmem = pl.BlockSpec(memory_space=pltpu.VMEM)
    return pl.pallas_call(
        lambda *refs: ready_kernel(experts, *refs),
        out_shape=[
            jax.ShapeDtypeStruct((own, width), F32),
            jax.ShapeDtypeStruct((experts * capacity, own), BF16),
        ],
        in_specs=[pl.BlockSpec(memory_space=pltpu.SMEM)] * 2 + [vmem] * 6,
        out_specs=[vmem] * 2,
        compiler_params=pltpu.CompilerParams(vmem_limit_bytes=8 * MIB),
        cost_estimate=pl.CostEstimate(flops=2 * 10 ** 9, bytes_accessed=10 ** 6, transcendentals=0),
        name="ready",
    )(me, owner, part, *xs, ids)


def route_kernel(base_ref, p1, p2, p3, gain_ref, chosen_ref, residual_ref, routed_ref, send_ref):
    arrived = [p[...].astype(F32) for p in (p1, p2, p3)]
    residual = (base_ref[...] + arrived[0]) + (arrived[1] + arrived[2])
    residual_ref[...] = residual
    mean = jnp.mean(residual * residual, -1, keepdims=True)
    routed = residual * lax.rsqrt(mean + EPSILON) * gain_ref[...]
    routed_ref[...] = routed
    send_ref[...] = dot(chosen_ref[...], routed.astype(BF16)).astype(BF16)


def route(base, parts, gain, chosen):
    own, width = base.shape
    vmem = pl.BlockSpec(memory_space=pltpu.VMEM)
    return pl.pallas_call(
        route_kernel,
        out_shape=[
            jax.ShapeDtypeStruct((own, width), F32),
            jax.ShapeDtypeStruct((own, width), F32),
            jax.ShapeDtypeStruct((chosen.shape[0], width), BF16),
        ],
        in_specs=[vmem] * 6,
        out_specs=[vmem] * 3,
        compiler_params=pltpu.CompilerParams(vmem_limit_bytes=8 * MIB),
        cost_estimate=pl.CostEstimate(flops=10 ** 9, bytes_accessed=10 ** 7, transcendentals=0),
        name="route",
    )(base, *parts, gain, chosen)


def weigh(routed_ref, router_ref, ids_ref, pick_ref, leading_ref):
    chosen, parts = slots(ids_ref, router_ref.shape[0], pick_ref.shape[1])
    tokens = routed_ref.shape[0]
    for k in range(2):
        pick_ref[k * tokens:(k + 1) * tokens, :] = jnp.transpose(parts[k]).astype(BF16)
    logits = lax.dot_general(
        router_ref[...], routed_ref[...], (((1,), (1,)), ((), ())),
        precision=lax.Precision.HIGHEST, preferred_element_type=F32,
    )
    gap = jnp.sum((chosen[0] - chosen[1]) * logits, 0, keepdims=True)
    leading = 1.0 / (1.0 + jnp.exp(-gap))
    leading_ref[...] = jnp.transpose(jnp.broadcast_to(leading, (128, tokens)))


def expert_kernel(rows_ref, gate_hbm, up_hbm, down_hbm, routed_ref, router_ref, ids_ref, out_ref, pick_ref,
                  leading_ref, gate_ref, up_ref, down_ref, hidden_ref, finished_ref, sems):
    total = rows_ref.shape[0]
    here, width, middle = gate_hbm.shape
    per = total // here
    experts = router_ref.shape[0]
    cap = pick_ref.shape[1] // experts
    deep, tall = width // PIECES, middle // PIECES
    copies, order = {}, []
    for e in range(here):
        for part, (source, target) in enumerate(((gate_hbm, gate_ref), (up_hbm, up_ref), (down_hbm, down_ref))):
            size = tall if part == 2 else deep
            for p in range(PIECES):
                at = (e, pl.ds(p * size, size))
                copies[e, part, p] = pltpu.make_async_copy(source.at[at], target.at[at], sems.at[e, part, p])
        for p in range(PIECES):
            order += [(e, 0, p), (e, 1, p)]
        order += [(e, 2, p) for p in range(PIECES)]
    for key in order[:FLIGHT]:
        copies[key].start()

    def take(*key):
        copies[key].wait()
        following = order.index(key) + FLIGHT
        if following < len(order):
            copies[order[following]].start()

    weigh(routed_ref, router_ref, ids_ref, pick_ref, leading_ref)
    r, c = iota((total, total), 0), iota((total, total), 1)

    def source(i):
        return (i % per) // cap * (here * cap) + i // per * cap + i % cap

    by_expert = (source(r) == c).astype(BF16)
    by_source = (source(c) == r).astype(BF16)
    rows = dot(by_expert, rows_ref[...]).astype(BF16)
    for e in range(here):
        mine = rows[e * per:(e + 1) * per]
        gate = up = 0.0
        for p in range(PIECES):
            at = slice(p * deep, (p + 1) * deep)
            take(e, 0, p)
            gate = gate + dot(mine[:, at], gate_ref[e, at])
            take(e, 1, p)
            up = up + dot(mine[:, at], up_ref[e, at])
        hidden_ref[...] = (gate / (1.0 + jnp.exp(-gate)) * up).astype(BF16)
        result = 0.0
        for p in range(PIECES):
            take(e, 2, p)
            at = slice(p * tall, (p + 1) * tall)
            result = result + dot(hidden_ref[:, at], down_ref[e, at])
        finished_ref[e * per:(e + 1) * per, :] = result.astype(BF16)
    for start in range(0, width, 512):
        at = slice(start, start + 512)
        out_ref[:, at] = dot(by_source, finished_ref[:, at]).astype(BF16)


PIECES = 4
FLIGHT = 10


def experts_here(rows, gate, up, down, routed, router, ids):
    here, width, middle = gate.shape
    per = rows.shape[0] // here
    tokens, experts = routed.shape[0], router.shape[0]
    capacity = 4 * tokens // experts
    vmem = pl.BlockSpec(memory_space=pltpu.VMEM)
    hbm = pl.BlockSpec(memory_space=pltpu.HBM)
    return pl.pallas_call(
        expert_kernel,
        out_shape=[
            jax.ShapeDtypeStruct(rows.shape, BF16),
            jax.ShapeDtypeStruct((2 * tokens, experts * capacity), BF16),
            jax.ShapeDtypeStruct((tokens, 128), F32),
        ],
        in_specs=[vmem] + [hbm] * 3 + [vmem] * 3,
        out_specs=[vmem] * 3,
        scratch_shapes=[
            pltpu.VMEM(gate.shape, BF16),
            pltpu.VMEM(up.shape, BF16),
            pltpu.VMEM(down.shape, BF16),
            pltpu.VMEM((per, middle), BF16),
            pltpu.VMEM(rows.shape, BF16),
            pltpu.SemaphoreType.DMA((here, 3, PIECES)),
        ],
        compiler_params=pltpu.CompilerParams(vmem_limit_bytes=46 * MIB),
        cost_estimate=pl.CostEstimate(flops=5 * 10 ** 9, bytes_accessed=10 ** 7, transcendentals=0),
        name="experts",
    )(rows, *[pltpu.with_memory_space_constraint(w, pltpu.HBM) for w in (gate, up, down)], routed, router, ids)


def combine_kernel(residual_ref, leading_ref, pick_ref, back_ref, out_ref):
    tokens = residual_ref.shape[0]
    picked = dot(pick_ref[...], back_ref[...])
    leading = leading_ref[:, 0:1]
    blended = leading * picked[:tokens] + (1.0 - leading) * picked[tokens:]
    out_ref[...] = (residual_ref[...] + blended).astype(BF16)


def combine(residual, leading, pick, back):
    vmem = pl.BlockSpec(memory_space=pltpu.VMEM)
    return pl.pallas_call(
        combine_kernel,
        out_shape=jax.ShapeDtypeStruct(residual.shape, BF16),
        in_specs=[vmem] * 4,
        out_specs=vmem,
        compiler_params=pltpu.CompilerParams(vmem_limit_bytes=16 * MIB),
        cost_estimate=pl.CostEstimate(flops=10 ** 9, bytes_accessed=10 ** 6, transcendentals=0),
        name="combine",
    )(residual, leading, pick, back)


def passed(x, slot, axes=("dp", "head")):
    owners, peers = (lax.axis_size(a) for a in axes)
    pairs = [(d * peers + z, d * peers + (z + STEPS[d < EDGE][slot]) % peers) for d in range(owners) for z in range(peers)]
    return lax.ppermute(x, axes, pairs)


def shards(tokens, mixer_gain, query_weight, key_weight, value_weight, beta_weight, head_gain, output_weight,
           expert_gain, router_weight, expert_ids, gate_weight, up_weight, down_weight):
    owners = lax.axis_size("dp")
    me = lax.axis_index("head").reshape(1).astype(jnp.int32)
    owner = lax.axis_index("dp").reshape(1).astype(jnp.int32)
    xs = [tokens] + [passed(tokens, slot) for slot in range(3)]
    gain = mixer_gain.reshape(lax.axis_size("head"), -1)
    here = first(me, owner, gain, tokens, query_weight, key_weight, value_weight, beta_weight.T, head_gain.reshape(1, -1),
                 output_weight)
    xs[0], weights, sums = here[0], here[1:5], here[7:]
    for slot in (0, 1):
        sums = more(slot, me, owner, gain, xs[slot + 1], weights, sums)
    parts = mixer(me, owner, gain, xs[3], weights, sums, here[5], here[6])
    arriving = [passed(part, slot) for slot, part in enumerate(parts[1:])]
    experts = router_weight.shape[1]
    capacity = 4 * parts[0].shape[0] // experts
    ids = expert_ids.T
    base, chosen = ready(me, owner, parts[0], xs, ids, experts, capacity)
    residual, routed, outgoing = route(base, arriving, expert_gain.reshape(1, -1), chosen)
    width = outgoing.shape[1]

    def exchanged(rows):
        rows = rows.reshape(owners, -1, width)
        rows = lax.all_to_all(rows, "dp", split_axis=0, concat_axis=0, tiled=True)
        return rows.reshape(-1, width)

    result, pick, leading = experts_here(
        exchanged(outgoing), gate_weight, up_weight, down_weight, routed, router_weight.T, ids
    )
    return combine(residual, leading, pick, exchanged(result))


def solution(mesh):
    return jax.shard_map(
        shards,
        mesh=mesh,
        in_specs=(
            P("dp", "head"),
            P(),
            P(None, "head"),
            P(None, None, "head"),
            P(None, None, "head"),
            P(None, "head"),
            P(),
            P("head", None),
            P(),
            P(),
            P(("dp", "head"), None),
            P("dp", None, None),
            P("dp", None, None),
            P("dp", None, None),
        ),
        out_specs=P(("dp", "head"), None),
        check_vma=False,
    )
```

```python
import jax
import jax.numpy as jnp
from jax import lax
from jax.experimental import pallas as pl
from jax.experimental.pallas import tpu as pltpu
from jax.sharding import PartitionSpec as P

DK = 128
NH = 3
CH = 32
SUB = CH * NH
WIDE = 128
BASE = 4
EPSILON = 1e-06
F32 = jnp.float32
BF16 = jnp.bfloat16
MIB = 1 << 20


def dot(a, b, dims=((1,), (0,))):
    return lax.dot_general(a, b, (dims, ((), ())), preferred_element_type=F32)


def split(a):
    high = a.astype(BF16)
    return high, (a - high.astype(F32)).astype(BF16)


def dot3(a, b, dims=((1,), (0,))):
    return dot(a[0], b[0], dims) + (dot(a[0], b[1], dims) + dot(a[1], b[0], dims))


def iota(shape, dim):
    return lax.broadcasted_iota(jnp.int32, shape, dim)


def rows_at(block, size):
    return pl.ds(pl.multiple_of(block * size, size), size)


NEAR = (1, 3)
SENT = (1, 2, 3)


def source_of(me_ref, shift, count):
    return lax.rem(me_ref[0] + (count - shift), count)


def gained(x_ref, gain_ref, source):
    wide = x_ref[...].astype(F32)
    return (wide * gain_ref[pl.ds(source, 1), :]).astype(BF16), jnp.sum(wide * wide, -1, keepdims=True)


def products(x, source, wq_ref, wk_ref, wv_ref, wb_ref):
    rows = rows_at(source, x.shape[1])
    yield dot(x, wq_ref[rows, :])
    for ref in (wk_ref, wv_ref):
        for m in range(NH):
            yield dot(x, ref[m, rows, :])
    yield dot(x, wb_ref[:, rows], ((1,), (1,)))


def first_kernel(me_ref, gain_ref, *refs):
    count = (len(refs) - 4) // 2
    here, there = refs[:count], refs[count:2 * count]
    sums_ref, beta_ref, square_ref, sems = refs[2 * count:]
    copies = [pltpu.make_async_copy(h, t, sems.at[i]) for i, (h, t) in enumerate(zip(here, there))]
    for copy in copies:
        copy.start()
    for copy in copies:
        copy.wait()
    x, square_ref[...] = gained(there[0], gain_ref, me_ref[0])
    for i, product in enumerate(products(x, me_ref[0], *there[1:5])):
        if i < 1 + 2 * NH:
            sums_ref[i] = product
        else:
            beta_ref[...] = product


def first(me, gain, tokens, wq, wk, wv, wb, *others):
    moved = (tokens, wq, wk, wv, wb, *others)
    length = tokens.shape[0]
    vmem = pl.BlockSpec(memory_space=pltpu.VMEM)
    made = [
        pltpu.VMEM((1 + 2 * NH, length, wq.shape[1]), F32),
        pltpu.VMEM((length, wb.shape[0]), F32),
        pltpu.VMEM((length, 1), F32),
    ]
    return pl.pallas_call(
        first_kernel,
        out_shape=[pltpu.VMEM(w.shape, w.dtype) for w in moved] + made,
        in_specs=[pl.BlockSpec(memory_space=pltpu.SMEM), vmem] + [pl.BlockSpec(memory_space=pltpu.HBM)] * len(moved),
        out_specs=[vmem] * (len(moved) + 3),
        scratch_shapes=[pltpu.SemaphoreType.DMA((len(moved),))],
        compiler_params=pltpu.CompilerParams(vmem_limit_bytes=4 * MIB),
        cost_estimate=pl.CostEstimate(flops=2 * 10 ** 9, bytes_accessed=10 ** 6, transcendentals=0),
        name="first",
    )(me, gain, *[pltpu.with_memory_space_constraint(w, pltpu.HBM) for w in moved])


def more_kernel(shift, me_ref, gain_ref, x_ref, wq_ref, wk_ref, wv_ref, wb_ref, sums_ref, beta_ref, square_ref,
                new_sums_ref, new_beta_ref, new_square_ref):
    source = source_of(me_ref, shift, gain_ref.shape[0])
    x, square = gained(x_ref, gain_ref, source)
    new_square_ref[...] = square_ref[...] + square
    for i, product in enumerate(products(x, source, wq_ref, wk_ref, wv_ref, wb_ref)):
        if i < 1 + 2 * NH:
            new_sums_ref[i] = sums_ref[i] + product
        else:
            new_beta_ref[...] = beta_ref[...] + product


def more(shift, me, gain, x, weights, sums):
    vmem = pl.BlockSpec(memory_space=pltpu.VMEM)
    return pl.pallas_call(
        lambda *refs: more_kernel(shift, *refs),
        out_shape=[pltpu.VMEM(a.shape, a.dtype) for a in sums],
        in_specs=[pl.BlockSpec(memory_space=pltpu.SMEM)] + [vmem] * 9,
        out_specs=[vmem] * 3,
        input_output_aliases={7: 0, 8: 1, 9: 2},
        compiler_params=pltpu.CompilerParams(vmem_limit_bytes=4 * MIB),
        cost_estimate=pl.CostEstimate(flops=10 ** 9, bytes_accessed=10 ** 6, transcendentals=0),
        name="more",
    )(me, gain, x, *weights, *sums)


def mixer_kernel(heads, me_ref, gain_ref, top_ref, bottom_ref, wq_ref, wk_ref, wv_ref, wb_ref, sums_ref, beta_ref, square_ref,
                 head_gain_ref, wo_ref, o0, o1, o2, o3, keys, beta_keys, rhs, queries, state_map, added, out_add, mixed):
    count, part = gain_ref.shape
    length = 2 * top_ref.shape[0]
    source = source_of(me_ref, count // 2, count)
    x, square = gained(jnp.concatenate([top_ref[...], bottom_ref[...]], 0), gain_ref, source)
    scale = lax.rsqrt((square_ref[...] + square) / (count * part) + EPSILON)
    last = products(x, source, wq_ref, wk_ref, wv_ref, wb_ref)
    whole = [(sums_ref[i] + next(last)) * scale for i in range(1 + 2 * NH)]
    beta = (beta_ref[...] + next(last)) * scale
    beta = 2.0 / (1.0 + jnp.exp(-beta))
    blocks = length // CH
    query = whole[0]
    for h in range(heads):
        q = query[:, h * DK:(h + 1) * DK]
        q = q * lax.rsqrt(jnp.sum(q * q, -1, keepdims=True) + EPSILON) * DK ** (-0.5)
        queries[h] = q.reshape(blocks, CH, DK)
    for edge in (SUB, WIDE + SUB):
        keys[:, :, edge:edge + WIDE - SUB, :] = jnp.zeros((heads, blocks, WIDE - SUB, DK), BF16)
    for m in range(NH):
        key = whole[1 + m]
        value = whole[1 + NH + m]
        for h in range(heads):
            b = beta[:, h * NH + m:h * NH + m + 1]
            k = key[:, h * DK:(h + 1) * DK]
            k = k * lax.rsqrt(jnp.sum(k * k, -1, keepdims=True) + EPSILON)
            high, low = split(k)
            keys[h, :, m * CH:(m + 1) * CH, :] = high.reshape(blocks, CH, DK)
            keys[h, :, WIDE + m * CH:WIDE + (m + 1) * CH, :] = low.reshape(blocks, CH, DK)
            rhs[h, :, m * CH:(m + 1) * CH, :DK] = (k * b).astype(BF16).reshape(blocks, CH, DK)
            rhs[h, :, m * CH:(m + 1) * CH, DK:] = (value[:, h * DK:(h + 1) * DK] * b).astype(BF16).reshape(blocks, CH, DK)
            beta_keys[h, :, m * CH:(m + 1) * CH, :] = jnp.broadcast_to(b, (length, DK)).reshape(blocks, CH, DK)

    row, col = iota((SUB, WIDE), 0), iota((SUB, WIDE), 1)
    inside = col < SUB
    row_t, col_t = row % CH, col % CH
    causal = inside & ((col_t < row_t) | ((col_t == row_t) & (col < row)))
    near = row_t // BASE == col_t // BASE
    eye = (row == col).astype(F32)
    seen = iota((CH, SUB), 1) % CH <= iota((CH, SUB), 0)
    blank = jnp.zeros((WIDE - SUB, WIDE), F32)

    def square(p):
        return dot(p[:, :SUB], p)

    def both(p, t):
        made = dot(p[:, :SUB], jnp.concatenate([p, t.astype(BF16)], 1))
        return made[:, :WIDE].astype(BF16), t + made[:, WIDE:]

    def doubled(powers, sums, terms):
        span = 2
        while 2 * span < terms:
            stepped = [both(p, t) for p, t in zip(powers, sums)]
            powers, sums = [p for p, _ in stepped], [t for _, t in stepped]
            span *= 2
        return [t + dot(p[:, :SUB], t.astype(BF16)) for p, t in zip(powers, sums)]

    unroll = UNROLL
    for start in range(0, blocks, unroll):
        at = [(h, c) for c in range(start, start + unroll) for h in range(heads)]
        pairs = [keys[i] for i in at]
        alike = [dot(k[:SUB], k, ((1,), (1,))) for k in pairs]
        alike = [
            a[:, :WIDE] + a[:, WIDE:] + jnp.transpose(jnp.concatenate([a[:, WIDE:], blank], 0))[:SUB] for a in alike
        ]
        lower = [jnp.where(causal, a * beta_keys[i], 0.0) for i, a in zip(at, alike)]
        power = [jnp.where(near, -l, 0.0) for l in lower]
        inverse = [eye + p for p in power]
        power = [square(p.astype(BF16)).astype(BF16) for p in power]
        inverse = doubled(power, inverse, BASE * NH)
        low = [t.astype(BF16) for t in inverse]
        power = [
            -dot(t[:, :SUB], jnp.where(near, 0.0, l).astype(BF16)) for t, l in zip(low, lower)
        ]
        power = [p.astype(BF16) for p in power]
        stepped = [both(p, t) for p, t in zip(power, inverse)]
        inverse = doubled([p for p, _ in stepped], [t for _, t in stepped], CH // BASE)
        high = [split(t) for t in inverse]
        parts = [split(l) for l in lower]
        none, gap = jnp.zeros((SUB, WIDE), BF16), jnp.zeros((WIDE - SUB, 2 * WIDE), BF16)
        made = [
            dot(
                jnp.concatenate([l[0], l[1]], 1),
                jnp.concatenate([jnp.concatenate(s, 1), gap, jnp.concatenate([s[0], none], 1), gap], 0),
            )
            for l, s in zip(parts, high)
        ]
        error = [eye - t - (m[:, :WIDE] + m[:, WIDE:]) for t, m in zip(inverse, made)]
        inverse = [t + dot(s[0][:, :SUB], e.astype(BF16)) for t, s, e in zip(inverse, high, error)]
        solved = [dot(t[:, :SUB].astype(BF16), rhs[i]).astype(BF16) for i, t in zip(at, inverse)]
        change = [dot(k[:SUB], s, ((0,), (0,))) for k, s in zip(pairs, solved)]
        qs = [queries[i] for i in at]
        attend = [jnp.where(seen, dot(q.astype(BF16), k[:SUB], ((1,), (1,))), 0.0).astype(BF16) for q, k in zip(qs, pairs)]
        effect = [dot(a, s) for a, s in zip(attend, solved)]
        for i, g, q, e in zip(at, change, qs, effect):
            state_map[i + (slice(0, CH),)] = (q - e[:, :DK]).astype(BF16)
            state_map[i + (slice(CH, CH + DK),)] = g[:, :DK].astype(BF16)
            added[i] = g[:, DK:]
            out_add[i] = e[:, DK:]

    states = [jnp.zeros((DK, DK), F32) for _ in range(heads)]
    for c in range(blocks):
        for h in range(heads):
            moved = dot(state_map[h, c], states[h].astype(BF16))
            out = moved[:CH] + out_add[h, c]
            states[h] = states[h] - moved[CH:] + added[h, c]
            out = out * lax.rsqrt(jnp.mean(out * out, -1, keepdims=True) + EPSILON) * head_gain_ref[...]
            mixed[c * CH:(c + 1) * CH, h * DK:(h + 1) * DK] = out.astype(BF16)
    own = length // count
    targets = [me_ref[0]] + [lax.rem(me_ref[0] + shift, count) for shift in SENT]
    rolled = jnp.concatenate([mixed[rows_at(block, own), :] for block in targets], 0)
    result = dot(rolled, wo_ref[...]).astype(BF16)
    for k, o in enumerate((o0, o1, o2, o3)):
        o[...] = result[k * own:(k + 1) * own]


UNROLL = 8


def mixer(me, gain, top, bottom, weights, sums, head_gain, wo):
    count = gain.shape[0]
    length = 2 * top.shape[0]
    heads = weights[0].shape[1] // DK
    blocks = length // CH
    own = length // count
    vmem = pl.BlockSpec(memory_space=pltpu.VMEM)
    return pl.pallas_call(
        lambda *refs: mixer_kernel(heads, *refs),
        out_shape=[jax.ShapeDtypeStruct((own, wo.shape[1]), BF16)] * count,
        in_specs=[pl.BlockSpec(memory_space=pltpu.SMEM)] + [vmem] * 12,
        out_specs=[vmem] * count,
        scratch_shapes=[
            pltpu.VMEM((heads, blocks, 2 * WIDE, DK), BF16),
            pltpu.VMEM((heads, blocks, SUB, DK), F32),
            pltpu.VMEM((heads, blocks, SUB, 2 * DK), BF16),
            pltpu.VMEM((heads, blocks, CH, DK), F32),
            pltpu.VMEM((heads, blocks, CH + DK, DK), BF16),
            pltpu.VMEM((heads, blocks, DK, DK), F32),
            pltpu.VMEM((heads, blocks, CH, DK), F32),
            pltpu.VMEM((length, heads * DK), BF16),
        ],
        compiler_params=pltpu.CompilerParams(vmem_limit_bytes=32 * MIB),
        cost_estimate=pl.CostEstimate(flops=2 * 10 ** 10, bytes_accessed=10 ** 7, transcendentals=0),
        name="mixer",
    )(me, gain, top, bottom, *weights, *sums, head_gain, wo)


def slots(ids_ref, experts, total):
    tokens = ids_ref.shape[1]
    capacity = total // experts
    label = iota((experts, tokens), 0)
    chosen = [(label == ids_ref[k:k + 1, :]).astype(F32) for k in range(2)]
    count = chosen[0] + chosen[1]
    before = (iota((tokens, tokens), 0) < iota((tokens, tokens), 1)).astype(BF16)
    earlier = dot(count.astype(BF16), before)
    spread = (iota((total, experts), 0) // capacity == iota((total, experts), 1)).astype(BF16)
    place = dot(spread, earlier.astype(BF16))
    fits = place == (iota((total, tokens), 0) % capacity).astype(F32)
    return chosen, [jnp.where(fits, dot(spread, c.astype(BF16)), 0.0) for c in chosen]


def ready_kernel(experts, me_ref, part_ref, x0, x1, x3, top_ref, bottom_ref, ids_ref, base_ref, chosen_ref):
    own, part = part_ref.shape[0], x0.shape[1]
    me, count = me_ref[0], x0.shape[0] // part_ref.shape[0]
    for shift, x in ((0, x0), (1, x1), (3, x3)):
        block = me if shift == 0 else source_of(me_ref, shift, count)
        base_ref[:, rows_at(block, part)] = x[rows_at(me, own), :].astype(F32)
    half = count // 2
    inner = rows_at(lax.rem(me, half), own)
    far = jnp.where(me < half, top_ref[inner, :].astype(F32), bottom_ref[inner, :].astype(F32))
    base_ref[:, rows_at(source_of(me_ref, half, count), part)] = far
    base_ref[...] = base_ref[...] + part_ref[...].astype(F32)
    _, chosen = slots(ids_ref, experts, chosen_ref.shape[0])
    chosen_ref[...] = (chosen[0] + chosen[1]).astype(BF16)


def ready(me, part, xs, ids, experts, capacity):
    own, width = part.shape
    vmem = pl.BlockSpec(memory_space=pltpu.VMEM)
    return pl.pallas_call(
        lambda *refs: ready_kernel(experts, *refs),
        out_shape=[
            jax.ShapeDtypeStruct((own, width), F32),
            jax.ShapeDtypeStruct((experts * capacity, own), BF16),
        ],
        in_specs=[pl.BlockSpec(memory_space=pltpu.SMEM)] + [vmem] * 7,
        out_specs=[vmem] * 2,
        compiler_params=pltpu.CompilerParams(vmem_limit_bytes=8 * MIB),
        cost_estimate=pl.CostEstimate(flops=2 * 10 ** 9, bytes_accessed=10 ** 6, transcendentals=0),
        name="ready",
    )(me, part, *xs, ids)


def route_kernel(base_ref, p1, p2, p3, gain_ref, chosen_ref, residual_ref, routed_ref, send_ref):
    arrived = [p[...].astype(F32) for p in (p1, p2, p3)]
    residual = (base_ref[...] + arrived[0]) + (arrived[1] + arrived[2])
    residual_ref[...] = residual
    mean = jnp.mean(residual * residual, -1, keepdims=True)
    routed = residual * lax.rsqrt(mean + EPSILON) * gain_ref[...]
    routed_ref[...] = routed
    send_ref[...] = dot(chosen_ref[...], routed.astype(BF16)).astype(BF16)


def route(base, parts, gain, chosen):
    own, width = base.shape
    vmem = pl.BlockSpec(memory_space=pltpu.VMEM)
    return pl.pallas_call(
        route_kernel,
        out_shape=[
            jax.ShapeDtypeStruct((own, width), F32),
            jax.ShapeDtypeStruct((own, width), F32),
            jax.ShapeDtypeStruct((chosen.shape[0], width), BF16),
        ],
        in_specs=[vmem] * 6,
        out_specs=[vmem] * 3,
        compiler_params=pltpu.CompilerParams(vmem_limit_bytes=8 * MIB),
        cost_estimate=pl.CostEstimate(flops=10 ** 9, bytes_accessed=10 ** 7, transcendentals=0),
        name="route",
    )(base, *parts, gain, chosen)


def weigh(routed_ref, router_ref, ids_ref, pick_ref, leading_ref):
    chosen, parts = slots(ids_ref, router_ref.shape[0], pick_ref.shape[1])
    tokens = routed_ref.shape[0]
    for k in range(2):
        pick_ref[k * tokens:(k + 1) * tokens, :] = jnp.transpose(parts[k]).astype(BF16)
    logits = lax.dot_general(
        router_ref[...], routed_ref[...], (((1,), (1,)), ((), ())),
        precision=lax.Precision.HIGHEST, preferred_element_type=F32,
    )
    gap = jnp.sum((chosen[0] - chosen[1]) * logits, 0, keepdims=True)
    leading = 1.0 / (1.0 + jnp.exp(-gap))
    leading_ref[...] = jnp.transpose(jnp.broadcast_to(leading, (128, tokens)))


def expert_kernel(rows_ref, gate_hbm, up_hbm, down_hbm, routed_ref, router_ref, ids_ref, out_ref, pick_ref,
                  leading_ref, gate_ref, up_ref, down_ref, hidden_ref, finished_ref, sems):
    total = rows_ref.shape[0]
    here, width, middle = gate_hbm.shape
    per = total // here
    experts = router_ref.shape[0]
    cap = pick_ref.shape[1] // experts
    deep, tall = width // PIECES, middle // PIECES
    copies, order = {}, []
    for e in range(here):
        for part, (source, target) in enumerate(((gate_hbm, gate_ref), (up_hbm, up_ref), (down_hbm, down_ref))):
            size = tall if part == 2 else deep
            for p in range(PIECES):
                at = (e, pl.ds(p * size, size))
                copies[e, part, p] = pltpu.make_async_copy(source.at[at], target.at[at], sems.at[e, part, p])
        for p in range(PIECES):
            order += [(e, 0, p), (e, 1, p)]
        order += [(e, 2, p) for p in range(PIECES)]
    for key in order[:FLIGHT]:
        copies[key].start()

    def take(*key):
        copies[key].wait()
        following = order.index(key) + FLIGHT
        if following < len(order):
            copies[order[following]].start()

    weigh(routed_ref, router_ref, ids_ref, pick_ref, leading_ref)
    r, c = iota((total, total), 0), iota((total, total), 1)

    def source(i):
        return (i % per) // cap * (here * cap) + i // per * cap + i % cap

    by_expert = (source(r) == c).astype(BF16)
    by_source = (source(c) == r).astype(BF16)
    rows = dot(by_expert, rows_ref[...]).astype(BF16)
    for e in range(here):
        mine = rows[e * per:(e + 1) * per]
        gate = up = 0.0
        for p in range(PIECES):
            at = slice(p * deep, (p + 1) * deep)
            take(e, 0, p)
            gate = gate + dot(mine[:, at], gate_ref[e, at])
            take(e, 1, p)
            up = up + dot(mine[:, at], up_ref[e, at])
        hidden_ref[...] = (gate / (1.0 + jnp.exp(-gate)) * up).astype(BF16)
        result = 0.0
        for p in range(PIECES):
            take(e, 2, p)
            at = slice(p * tall, (p + 1) * tall)
            result = result + dot(hidden_ref[:, at], down_ref[e, at])
        finished_ref[e * per:(e + 1) * per, :] = result.astype(BF16)
    for start in range(0, width, 512):
        at = slice(start, start + 512)
        out_ref[:, at] = dot(by_source, finished_ref[:, at]).astype(BF16)


PIECES = 4
FLIGHT = 10


def experts_here(rows, gate, up, down, routed, router, ids):
    here, width, middle = gate.shape
    per = rows.shape[0] // here
    tokens, experts = routed.shape[0], router.shape[0]
    capacity = 4 * tokens // experts
    vmem = pl.BlockSpec(memory_space=pltpu.VMEM)
    hbm = pl.BlockSpec(memory_space=pltpu.HBM)
    return pl.pallas_call(
        expert_kernel,
        out_shape=[
            jax.ShapeDtypeStruct(rows.shape, BF16),
            jax.ShapeDtypeStruct((2 * tokens, experts * capacity), BF16),
            jax.ShapeDtypeStruct((tokens, 128), F32),
        ],
        in_specs=[vmem] + [hbm] * 3 + [vmem] * 3,
        out_specs=[vmem] * 3,
        scratch_shapes=[
            pltpu.VMEM(gate.shape, BF16),
            pltpu.VMEM(up.shape, BF16),
            pltpu.VMEM(down.shape, BF16),
            pltpu.VMEM((per, middle), BF16),
            pltpu.VMEM(rows.shape, BF16),
            pltpu.SemaphoreType.DMA((here, 3, PIECES)),
        ],
        compiler_params=pltpu.CompilerParams(vmem_limit_bytes=46 * MIB),
        cost_estimate=pl.CostEstimate(flops=5 * 10 ** 9, bytes_accessed=10 ** 7, transcendentals=0),
        name="experts",
    )(rows, *[pltpu.with_memory_space_constraint(w, pltpu.HBM) for w in (gate, up, down)], routed, router, ids)


def combine_kernel(residual_ref, leading_ref, pick_ref, back_ref, out_ref):
    tokens = residual_ref.shape[0]
    picked = dot(pick_ref[...], back_ref[...])
    leading = leading_ref[:, 0:1]
    blended = leading * picked[:tokens] + (1.0 - leading) * picked[tokens:]
    out_ref[...] = (residual_ref[...] + blended).astype(BF16)


def combine(residual, leading, pick, back):
    vmem = pl.BlockSpec(memory_space=pltpu.VMEM)
    return pl.pallas_call(
        combine_kernel,
        out_shape=jax.ShapeDtypeStruct(residual.shape, BF16),
        in_specs=[vmem] * 4,
        out_specs=vmem,
        compiler_params=pltpu.CompilerParams(vmem_limit_bytes=16 * MIB),
        cost_estimate=pl.CostEstimate(flops=10 ** 9, bytes_accessed=10 ** 6, transcendentals=0),
        name="combine",
    )(residual, leading, pick, back)


def passed(x, k, axis):
    size = lax.axis_size(axis)
    return lax.ppermute(x, axis, [(i, (i + k) % size) for i in range(size)])


def shards(tokens, mixer_gain, query_weight, key_weight, value_weight, beta_weight, head_gain, output_weight,
           expert_gain, router_weight, expert_ids, gate_weight, up_weight, down_weight):
    owners = lax.axis_size("dp")
    me = lax.axis_index("head").reshape(1).astype(jnp.int32)
    left, right = (passed(tokens, shift, "head") for shift in NEAR)
    half = tokens.shape[0] // 2
    top, bottom = passed(left[:half], NEAR[0], "head"), passed(right[half:], NEAR[1], "head")
    gain = mixer_gain.reshape(lax.axis_size("head"), -1)
    here = first(me, gain, tokens, query_weight, key_weight, value_weight, beta_weight.T, head_gain.reshape(1, -1),
                 output_weight)
    weights, sums = here[1:5], here[7:]
    for shift, x in zip(NEAR, (left, right)):
        sums = more(shift, me, gain, x, weights, sums)
    parts = mixer(me, gain, top, bottom, weights, sums, here[5], here[6])
    arriving = [passed(part, shift, "head") for shift, part in zip(SENT, parts[1:])]
    experts = router_weight.shape[1]
    capacity = 4 * parts[0].shape[0] // experts
    ids = expert_ids.T
    base, chosen = ready(me, parts[0], (here[0], left, right, top, bottom), ids, experts, capacity)
    residual, routed, outgoing = route(base, arriving, expert_gain.reshape(1, -1), chosen)
    width = outgoing.shape[1]

    def exchanged(rows):
        rows = rows.reshape(owners, -1, width)
        rows = lax.all_to_all(rows, "dp", split_axis=0, concat_axis=0, tiled=True)
        return rows.reshape(-1, width)

    result, pick, leading = experts_here(
        exchanged(outgoing), gate_weight, up_weight, down_weight, routed, router_weight.T, ids
    )
    return combine(residual, leading, pick, exchanged(result))


def solution(mesh):
    return jax.shard_map(
        shards,
        mesh=mesh,
        in_specs=(
            P("dp", "head"),
            P(),
            P(None, "head"),
            P(None, None, "head"),
            P(None, None, "head"),
            P(None, "head"),
            P(),
            P("head", None),
            P(),
            P(),
            P(("dp", "head"), None),
            P("dp", None, None),
            P("dp", None, None),
            P("dp", None, None),
        ),
        out_specs=P(("dp", "head"), None),
        check_vma=False,
    )
```

```python
import jax
import jax.numpy as jnp
from jax import lax
from jax.experimental import pallas as pl
from jax.experimental.pallas import tpu as pltpu
from jax.sharding import PartitionSpec as P

DK = 128
NH = 3
CH = 32
SUB = CH * NH
WIDE = 128
BASE = 4
EPSILON = 1e-06
F32 = jnp.float32
BF16 = jnp.bfloat16
MIB = 1 << 20


def dot(a, b, dims=((1,), (0,))):
    return lax.dot_general(a, b, (dims, ((), ())), preferred_element_type=F32)


def split(a):
    high = a.astype(BF16)
    return high, (a - high.astype(F32)).astype(BF16)


def dot3(a, b, dims=((1,), (0,))):
    return dot(a[0], b[0], dims) + (dot(a[0], b[1], dims) + dot(a[1], b[0], dims))


def iota(shape, dim):
    return lax.broadcasted_iota(jnp.int32, shape, dim)


def rows_at(block, size):
    return pl.ds(pl.multiple_of(block * size, size), size)


NEAR = (1, 3)
SENT = (1, 2, 3)


def source_of(me_ref, shift, count):
    return lax.rem(me_ref[0] + (count - shift), count)


def gained(x_ref, gain_ref, source):
    wide = x_ref[...].astype(F32)
    return (wide * gain_ref[pl.ds(source, 1), :]).astype(BF16), jnp.sum(wide * wide, -1, keepdims=True)


def products(x, source, wq_ref, wk_ref, wv_ref, wb_ref):
    rows = rows_at(source, x.shape[1])
    yield dot(x, wq_ref[rows, :])
    for ref in (wk_ref, wv_ref):
        for m in range(NH):
            yield dot(x, ref[m, rows, :])
    yield dot(x, wb_ref[:, rows], ((1,), (1,)))


def first_kernel(me_ref, gain_ref, *refs):
    count = (len(refs) - 4) // 2
    here, there = refs[:count], refs[count:2 * count]
    sums_ref, beta_ref, square_ref, sems = refs[2 * count:]
    copies = [pltpu.make_async_copy(h, t, sems.at[i]) for i, (h, t) in enumerate(zip(here, there))]
    for copy in copies:
        copy.start()
    for copy in copies:
        copy.wait()
    x, square_ref[...] = gained(there[0], gain_ref, me_ref[0])
    for i, product in enumerate(products(x, me_ref[0], *there[1:5])):
        if i < 1 + 2 * NH:
            sums_ref[i] = product
        else:
            beta_ref[...] = product


def first(me, gain, tokens, wq, wk, wv, wb, *others):
    moved = (tokens, wq, wk, wv, wb, *others)
    length = tokens.shape[0]
    vmem = pl.BlockSpec(memory_space=pltpu.VMEM)
    made = [
        pltpu.VMEM((1 + 2 * NH, length, wq.shape[1]), F32),
        pltpu.VMEM((length, wb.shape[0]), F32),
        pltpu.VMEM((length, 1), F32),
    ]
    return pl.pallas_call(
        first_kernel,
        out_shape=[pltpu.VMEM(w.shape, w.dtype) for w in moved] + made,
        in_specs=[pl.BlockSpec(memory_space=pltpu.SMEM), vmem] + [pl.BlockSpec(memory_space=pltpu.HBM)] * len(moved),
        out_specs=[vmem] * (len(moved) + 3),
        scratch_shapes=[pltpu.SemaphoreType.DMA((len(moved),))],
        compiler_params=pltpu.CompilerParams(vmem_limit_bytes=4 * MIB),
        cost_estimate=pl.CostEstimate(flops=2 * 10 ** 9, bytes_accessed=10 ** 6, transcendentals=0),
        name="first",
    )(me, gain, *[pltpu.with_memory_space_constraint(w, pltpu.HBM) for w in moved])


def more_kernel(shift, me_ref, gain_ref, x_ref, wq_ref, wk_ref, wv_ref, wb_ref, sums_ref, beta_ref, square_ref,
                new_sums_ref, new_beta_ref, new_square_ref):
    source = source_of(me_ref, shift, gain_ref.shape[0])
    x, square = gained(x_ref, gain_ref, source)
    new_square_ref[...] = square_ref[...] + square
    for i, product in enumerate(products(x, source, wq_ref, wk_ref, wv_ref, wb_ref)):
        if i < 1 + 2 * NH:
            new_sums_ref[i] = sums_ref[i] + product
        else:
            new_beta_ref[...] = beta_ref[...] + product


def more(shift, me, gain, x, weights, sums):
    vmem = pl.BlockSpec(memory_space=pltpu.VMEM)
    return pl.pallas_call(
        lambda *refs: more_kernel(shift, *refs),
        out_shape=[pltpu.VMEM(a.shape, a.dtype) for a in sums],
        in_specs=[pl.BlockSpec(memory_space=pltpu.SMEM)] + [vmem] * 9,
        out_specs=[vmem] * 3,
        input_output_aliases={7: 0, 8: 1, 9: 2},
        compiler_params=pltpu.CompilerParams(vmem_limit_bytes=4 * MIB),
        cost_estimate=pl.CostEstimate(flops=10 ** 9, bytes_accessed=10 ** 6, transcendentals=0),
        name="more",
    )(me, gain, x, *weights, *sums)


def mixer_kernel(heads, me_ref, gain_ref, top_ref, bottom_ref, wq_ref, wk_ref, wv_ref, wb_ref, sums_ref, beta_ref, square_ref,
                 head_gain_ref, wo_ref, o0, o1, o2, o3, keys, beta_keys, rhs, queries, state_map, added, out_add, mixed):
    count, part = gain_ref.shape
    length = 2 * top_ref.shape[0]
    source = source_of(me_ref, count // 2, count)
    x, square = gained(jnp.concatenate([top_ref[...], bottom_ref[...]], 0), gain_ref, source)
    scale = lax.rsqrt((square_ref[...] + square) / (count * part) + EPSILON)
    last = products(x, source, wq_ref, wk_ref, wv_ref, wb_ref)
    whole = [(sums_ref[i] + next(last)) * scale for i in range(1 + 2 * NH)]
    beta = (beta_ref[...] + next(last)) * scale
    beta = 2.0 / (1.0 + jnp.exp(-beta))
    blocks = length // CH
    query = whole[0]
    for h in range(heads):
        q = query[:, h * DK:(h + 1) * DK]
        q = q * lax.rsqrt(jnp.sum(q * q, -1, keepdims=True) + EPSILON) * DK ** (-0.5)
        queries[h] = q.reshape(blocks, CH, DK)
    for edge in (SUB, WIDE + SUB):
        keys[:, :, edge:edge + WIDE - SUB, :] = jnp.zeros((heads, blocks, WIDE - SUB, DK), BF16)
    for m in range(NH):
        key = whole[1 + m]
        value = whole[1 + NH + m]
        for h in range(heads):
            b = beta[:, h * NH + m:h * NH + m + 1]
            k = key[:, h * DK:(h + 1) * DK]
            k = k * lax.rsqrt(jnp.sum(k * k, -1, keepdims=True) + EPSILON)
            high, low = split(k)
            keys[h, :, m * CH:(m + 1) * CH, :] = high.reshape(blocks, CH, DK)
            keys[h, :, WIDE + m * CH:WIDE + (m + 1) * CH, :] = low.reshape(blocks, CH, DK)
            rhs[h, :, m * CH:(m + 1) * CH, :DK] = (k * b).astype(BF16).reshape(blocks, CH, DK)
            rhs[h, :, m * CH:(m + 1) * CH, DK:] = (value[:, h * DK:(h + 1) * DK] * b).astype(BF16).reshape(blocks, CH, DK)
            beta_keys[h, :, m * CH:(m + 1) * CH, :] = jnp.broadcast_to(b, (length, DK)).reshape(blocks, CH, DK)

    row, col = iota((SUB, WIDE), 0), iota((SUB, WIDE), 1)
    inside = col < SUB
    row_t, col_t = row % CH, col % CH
    causal = inside & ((col_t < row_t) | ((col_t == row_t) & (col < row)))
    near = row_t // BASE == col_t // BASE
    eye = (row == col).astype(F32)
    seen = iota((CH, SUB), 1) % CH <= iota((CH, SUB), 0)
    blank = jnp.zeros((WIDE - SUB, WIDE), F32)

    def square(p):
        return dot(p[:, :SUB], p)

    def both(p, t):
        made = dot(p[:, :SUB], jnp.concatenate([p, t.astype(BF16)], 1))
        return made[:, :WIDE].astype(BF16), t + made[:, WIDE:]

    def doubled(powers, sums, terms):
        span = 2
        while 2 * span < terms:
            stepped = [both(p, t) for p, t in zip(powers, sums)]
            powers, sums = [p for p, _ in stepped], [t for _, t in stepped]
            span *= 2
        return [t + dot(p[:, :SUB], t.astype(BF16)) for p, t in zip(powers, sums)]

    unroll = UNROLL
    for start in range(0, blocks, unroll):
        at = [(h, c) for c in range(start, start + unroll) for h in range(heads)]
        pairs = [keys[i] for i in at]
        alike = [dot(k[:SUB], k, ((1,), (1,))) for k in pairs]
        alike = [
            a[:, :WIDE] + a[:, WIDE:] + jnp.transpose(jnp.concatenate([a[:, WIDE:], blank], 0))[:SUB] for a in alike
        ]
        lower = [jnp.where(causal, a * beta_keys[i], 0.0) for i, a in zip(at, alike)]
        power = [jnp.where(near, -l, 0.0) for l in lower]
        inverse = [eye + p for p in power]
        power = [square(p.astype(BF16)).astype(BF16) for p in power]
        inverse = doubled(power, inverse, BASE * NH)
        low = [t.astype(BF16) for t in inverse]
        power = [
            -dot(t[:, :SUB], jnp.where(near, 0.0, l).astype(BF16)) for t, l in zip(low, lower)
        ]
        power = [p.astype(BF16) for p in power]
        stepped = [both(p, t) for p, t in zip(power, inverse)]
        inverse = doubled([p for p, _ in stepped], [t for _, t in stepped], CH // BASE)
        high = [split(t) for t in inverse]
        parts = [split(l) for l in lower]
        none, gap = jnp.zeros((SUB, WIDE), BF16), jnp.zeros((WIDE - SUB, 2 * WIDE), BF16)
        made = [
            dot(
                jnp.concatenate([l[0], l[1]], 1),
                jnp.concatenate([jnp.concatenate(s, 1), gap, jnp.concatenate([s[0], none], 1), gap], 0),
            )
            for l, s in zip(parts, high)
        ]
        error = [eye - t - (m[:, :WIDE] + m[:, WIDE:]) for t, m in zip(inverse, made)]
        inverse = [t + dot(s[0][:, :SUB], e.astype(BF16)) for t, s, e in zip(inverse, high, error)]
        solved = [dot(t[:, :SUB].astype(BF16), rhs[i]).astype(BF16) for i, t in zip(at, inverse)]
        change = [dot(k[:SUB], s, ((0,), (0,))) for k, s in zip(pairs, solved)]
        qs = [queries[i] for i in at]
        attend = [jnp.where(seen, dot(q.astype(BF16), k[:SUB], ((1,), (1,))), 0.0).astype(BF16) for q, k in zip(qs, pairs)]
        effect = [dot(a, s) for a, s in zip(attend, solved)]
        reads = [(q - e[:, :DK]) for q, e in zip(qs, effect)]
        for n in range(0, unroll, 2):
            for h in range(heads):
                one, two = n * heads + h, (n + 1) * heads + h
                pair = (h, (start + n) // 2)
                later = jnp.concatenate([reads[two], change[two][:, :DK]], 0).astype(BF16)
                both_steps = dot(later, change[one].astype(BF16))
                state_map[pair + (slice(0, CH),)] = reads[one].astype(BF16)
                state_map[pair + (slice(CH, 2 * CH),)] = (reads[two] - both_steps[:CH, :DK]).astype(BF16)
                state_map[pair + (slice(2 * CH, 2 * CH + DK),)] = (
                    change[one][:, :DK] + (change[two][:, :DK] - both_steps[CH:, :DK])
                ).astype(BF16)
                added[pair] = change[one][:, DK:] + (change[two][:, DK:] - both_steps[CH:, DK:])
                out_add[pair + (slice(0, CH),)] = effect[one][:, DK:]
                out_add[pair + (slice(CH, 2 * CH),)] = effect[two][:, DK:] + both_steps[:CH, DK:]

    states = [jnp.zeros((DK, DK), F32) for _ in range(heads)]
    for c in range(blocks // 2):
        for h in range(heads):
            moved = dot(state_map[h, c], states[h].astype(BF16))
            out = moved[:2 * CH] + out_add[h, c]
            states[h] = states[h] - moved[2 * CH:] + added[h, c]
            out = out * lax.rsqrt(jnp.mean(out * out, -1, keepdims=True) + EPSILON) * head_gain_ref[...]
            mixed[c * 2 * CH:(c + 1) * 2 * CH, h * DK:(h + 1) * DK] = out.astype(BF16)
    own = length // count
    targets = [me_ref[0]] + [lax.rem(me_ref[0] + shift, count) for shift in SENT]
    rolled = jnp.concatenate([mixed[rows_at(block, own), :] for block in targets], 0)
    result = dot(rolled, wo_ref[...]).astype(BF16)
    for k, o in enumerate((o0, o1, o2, o3)):
        o[...] = result[k * own:(k + 1) * own]


UNROLL = 8


def mixer(me, gain, top, bottom, weights, sums, head_gain, wo):
    count = gain.shape[0]
    length = 2 * top.shape[0]
    heads = weights[0].shape[1] // DK
    blocks = length // CH
    own = length // count
    vmem = pl.BlockSpec(memory_space=pltpu.VMEM)
    return pl.pallas_call(
        lambda *refs: mixer_kernel(heads, *refs),
        out_shape=[jax.ShapeDtypeStruct((own, wo.shape[1]), BF16)] * count,
        in_specs=[pl.BlockSpec(memory_space=pltpu.SMEM)] + [vmem] * 12,
        out_specs=[vmem] * count,
        scratch_shapes=[
            pltpu.VMEM((heads, blocks, 2 * WIDE, DK), BF16),
            pltpu.VMEM((heads, blocks, SUB, DK), F32),
            pltpu.VMEM((heads, blocks, SUB, 2 * DK), BF16),
            pltpu.VMEM((heads, blocks, CH, DK), F32),
            pltpu.VMEM((heads, blocks // 2, 2 * CH + DK, DK), BF16),
            pltpu.VMEM((heads, blocks // 2, DK, DK), F32),
            pltpu.VMEM((heads, blocks // 2, 2 * CH, DK), F32),
            pltpu.VMEM((length, heads * DK), BF16),
        ],
        compiler_params=pltpu.CompilerParams(vmem_limit_bytes=32 * MIB),
        cost_estimate=pl.CostEstimate(flops=2 * 10 ** 10, bytes_accessed=10 ** 7, transcendentals=0),
        name="mixer",
    )(me, gain, top, bottom, *weights, *sums, head_gain, wo)


def slots(ids_ref, experts, total):
    tokens = ids_ref.shape[1]
    capacity = total // experts
    label = iota((experts, tokens), 0)
    chosen = [(label == ids_ref[k:k + 1, :]).astype(F32) for k in range(2)]
    count = chosen[0] + chosen[1]
    before = (iota((tokens, tokens), 0) < iota((tokens, tokens), 1)).astype(BF16)
    earlier = dot(count.astype(BF16), before)
    spread = (iota((total, experts), 0) // capacity == iota((total, experts), 1)).astype(BF16)
    place = dot(spread, earlier.astype(BF16))
    fits = place == (iota((total, tokens), 0) % capacity).astype(F32)
    return chosen, [jnp.where(fits, dot(spread, c.astype(BF16)), 0.0) for c in chosen]


def ready_kernel(experts, me_ref, part_ref, x0, x1, x3, top_ref, bottom_ref, ids_ref, base_ref, chosen_ref):
    own, part = part_ref.shape[0], x0.shape[1]
    me, count = me_ref[0], x0.shape[0] // part_ref.shape[0]
    for shift, x in ((0, x0), (1, x1), (3, x3)):
        block = me if shift == 0 else source_of(me_ref, shift, count)
        base_ref[:, rows_at(block, part)] = x[rows_at(me, own), :].astype(F32)
    half = count // 2
    inner = rows_at(lax.rem(me, half), own)
    far = jnp.where(me < half, top_ref[inner, :].astype(F32), bottom_ref[inner, :].astype(F32))
    base_ref[:, rows_at(source_of(me_ref, half, count), part)] = far
    base_ref[...] = base_ref[...] + part_ref[...].astype(F32)
    _, chosen = slots(ids_ref, experts, chosen_ref.shape[0])
    chosen_ref[...] = (chosen[0] + chosen[1]).astype(BF16)


def ready(me, part, xs, ids, experts, capacity):
    own, width = part.shape
    vmem = pl.BlockSpec(memory_space=pltpu.VMEM)
    return pl.pallas_call(
        lambda *refs: ready_kernel(experts, *refs),
        out_shape=[
            jax.ShapeDtypeStruct((own, width), F32),
            jax.ShapeDtypeStruct((experts * capacity, own), BF16),
        ],
        in_specs=[pl.BlockSpec(memory_space=pltpu.SMEM)] + [vmem] * 7,
        out_specs=[vmem] * 2,
        compiler_params=pltpu.CompilerParams(vmem_limit_bytes=8 * MIB),
        cost_estimate=pl.CostEstimate(flops=2 * 10 ** 9, bytes_accessed=10 ** 6, transcendentals=0),
        name="ready",
    )(me, part, *xs, ids)


def route_kernel(base_ref, p1, p2, p3, gain_ref, chosen_ref, residual_ref, routed_ref, send_ref):
    arrived = [p[...].astype(F32) for p in (p1, p2, p3)]
    residual = (base_ref[...] + arrived[0]) + (arrived[1] + arrived[2])
    residual_ref[...] = residual
    mean = jnp.mean(residual * residual, -1, keepdims=True)
    routed = residual * lax.rsqrt(mean + EPSILON) * gain_ref[...]
    routed_ref[...] = routed
    send_ref[...] = dot(chosen_ref[...], routed.astype(BF16)).astype(BF16)


def route(base, parts, gain, chosen):
    own, width = base.shape
    vmem = pl.BlockSpec(memory_space=pltpu.VMEM)
    return pl.pallas_call(
        route_kernel,
        out_shape=[
            jax.ShapeDtypeStruct((own, width), F32),
            jax.ShapeDtypeStruct((own, width), F32),
            jax.ShapeDtypeStruct((chosen.shape[0], width), BF16),
        ],
        in_specs=[vmem] * 6,
        out_specs=[vmem] * 3,
        compiler_params=pltpu.CompilerParams(vmem_limit_bytes=8 * MIB),
        cost_estimate=pl.CostEstimate(flops=10 ** 9, bytes_accessed=10 ** 7, transcendentals=0),
        name="route",
    )(base, *parts, gain, chosen)


def weigh(routed_ref, router_ref, ids_ref, pick_ref, leading_ref):
    chosen, parts = slots(ids_ref, router_ref.shape[0], pick_ref.shape[1])
    tokens = routed_ref.shape[0]
    for k in range(2):
        pick_ref[k * tokens:(k + 1) * tokens, :] = jnp.transpose(parts[k]).astype(BF16)
    logits = lax.dot_general(
        router_ref[...], routed_ref[...], (((1,), (1,)), ((), ())),
        precision=lax.Precision.HIGHEST, preferred_element_type=F32,
    )
    gap = jnp.sum((chosen[0] - chosen[1]) * logits, 0, keepdims=True)
    leading = 1.0 / (1.0 + jnp.exp(-gap))
    leading_ref[...] = jnp.transpose(jnp.broadcast_to(leading, (128, tokens)))


def expert_kernel(rows_ref, gate_hbm, up_hbm, down_hbm, routed_ref, router_ref, ids_ref, out_ref, pick_ref,
                  leading_ref, gate_ref, up_ref, down_ref, hidden_ref, finished_ref, sems):
    total = rows_ref.shape[0]
    here, width, middle = gate_hbm.shape
    per = total // here
    experts = router_ref.shape[0]
    cap = pick_ref.shape[1] // experts
    deep, tall = width // PIECES, middle // PIECES
    copies, order = {}, []
    for e in range(here):
        for part, (source, target) in enumerate(((gate_hbm, gate_ref), (up_hbm, up_ref), (down_hbm, down_ref))):
            size = tall if part == 2 else deep
            for p in range(PIECES):
                at = (e, pl.ds(p * size, size))
                copies[e, part, p] = pltpu.make_async_copy(source.at[at], target.at[at], sems.at[e, part, p])
        for p in range(PIECES):
            order += [(e, 0, p), (e, 1, p)]
        order += [(e, 2, p) for p in range(PIECES)]
    for key in order[:FLIGHT]:
        copies[key].start()

    def take(*key):
        copies[key].wait()
        following = order.index(key) + FLIGHT
        if following < len(order):
            copies[order[following]].start()

    weigh(routed_ref, router_ref, ids_ref, pick_ref, leading_ref)
    r, c = iota((total, total), 0), iota((total, total), 1)

    def source(i):
        return (i % per) // cap * (here * cap) + i // per * cap + i % cap

    by_expert = (source(r) == c).astype(BF16)
    by_source = (source(c) == r).astype(BF16)
    rows = dot(by_expert, rows_ref[...]).astype(BF16)
    for e in range(here):
        mine = rows[e * per:(e + 1) * per]
        gate = up = 0.0
        for p in range(PIECES):
            at = slice(p * deep, (p + 1) * deep)
            take(e, 0, p)
            gate = gate + dot(mine[:, at], gate_ref[e, at])
            take(e, 1, p)
            up = up + dot(mine[:, at], up_ref[e, at])
        hidden_ref[...] = (gate / (1.0 + jnp.exp(-gate)) * up).astype(BF16)
        result = 0.0
        for p in range(PIECES):
            take(e, 2, p)
            at = slice(p * tall, (p + 1) * tall)
            result = result + dot(hidden_ref[:, at], down_ref[e, at])
        finished_ref[e * per:(e + 1) * per, :] = result.astype(BF16)
    for start in range(0, width, 512):
        at = slice(start, start + 512)
        out_ref[:, at] = dot(by_source, finished_ref[:, at]).astype(BF16)


PIECES = 4
FLIGHT = 10


def experts_here(rows, gate, up, down, routed, router, ids):
    here, width, middle = gate.shape
    per = rows.shape[0] // here
    tokens, experts = routed.shape[0], router.shape[0]
    capacity = 4 * tokens // experts
    vmem = pl.BlockSpec(memory_space=pltpu.VMEM)
    hbm = pl.BlockSpec(memory_space=pltpu.HBM)
    return pl.pallas_call(
        expert_kernel,
        out_shape=[
            jax.ShapeDtypeStruct(rows.shape, BF16),
            jax.ShapeDtypeStruct((2 * tokens, experts * capacity), BF16),
            jax.ShapeDtypeStruct((tokens, 128), F32),
        ],
        in_specs=[vmem] + [hbm] * 3 + [vmem] * 3,
        out_specs=[vmem] * 3,
        scratch_shapes=[
            pltpu.VMEM(gate.shape, BF16),
            pltpu.VMEM(up.shape, BF16),
            pltpu.VMEM(down.shape, BF16),
            pltpu.VMEM((per, middle), BF16),
            pltpu.VMEM(rows.shape, BF16),
            pltpu.SemaphoreType.DMA((here, 3, PIECES)),
        ],
        compiler_params=pltpu.CompilerParams(vmem_limit_bytes=46 * MIB),
        cost_estimate=pl.CostEstimate(flops=5 * 10 ** 9, bytes_accessed=10 ** 7, transcendentals=0),
        name="experts",
    )(rows, *[pltpu.with_memory_space_constraint(w, pltpu.HBM) for w in (gate, up, down)], routed, router, ids)


def combine_kernel(residual_ref, leading_ref, pick_ref, back_ref, out_ref):
    tokens = residual_ref.shape[0]
    picked = dot(pick_ref[...], back_ref[...])
    leading = leading_ref[:, 0:1]
    blended = leading * picked[:tokens] + (1.0 - leading) * picked[tokens:]
    out_ref[...] = (residual_ref[...] + blended).astype(BF16)


def combine(residual, leading, pick, back):
    vmem = pl.BlockSpec(memory_space=pltpu.VMEM)
    return pl.pallas_call(
        combine_kernel,
        out_shape=jax.ShapeDtypeStruct(residual.shape, BF16),
        in_specs=[vmem] * 4,
        out_specs=vmem,
        compiler_params=pltpu.CompilerParams(vmem_limit_bytes=16 * MIB),
        cost_estimate=pl.CostEstimate(flops=10 ** 9, bytes_accessed=10 ** 6, transcendentals=0),
        name="combine",
    )(residual, leading, pick, back)


def passed(x, k, axis):
    size = lax.axis_size(axis)
    return lax.ppermute(x, axis, [(i, (i + k) % size) for i in range(size)])


def shards(tokens, mixer_gain, query_weight, key_weight, value_weight, beta_weight, head_gain, output_weight,
           expert_gain, router_weight, expert_ids, gate_weight, up_weight, down_weight):
    owners = lax.axis_size("dp")
    me = lax.axis_index("head").reshape(1).astype(jnp.int32)
    left, right = (passed(tokens, shift, "head") for shift in NEAR)
    half = tokens.shape[0] // 2
    top, bottom = passed(left[:half], NEAR[0], "head"), passed(right[half:], NEAR[1], "head")
    gain = mixer_gain.reshape(lax.axis_size("head"), -1)
    here = first(me, gain, tokens, query_weight, key_weight, value_weight, beta_weight.T, head_gain.reshape(1, -1),
                 output_weight)
    weights, sums = here[1:5], here[7:]
    for shift, x in zip(NEAR, (left, right)):
        sums = more(shift, me, gain, x, weights, sums)
    parts = mixer(me, gain, top, bottom, weights, sums, here[5], here[6])
    arriving = [passed(part, shift, "head") for shift, part in zip(SENT, parts[1:])]
    experts = router_weight.shape[1]
    capacity = 4 * parts[0].shape[0] // experts
    ids = expert_ids.T
    base, chosen = ready(me, parts[0], (here[0], left, right, top, bottom), ids, experts, capacity)
    residual, routed, outgoing = route(base, arriving, expert_gain.reshape(1, -1), chosen)
    width = outgoing.shape[1]

    def exchanged(rows):
        rows = rows.reshape(owners, -1, width)
        rows = lax.all_to_all(rows, "dp", split_axis=0, concat_axis=0, tiled=True)
        return rows.reshape(-1, width)

    result, pick, leading = experts_here(
        exchanged(outgoing), gate_weight, up_weight, down_weight, routed, router_weight.T, ids
    )
    return combine(residual, leading, pick, exchanged(result))


def solution(mesh):
    return jax.shard_map(
        shards,
        mesh=mesh,
        in_specs=(
            P("dp", "head"),
            P(),
            P(None, "head"),
            P(None, None, "head"),
            P(None, None, "head"),
            P(None, "head"),
            P(),
            P("head", None),
            P(),
            P(),
            P(("dp", "head"), None),
            P("dp", None, None),
            P("dp", None, None),
            P("dp", None, None),
        ),
        out_specs=P(("dp", "head"), None),
        check_vma=False,
    )
```

```python
import jax
import jax.numpy as jnp
from jax import lax
from jax.experimental import pallas as pl
from jax.experimental.pallas import tpu as pltpu
from jax.sharding import PartitionSpec as P

DK = 128
NH = 3
CH = 32
SUB = CH * NH
WIDE = 128
BASE = 4
EPSILON = 1e-06
F32 = jnp.float32
BF16 = jnp.bfloat16
MIB = 1 << 20


def dot(a, b, dims=((1,), (0,))):
    return lax.dot_general(a, b, (dims, ((), ())), preferred_element_type=F32)


def split(a):
    high = a.astype(BF16)
    return high, (a - high.astype(F32)).astype(BF16)


def dot3(a, b, dims=((1,), (0,))):
    return dot(a[0], b[0], dims) + (dot(a[0], b[1], dims) + dot(a[1], b[0], dims))


def iota(shape, dim):
    return lax.broadcasted_iota(jnp.int32, shape, dim)


def rows_at(block, size):
    return pl.ds(pl.multiple_of(block * size, size), size)


NEAR = (1, 3)
SENT = (2, 1, 3)


def source_of(me_ref, shift, count):
    return lax.rem(me_ref[0] + (count - shift), count)


def gained(x_ref, gain_ref, source):
    wide = x_ref[...].astype(F32)
    return (wide * gain_ref[pl.ds(source, 1), :]).astype(BF16), jnp.sum(wide * wide, -1, keepdims=True)


def products(x, source, wq_ref, wk_ref, wv_ref, wb_ref):
    rows = rows_at(source, x.shape[1])
    yield dot(x, wq_ref[rows, :])
    for ref in (wk_ref, wv_ref):
        for m in range(NH):
            yield dot(x, ref[m, rows, :])
    yield dot(x, wb_ref[:, rows], ((1,), (1,)))


def first_kernel(me_ref, gain_ref, *refs):
    count = (len(refs) - 4) // 2
    here, there = refs[:count], refs[count:2 * count]
    sums_ref, beta_ref, square_ref, sems = refs[2 * count:]
    copies = [pltpu.make_async_copy(h, t, sems.at[i]) for i, (h, t) in enumerate(zip(here, there))]
    for copy in copies:
        copy.start()
    for copy in copies:
        copy.wait()
    x, square_ref[...] = gained(there[0], gain_ref, me_ref[0])
    for i, product in enumerate(products(x, me_ref[0], *there[1:5])):
        if i < 1 + 2 * NH:
            sums_ref[i] = product
        else:
            beta_ref[...] = product


def first(me, gain, tokens, wq, wk, wv, wb, *others):
    moved = (tokens, wq, wk, wv, wb, *others)
    length = tokens.shape[0]
    vmem = pl.BlockSpec(memory_space=pltpu.VMEM)
    made = [
        pltpu.VMEM((1 + 2 * NH, length, wq.shape[1]), F32),
        pltpu.VMEM((length, wb.shape[0]), F32),
        pltpu.VMEM((length, 1), F32),
    ]
    return pl.pallas_call(
        first_kernel,
        out_shape=[pltpu.VMEM(w.shape, w.dtype) for w in moved] + made,
        in_specs=[pl.BlockSpec(memory_space=pltpu.SMEM), vmem] + [pl.BlockSpec(memory_space=pltpu.HBM)] * len(moved),
        out_specs=[vmem] * (len(moved) + 3),
        scratch_shapes=[pltpu.SemaphoreType.DMA((len(moved),))],
        compiler_params=pltpu.CompilerParams(vmem_limit_bytes=4 * MIB),
        cost_estimate=pl.CostEstimate(flops=2 * 10 ** 9, bytes_accessed=10 ** 6, transcendentals=0),
        name="first",
    )(me, gain, *[pltpu.with_memory_space_constraint(w, pltpu.HBM) for w in moved])


def more_kernel(shift, me_ref, gain_ref, x_ref, wq_ref, wk_ref, wv_ref, wb_ref, sums_ref, beta_ref, square_ref,
                new_sums_ref, new_beta_ref, new_square_ref):
    source = source_of(me_ref, shift, gain_ref.shape[0])
    x, square = gained(x_ref, gain_ref, source)
    new_square_ref[...] = square_ref[...] + square
    for i, product in enumerate(products(x, source, wq_ref, wk_ref, wv_ref, wb_ref)):
        if i < 1 + 2 * NH:
            new_sums_ref[i] = sums_ref[i] + product
        else:
            new_beta_ref[...] = beta_ref[...] + product


def more(shift, me, gain, x, weights, sums):
    vmem = pl.BlockSpec(memory_space=pltpu.VMEM)
    return pl.pallas_call(
        lambda *refs: more_kernel(shift, *refs),
        out_shape=[pltpu.VMEM(a.shape, a.dtype) for a in sums],
        in_specs=[pl.BlockSpec(memory_space=pltpu.SMEM)] + [vmem] * 9,
        out_specs=[vmem] * 3,
        input_output_aliases={7: 0, 8: 1, 9: 2},
        compiler_params=pltpu.CompilerParams(vmem_limit_bytes=4 * MIB),
        cost_estimate=pl.CostEstimate(flops=10 ** 9, bytes_accessed=10 ** 6, transcendentals=0),
        name="more",
    )(me, gain, x, *weights, *sums)


def mixer_kernel(heads, me_ref, gain_ref, top_ref, bottom_ref, wq_ref, wk_ref, wv_ref, wb_ref, sums_ref, beta_ref, square_ref,
                 head_gain_ref, wo_ref, o0, o1, o2, o3, keys, beta_keys, rhs, queries, state_map, added, out_add, mixed):
    count, part = gain_ref.shape
    length = 2 * top_ref.shape[0]
    source = source_of(me_ref, count // 2, count)
    x, square = gained(jnp.concatenate([top_ref[...], bottom_ref[...]], 0), gain_ref, source)
    scale = lax.rsqrt((square_ref[...] + square) / (count * part) + EPSILON)
    last = products(x, source, wq_ref, wk_ref, wv_ref, wb_ref)
    whole = [(sums_ref[i] + next(last)) * scale for i in range(1 + 2 * NH)]
    beta = (beta_ref[...] + next(last)) * scale
    beta = 2.0 / (1.0 + jnp.exp(-beta))
    blocks = length // CH
    query = whole[0]
    for h in range(heads):
        q = query[:, h * DK:(h + 1) * DK]
        q = q * lax.rsqrt(jnp.sum(q * q, -1, keepdims=True) + EPSILON) * DK ** (-0.5)
        queries[h] = q.reshape(blocks, CH, DK)
    for edge in (SUB, WIDE + SUB):
        keys[:, :, edge:edge + WIDE - SUB, :] = jnp.zeros((heads, blocks, WIDE - SUB, DK), BF16)
    for m in range(NH):
        key = whole[1 + m]
        value = whole[1 + NH + m]
        for h in range(heads):
            b = beta[:, h * NH + m:h * NH + m + 1]
            k = key[:, h * DK:(h + 1) * DK]
            k = k * lax.rsqrt(jnp.sum(k * k, -1, keepdims=True) + EPSILON)
            high, low = split(k)
            keys[h, :, m * CH:(m + 1) * CH, :] = high.reshape(blocks, CH, DK)
            keys[h, :, WIDE + m * CH:WIDE + (m + 1) * CH, :] = low.reshape(blocks, CH, DK)
            rhs[h, :, m * CH:(m + 1) * CH, :DK] = (k * b).astype(BF16).reshape(blocks, CH, DK)
            rhs[h, :, m * CH:(m + 1) * CH, DK:] = (value[:, h * DK:(h + 1) * DK] * b).astype(BF16).reshape(blocks, CH, DK)
            beta_keys[h, :, m * CH:(m + 1) * CH, :] = jnp.broadcast_to(b, (length, DK)).reshape(blocks, CH, DK)

    row, col = iota((SUB, WIDE), 0), iota((SUB, WIDE), 1)
    inside = col < SUB
    row_t, col_t = row % CH, col % CH
    causal = inside & ((col_t < row_t) | ((col_t == row_t) & (col < row)))
    near = row_t // BASE == col_t // BASE
    eye = (row == col).astype(F32)
    seen = iota((CH, SUB), 1) % CH <= iota((CH, SUB), 0)
    blank = jnp.zeros((WIDE - SUB, WIDE), F32)

    def square(p):
        return dot(p[:, :SUB], p)

    def both(p, t):
        made = dot(p[:, :SUB], jnp.concatenate([p, t.astype(BF16)], 1))
        return made[:, :WIDE].astype(BF16), t + made[:, WIDE:]

    def doubled(powers, sums, terms):
        span = 2
        while 2 * span < terms:
            stepped = [both(p, t) for p, t in zip(powers, sums)]
            powers, sums = [p for p, _ in stepped], [t for _, t in stepped]
            span *= 2
        return [t + dot(p[:, :SUB], t.astype(BF16)) for p, t in zip(powers, sums)]

    unroll = UNROLL
    for start in range(0, blocks, unroll):
        at = [(h, c) for c in range(start, start + unroll) for h in range(heads)]
        pairs = [keys[i] for i in at]
        alike = [dot(k[:SUB], k, ((1,), (1,))) for k in pairs]
        alike = [
            a[:, :WIDE] + a[:, WIDE:] + jnp.transpose(jnp.concatenate([a[:, WIDE:], blank], 0))[:SUB] for a in alike
        ]
        lower = [jnp.where(causal, a * beta_keys[i], 0.0) for i, a in zip(at, alike)]
        power = [jnp.where(near, -l, 0.0) for l in lower]
        inverse = [eye + p for p in power]
        power = [square(p.astype(BF16)).astype(BF16) for p in power]
        inverse = doubled(power, inverse, BASE * NH)
        low = [t.astype(BF16) for t in inverse]
        power = [
            -dot(t[:, :SUB], jnp.where(near, 0.0, l).astype(BF16)) for t, l in zip(low, lower)
        ]
        power = [p.astype(BF16) for p in power]
        stepped = [both(p, t) for p, t in zip(power, inverse)]
        inverse = doubled([p for p, _ in stepped], [t for _, t in stepped], CH // BASE)
        high = [split(t) for t in inverse]
        parts = [split(l) for l in lower]
        none, gap = jnp.zeros((SUB, WIDE), BF16), jnp.zeros((WIDE - SUB, 2 * WIDE), BF16)
        made = [
            dot(
                jnp.concatenate([l[0], l[1]], 1),
                jnp.concatenate([jnp.concatenate(s, 1), gap, jnp.concatenate([s[0], none], 1), gap], 0),
            )
            for l, s in zip(parts, high)
        ]
        error = [eye - t - (m[:, :WIDE] + m[:, WIDE:]) for t, m in zip(inverse, made)]
        inverse = [t + dot(s[0][:, :SUB], e.astype(BF16)) for t, s, e in zip(inverse, high, error)]
        solved = [dot(t[:, :SUB].astype(BF16), rhs[i]).astype(BF16) for i, t in zip(at, inverse)]
        change = [dot(k[:SUB], s, ((0,), (0,))) for k, s in zip(pairs, solved)]
        qs = [queries[i] for i in at]
        attend = [jnp.where(seen, dot(q.astype(BF16), k[:SUB], ((1,), (1,))), 0.0).astype(BF16) for q, k in zip(qs, pairs)]
        effect = [dot(a, s) for a, s in zip(attend, solved)]
        reads = [(q - e[:, :DK]) for q, e in zip(qs, effect)]
        for n in range(0, unroll, 2):
            for h in range(heads):
                one, two = n * heads + h, (n + 1) * heads + h
                pair = (h, (start + n) // 2)
                later = jnp.concatenate([reads[two], change[two][:, :DK]], 0).astype(BF16)
                both_steps = dot(later, change[one].astype(BF16))
                state_map[pair + (slice(0, CH),)] = reads[one].astype(BF16)
                state_map[pair + (slice(CH, 2 * CH),)] = (reads[two] - both_steps[:CH, :DK]).astype(BF16)
                state_map[pair + (slice(2 * CH, 2 * CH + DK),)] = (
                    change[one][:, :DK] + (change[two][:, :DK] - both_steps[CH:, :DK])
                ).astype(BF16)
                added[pair] = change[one][:, DK:] + (change[two][:, DK:] - both_steps[CH:, DK:])
                out_add[pair + (slice(0, CH),)] = effect[one][:, DK:]
                out_add[pair + (slice(CH, 2 * CH),)] = effect[two][:, DK:] + both_steps[:CH, DK:]

    states = [jnp.zeros((DK, DK), F32) for _ in range(heads)]
    for c in range(blocks // 2):
        for h in range(heads):
            moved = dot(state_map[h, c], states[h].astype(BF16))
            out = moved[:2 * CH] + out_add[h, c]
            states[h] = states[h] - moved[2 * CH:] + added[h, c]
            out = out * lax.rsqrt(jnp.mean(out * out, -1, keepdims=True) + EPSILON) * head_gain_ref[...]
            mixed[c * 2 * CH:(c + 1) * 2 * CH, h * DK:(h + 1) * DK] = out.astype(BF16)
    own = length // count
    targets = [me_ref[0]] + [lax.rem(me_ref[0] + shift, count) for shift in SENT]
    rolled = jnp.concatenate([mixed[rows_at(block, own), :] for block in targets], 0)
    result = dot(rolled, wo_ref[...]).astype(BF16)
    for k, o in enumerate((o0, o1, o2, o3)):
        o[...] = result[k * own:(k + 1) * own]


UNROLL = 8


def mixer(me, gain, top, bottom, weights, sums, head_gain, wo):
    count = gain.shape[0]
    length = 2 * top.shape[0]
    heads = weights[0].shape[1] // DK
    blocks = length // CH
    own = length // count
    vmem = pl.BlockSpec(memory_space=pltpu.VMEM)
    return pl.pallas_call(
        lambda *refs: mixer_kernel(heads, *refs),
        out_shape=[jax.ShapeDtypeStruct((own, wo.shape[1]), BF16)] * count,
        in_specs=[pl.BlockSpec(memory_space=pltpu.SMEM)] + [vmem] * 12,
        out_specs=[vmem] * count,
        scratch_shapes=[
            pltpu.VMEM((heads, blocks, 2 * WIDE, DK), BF16),
            pltpu.VMEM((heads, blocks, SUB, DK), F32),
            pltpu.VMEM((heads, blocks, SUB, 2 * DK), BF16),
            pltpu.VMEM((heads, blocks, CH, DK), F32),
            pltpu.VMEM((heads, blocks // 2, 2 * CH + DK, DK), BF16),
            pltpu.VMEM((heads, blocks // 2, DK, DK), F32),
            pltpu.VMEM((heads, blocks // 2, 2 * CH, DK), F32),
            pltpu.VMEM((length, heads * DK), BF16),
        ],
        compiler_params=pltpu.CompilerParams(vmem_limit_bytes=32 * MIB),
        cost_estimate=pl.CostEstimate(flops=2 * 10 ** 10, bytes_accessed=10 ** 7, transcendentals=0),
        name="mixer",
    )(me, gain, top, bottom, *weights, *sums, head_gain, wo)


def slots(ids_ref, experts, total):
    tokens = ids_ref.shape[1]
    capacity = total // experts
    label = iota((experts, tokens), 0)
    chosen = [(label == ids_ref[k:k + 1, :]).astype(F32) for k in range(2)]
    count = chosen[0] + chosen[1]
    before = (iota((tokens, tokens), 0) < iota((tokens, tokens), 1)).astype(BF16)
    earlier = dot(count.astype(BF16), before)
    spread = (iota((total, experts), 0) // capacity == iota((total, experts), 1)).astype(BF16)
    place = dot(spread, earlier.astype(BF16))
    fits = place == (iota((total, tokens), 0) % capacity).astype(F32)
    return chosen, [jnp.where(fits, dot(spread, c.astype(BF16)), 0.0) for c in chosen]


def ready_kernel(experts, me_ref, part_ref, x0, x1, x3, top_ref, bottom_ref, ids_ref, base_ref, chosen_ref):
    own, part = part_ref.shape[0], x0.shape[1]
    me, count = me_ref[0], x0.shape[0] // part_ref.shape[0]
    for shift, x in ((0, x0), (1, x1), (3, x3)):
        block = me if shift == 0 else source_of(me_ref, shift, count)
        base_ref[:, rows_at(block, part)] = x[rows_at(me, own), :].astype(F32)
    half = count // 2
    inner = rows_at(lax.rem(me, half), own)
    far = jnp.where(me < half, top_ref[inner, :].astype(F32), bottom_ref[inner, :].astype(F32))
    base_ref[:, rows_at(source_of(me_ref, half, count), part)] = far
    base_ref[...] = base_ref[...] + part_ref[...].astype(F32)
    _, chosen = slots(ids_ref, experts, chosen_ref.shape[0])
    chosen_ref[...] = (chosen[0] + chosen[1]).astype(BF16)


def ready(me, part, xs, ids, experts, capacity):
    own, width = part.shape
    vmem = pl.BlockSpec(memory_space=pltpu.VMEM)
    return pl.pallas_call(
        lambda *refs: ready_kernel(experts, *refs),
        out_shape=[
            jax.ShapeDtypeStruct((own, width), F32),
            jax.ShapeDtypeStruct((experts * capacity, own), BF16),
        ],
        in_specs=[pl.BlockSpec(memory_space=pltpu.SMEM)] + [vmem] * 7,
        out_specs=[vmem] * 2,
        compiler_params=pltpu.CompilerParams(vmem_limit_bytes=8 * MIB),
        cost_estimate=pl.CostEstimate(flops=2 * 10 ** 9, bytes_accessed=10 ** 6, transcendentals=0),
        name="ready",
    )(me, part, *xs, ids)


def route_kernel(base_ref, p1, p2, p3, gain_ref, chosen_ref, residual_ref, routed_ref, send_ref):
    arrived = [p[...].astype(F32) for p in (p1, p2, p3)]
    residual = (base_ref[...] + arrived[0]) + (arrived[1] + arrived[2])
    residual_ref[...] = residual
    mean = jnp.mean(residual * residual, -1, keepdims=True)
    routed = residual * lax.rsqrt(mean + EPSILON) * gain_ref[...]
    routed_ref[...] = routed
    send_ref[...] = dot(chosen_ref[...], routed.astype(BF16)).astype(BF16)


def route(base, parts, gain, chosen):
    own, width = base.shape
    vmem = pl.BlockSpec(memory_space=pltpu.VMEM)
    return pl.pallas_call(
        route_kernel,
        out_shape=[
            jax.ShapeDtypeStruct((own, width), F32),
            jax.ShapeDtypeStruct((own, width), F32),
            jax.ShapeDtypeStruct((chosen.shape[0], width), BF16),
        ],
        in_specs=[vmem] * 6,
        out_specs=[vmem] * 3,
        compiler_params=pltpu.CompilerParams(vmem_limit_bytes=8 * MIB),
        cost_estimate=pl.CostEstimate(flops=10 ** 9, bytes_accessed=10 ** 7, transcendentals=0),
        name="route",
    )(base, *parts, gain, chosen)


def weigh(routed_ref, router_ref, ids_ref, pick_ref, leading_ref):
    chosen, parts = slots(ids_ref, router_ref.shape[0], pick_ref.shape[1])
    tokens = routed_ref.shape[0]
    for k in range(2):
        pick_ref[k * tokens:(k + 1) * tokens, :] = jnp.transpose(parts[k]).astype(BF16)
    logits = lax.dot_general(
        router_ref[...], routed_ref[...], (((1,), (1,)), ((), ())),
        precision=lax.Precision.HIGHEST, preferred_element_type=F32,
    )
    gap = jnp.sum((chosen[0] - chosen[1]) * logits, 0, keepdims=True)
    leading = 1.0 / (1.0 + jnp.exp(-gap))
    leading_ref[...] = jnp.transpose(jnp.broadcast_to(leading, (128, tokens)))


def expert_kernel(rows_ref, gate_hbm, up_hbm, down_hbm, routed_ref, router_ref, ids_ref, out_ref, pick_ref,
                  leading_ref, gate_ref, up_ref, down_ref, hidden_ref, finished_ref, sems):
    total = rows_ref.shape[0]
    here, width, middle = gate_hbm.shape
    per = total // here
    experts = router_ref.shape[0]
    cap = pick_ref.shape[1] // experts
    deep, tall = width // PIECES, middle // PIECES
    copies, order = {}, []
    for e in range(here):
        for part, (source, target) in enumerate(((gate_hbm, gate_ref), (up_hbm, up_ref), (down_hbm, down_ref))):
            size = tall if part == 2 else deep
            for p in range(PIECES):
                at = (e, pl.ds(p * size, size))
                copies[e, part, p] = pltpu.make_async_copy(source.at[at], target.at[at], sems.at[e, part, p])
        for p in range(PIECES):
            order += [(e, 0, p), (e, 1, p)]
        order += [(e, 2, p) for p in range(PIECES)]
    for key in order[:FLIGHT]:
        copies[key].start()

    def take(*key):
        copies[key].wait()
        following = order.index(key) + FLIGHT
        if following < len(order):
            copies[order[following]].start()

    weigh(routed_ref, router_ref, ids_ref, pick_ref, leading_ref)
    r, c = iota((total, total), 0), iota((total, total), 1)

    def source(i):
        return (i % per) // cap * (here * cap) + i // per * cap + i % cap

    by_expert = (source(r) == c).astype(BF16)
    by_source = (source(c) == r).astype(BF16)
    rows = dot(by_expert, rows_ref[...]).astype(BF16)
    for e in range(here):
        mine = rows[e * per:(e + 1) * per]
        gate = up = 0.0
        for p in range(PIECES):
            at = slice(p * deep, (p + 1) * deep)
            take(e, 0, p)
            gate = gate + dot(mine[:, at], gate_ref[e, at])
            take(e, 1, p)
            up = up + dot(mine[:, at], up_ref[e, at])
        hidden_ref[...] = (gate / (1.0 + jnp.exp(-gate)) * up).astype(BF16)
        result = 0.0
        for p in range(PIECES):
            take(e, 2, p)
            at = slice(p * tall, (p + 1) * tall)
            result = result + dot(hidden_ref[:, at], down_ref[e, at])
        finished_ref[e * per:(e + 1) * per, :] = result.astype(BF16)
    for start in range(0, width, 512):
        at = slice(start, start + 512)
        out_ref[:, at] = dot(by_source, finished_ref[:, at]).astype(BF16)


PIECES = 4
FLIGHT = 10


def experts_here(rows, gate, up, down, routed, router, ids):
    here, width, middle = gate.shape
    per = rows.shape[0] // here
    tokens, experts = routed.shape[0], router.shape[0]
    capacity = 4 * tokens // experts
    vmem = pl.BlockSpec(memory_space=pltpu.VMEM)
    hbm = pl.BlockSpec(memory_space=pltpu.HBM)
    return pl.pallas_call(
        expert_kernel,
        out_shape=[
            jax.ShapeDtypeStruct(rows.shape, BF16),
            jax.ShapeDtypeStruct((2 * tokens, experts * capacity), BF16),
            jax.ShapeDtypeStruct((tokens, 128), F32),
        ],
        in_specs=[vmem] + [hbm] * 3 + [vmem] * 3,
        out_specs=[vmem] * 3,
        scratch_shapes=[
            pltpu.VMEM(gate.shape, BF16),
            pltpu.VMEM(up.shape, BF16),
            pltpu.VMEM(down.shape, BF16),
            pltpu.VMEM((per, middle), BF16),
            pltpu.VMEM(rows.shape, BF16),
            pltpu.SemaphoreType.DMA((here, 3, PIECES)),
        ],
        compiler_params=pltpu.CompilerParams(vmem_limit_bytes=46 * MIB),
        cost_estimate=pl.CostEstimate(flops=5 * 10 ** 9, bytes_accessed=10 ** 7, transcendentals=0),
        name="experts",
    )(rows, *[pltpu.with_memory_space_constraint(w, pltpu.HBM) for w in (gate, up, down)], routed, router, ids)


def combine_kernel(residual_ref, leading_ref, pick_ref, back_ref, out_ref):
    tokens = residual_ref.shape[0]
    picked = dot(pick_ref[...], back_ref[...])
    leading = leading_ref[:, 0:1]
    blended = leading * picked[:tokens] + (1.0 - leading) * picked[tokens:]
    out_ref[...] = (residual_ref[...] + blended).astype(BF16)


def combine(residual, leading, pick, back):
    vmem = pl.BlockSpec(memory_space=pltpu.VMEM)
    return pl.pallas_call(
        combine_kernel,
        out_shape=jax.ShapeDtypeStruct(residual.shape, BF16),
        in_specs=[vmem] * 4,
        out_specs=vmem,
        compiler_params=pltpu.CompilerParams(vmem_limit_bytes=16 * MIB),
        cost_estimate=pl.CostEstimate(flops=10 ** 9, bytes_accessed=10 ** 6, transcendentals=0),
        name="combine",
    )(residual, leading, pick, back)


def passed(x, k, axis):
    size = lax.axis_size(axis)
    return lax.ppermute(x, axis, [(i, (i + k) % size) for i in range(size)])


def shards(tokens, mixer_gain, query_weight, key_weight, value_weight, beta_weight, head_gain, output_weight,
           expert_gain, router_weight, expert_ids, gate_weight, up_weight, down_weight):
    owners = lax.axis_size("dp")
    me = lax.axis_index("head").reshape(1).astype(jnp.int32)
    left, right = (passed(tokens, shift, "head") for shift in NEAR)
    half = tokens.shape[0] // 2
    top, bottom = passed(left[:half], NEAR[0], "head"), passed(right[half:], NEAR[1], "head")
    gain = mixer_gain.reshape(lax.axis_size("head"), -1)
    here = first(me, gain, tokens, query_weight, key_weight, value_weight, beta_weight.T, head_gain.reshape(1, -1),
                 output_weight)
    weights, sums = here[1:5], here[7:]
    for shift, x in zip(NEAR, (left, right)):
        sums = more(shift, me, gain, x, weights, sums)
    parts = mixer(me, gain, top, bottom, weights, sums, here[5], here[6])
    arriving = [passed(part, shift, "head") for shift, part in zip(SENT, parts[1:])]
    experts = router_weight.shape[1]
    capacity = 4 * parts[0].shape[0] // experts
    ids = expert_ids.T
    base, chosen = ready(me, parts[0], (here[0], left, right, top, bottom), ids, experts, capacity)
    residual, routed, outgoing = route(base, arriving, expert_gain.reshape(1, -1), chosen)
    width = outgoing.shape[1]

    def exchanged(rows):
        rows = rows.reshape(owners, -1, width)
        rows = lax.all_to_all(rows, "dp", split_axis=0, concat_axis=0, tiled=True)
        return rows.reshape(-1, width)

    result, pick, leading = experts_here(
        exchanged(outgoing), gate_weight, up_weight, down_weight, routed, router_weight.T, ids
    )
    return combine(residual, leading, pick, exchanged(result))


def solution(mesh):
    return jax.shard_map(
        shards,
        mesh=mesh,
        in_specs=(
            P("dp", "head"),
            P(),
            P(None, "head"),
            P(None, None, "head"),
            P(None, None, "head"),
            P(None, "head"),
            P(),
            P("head", None),
            P(),
            P(),
            P(("dp", "head"), None),
            P("dp", None, None),
            P("dp", None, None),
            P("dp", None, None),
        ),
        out_specs=P(("dp", "head"), None),
        check_vma=False,
    )
```
